128 devices in a mesh: gx: 8 (over x, z_lo), gy: 16 (over z_hi, y, core).
Axes of the slice: x: 4, y: 4, z: 4 (z_hi: 2, z_lo: 2; z = z_hi * 2 + z_lo), core: 2. Of those that a mesh axis runs over, the one named last changes fastest.
Arguments:
- position: float32 [2, 48, 96, 128], P(None, 'gx', 'gy'), may hold values from 0 to 1
- velocity: float32 [2, 48, 96, 128], P(None, 'gx', 'gy'), may hold values from -3 to 3
- other_accel: float32 [2, 48, 96, 128], P(None, 'gx', 'gy'), may hold values from -5 to 5
- phase_ids: int32 [48, 96, 128], P('gx', 'gy'), may hold values from 0 to 1, as said below
- counts: int32 [48, 96], P('gx', 'gy'), may hold values from 48 to 128, as said below
Outputs:
- new_position: float32 [2, 48, 96, 128], P(None, 'gx', 'gy')
- new_velocity: float32 [2, 48, 96, 128], P(None, 'gx', 'gy')
- pressure: float32 [48, 96, 128], P('gx', 'gy')
- monitor: float32 [4, 4], replicated
The draws below stay inside these ranges and needn't reach their ends.
Inputs may be any that keep to these rules, and one draw needn't show every extreme that they name: `counts`: each entry is the number of live slots of its cell; the live slots are the first ones of the cell; some cell holds 128. `phase_ids`: both phases occur among the live slots.
All inputs are finite; a program needn't handle non-finite values.
Results may differ from the reference program's by a relative error of at most 0.0001.
Values sent between devices are 32-bit elements; how exact they have to be, the bound alone decides.
A program may use at most 64 MiB of HBM per device.

```python
import jax
import jax.numpy as jnp
from jax import lax

SLOTS = 128
ITERS = 4
CELLS_X = 48
CELLS_Y = 96


def draw_counts(key, part):
    values = jax.random.randint(key, (CELLS_X, CELLS_Y), 48, SLOTS + 1, dtype=jnp.int32)
    return values.at[0, 0].set(SLOTS)


def draw_phase_ids(key, part):
    values = jax.random.randint(key, (CELLS_X, CELLS_Y, SLOTS), 0, 2, dtype=jnp.int32)
    return values.at[0, 0, 0].set(0).at[0, 0, 1].set(1)


def block_scale(own_key, dims, pieces, smallest, largest):
    factor_of = 1.0
    for axis_at, parts in pieces:
        draws = jax.random.uniform(jax.random.fold_in(jax.random.fold_in(own_key, 6), axis_at), (parts,), jnp.float32, smallest / len(pieces), largest / len(pieces))
        factor_of = factor_of * jnp.repeat(jnp.exp(draws), dims[axis_at] // parts).reshape((-1,) + (1,) * (len(dims) - 1 - axis_at))
    return factor_of


def gaussian(own_key, dims, deviation, reach, split=(), kind=jnp.bfloat16):
    drawn = jax.random.normal(own_key, dims, jnp.float32) * deviation
    if len(split) > 0:
        drawn = block_scale(own_key, dims, split, -0.22, 0.18) * drawn
    return jnp.clip(drawn, min=-reach, max=reach).astype(kind)


def setup_inputs(seed: int = 0) -> dict:
    seeds = jax.random.split(jax.random.key(seed), 6)
    position = jnp.clip(1.0 * jax.random.uniform(seeds[0], (2, CELLS_X, CELLS_Y, SLOTS), jnp.float32) ** block_scale(seeds[0], (2, CELLS_X, CELLS_Y, SLOTS), ((1, 8), (2, 16)), -0.2, 0.2), 0.0, 1.0)
    velocity = gaussian(seeds[1], (2, CELLS_X, CELLS_Y, SLOTS), 0.5, 3.0, ((1, 8), (2, 16)), jnp.float32)
    other_accel = gaussian(seeds[2], (2, CELLS_X, CELLS_Y, SLOTS), 1.0, 5.0, ((1, 8), (2, 16)), jnp.float32)
    phase_ids = draw_phase_ids(jax.random.fold_in(seeds[5], 71), 0)
    counts = draw_counts(jax.random.fold_in(seeds[5], 71), 0)
    return {"position": position, "velocity": velocity, "other_accel": other_accel, "phase_ids": phase_ids, "counts": counts}


TIME_STEP = 0.05
KERNEL_NORM = 4.0 / (3.141592653589793 * 64.0)
REST_LIGHT = 1.2
REST_HEAVY = 1.5
STIFF_LIGHT = 100.0
STIFF_HEAVY = 200.0
MASS_LIGHT = 1.0
MASS_HEAVY = 1.5
SENTINEL = 1.0e30


def window_of(source, off_x, off_y, row_count, col_count):
    return source[1 + off_x:1 + off_x + row_count, 1 + off_y:1 + off_y + col_count]


def pair_sums(centers, padded_list, with_force):
    center_x, center_y = centers[0], centers[1]
    near_x, near_y, near_live = padded_list[0], padded_list[1], padded_list[2]
    row_count, col_count = center_x.shape[0], center_x.shape[1]
    total_a = jnp.zeros_like(center_x)
    total_b = jnp.zeros_like(center_x)
    for off_x in (-1, 0, 1):
        for off_y in (-1, 0, 1):
            other_x = window_of(near_x, off_x, off_y, row_count, col_count)
            other_y = window_of(near_y, off_x, off_y, row_count, col_count)
            other_live = window_of(near_live, off_x, off_y, row_count, col_count)
            diff_x = center_x[..., :, None] - (other_x[..., None, :] + off_x)
            diff_y = center_y[..., :, None] - (other_y[..., None, :] + off_y)
            intersection = jnp.maximum(1.0 - diff_x * diff_x - diff_y * diff_y, 0.0) * other_live[..., None, :]
            if with_force:
                other_term = window_of(padded_list[3], off_x, off_y, row_count, col_count)
                pair_coef = intersection * intersection * (centers[2][..., :, None] + other_term[..., None, :])
                total_a = total_a + jnp.sum(pair_coef * diff_x, axis=-1)
                total_b = total_b + jnp.sum(pair_coef * diff_y, axis=-1)
            else:
                total_a = total_a + jnp.sum(intersection * intersection * intersection, axis=-1)
    if with_force:
        return (total_a, total_b)
    return (total_a,)


def blocked(with_force, centers, padded_list, row_count):
    block_count = row_count // 2

    def one_block(block_index):
        first_row = block_index * 2
        center_part = tuple(lax.dynamic_slice_in_dim(source, first_row, 2, 0) for source in centers)
        padded_part = tuple(lax.dynamic_slice_in_dim(source, first_row, 4, 0) for source in padded_list)
        return pair_sums(center_part, padded_part, with_force)

    results = lax.map(one_block, jnp.arange(block_count, dtype=jnp.int32))
    return tuple(source.reshape((row_count,) + source.shape[2:]) for source in results)


def local_bounds(density_ratio, live_bool, heavy_bool):
    light_sel = live_bool & jnp.logical_not(heavy_bool)
    heavy_sel = live_bool & heavy_bool
    top_ratio = jnp.stack([jnp.max(jnp.where(light_sel, density_ratio, -SENTINEL)),
                           jnp.max(jnp.where(heavy_sel, density_ratio, -SENTINEL))])
    low_ratio = jnp.stack([jnp.min(jnp.where(light_sel, density_ratio, SENTINEL)),
                           jnp.min(jnp.where(heavy_sel, density_ratio, SENTINEL))])
    return top_ratio, low_ratio


def wrapped(source):
    return jnp.pad(source, ((1, 1), (1, 1), (0, 0)), mode="wrap")


def reference(position, velocity, other_accel, phase_ids, counts):
    slot_index = jnp.arange(position.shape[-1], dtype=jnp.int32)
    live_bool = slot_index[None, None, :] < counts[:, :, None]
    heavy_bool = phase_ids == 1
    live_mask = live_bool.astype(jnp.float32)
    rest_density = jnp.where(heavy_bool, REST_HEAVY, REST_LIGHT).astype(jnp.float32)
    stiffness = jnp.where(heavy_bool, STIFF_HEAVY, STIFF_LIGHT).astype(jnp.float32)
    particle_mass = jnp.where(heavy_bool, MASS_HEAVY, MASS_LIGHT).astype(jnp.float32)
    pressure = jnp.zeros_like(live_mask)
    accel_x = jnp.zeros_like(live_mask)
    accel_y = jnp.zeros_like(live_mask)
    monitor_rows = []
    row_total = position.shape[1]
    for iteration in range(ITERS):
        vel_x = velocity[0] + TIME_STEP * (other_accel[0] + accel_x)
        vel_y = velocity[1] + TIME_STEP * (other_accel[1] + accel_y)
        pos_x = position[0] + TIME_STEP * vel_x
        pos_y = position[1] + TIME_STEP * vel_y
        (density_sum,) = blocked(False, (pos_x, pos_y), (wrapped(pos_x), wrapped(pos_y), wrapped(live_mask)), row_total)
        density = KERNEL_NORM * density_sum
        density_ratio = density / rest_density
        top_ratio, low_ratio = local_bounds(density_ratio, live_bool, heavy_bool)
        relaxation = 1.0 / (1.0 + top_ratio - low_ratio)
        particle_relax = jnp.where(heavy_bool, relaxation[1], relaxation[0])
        pressure = live_mask * (pressure + stiffness * particle_relax * (density_ratio - 1.0))
        safe_density = jnp.where(live_bool, density, 1.0)
        press_term = jnp.where(live_bool, pressure / (safe_density * safe_density), 0.0)
        force_x, force_y = blocked(True, (pos_x, pos_y, press_term),
                                   (wrapped(pos_x), wrapped(pos_y), wrapped(live_mask), wrapped(press_term)), row_total)
        accel_x = live_mask * (6.0 * KERNEL_NORM / particle_mass) * force_x
        accel_y = live_mask * (6.0 * KERNEL_NORM / particle_mass) * force_y
        monitor_rows.append(jnp.concatenate([top_ratio, low_ratio]))
    new_vel_x = live_mask * (velocity[0] + TIME_STEP * (other_accel[0] + accel_x))
    new_vel_y = live_mask * (velocity[1] + TIME_STEP * (other_accel[1] + accel_y))
    new_pos_x = live_mask * (position[0] + TIME_STEP * new_vel_x)
    new_pos_y = live_mask * (position[1] + TIME_STEP * new_vel_y)
    return (jnp.stack([new_pos_x, new_pos_y]), jnp.stack([new_vel_x, new_vel_y]), pressure, jnp.stack(monitor_rows))
```

```python
import functools

import jax
import jax.numpy as jnp
from jax import lax
from jax.experimental import pallas as pl
from jax.experimental.pallas import tpu as pltpu
from jax.sharding import PartitionSpec as P

ITERS = 4
TIME_STEP = 0.05
KERNEL_NORM = 4.0 / (3.141592653589793 * 64.0)
REST_LIGHT = 1.2
REST_HEAVY = 1.5
STIFF_LIGHT = 100.0
STIFF_HEAVY = 200.0
MASS_LIGHT = 1.0
MASS_HEAVY = 1.5
FAR = float(2**30)
NEG = -1e30
MESH = pl.DeviceIdType.MESH
ROWS = 6
COLS = 6
FS = 64
DIRS = ((-1, 0), (1, 0), (0, -1), (0, 1), (-1, -1), (-1, 1), (1, -1), (1, 1))

f32 = jnp.float32
bf16 = jnp.bfloat16


def rnd(v):
    return v.astype(bf16).astype(f32)


def split3(v):
    h = rnd(v)
    r = v - h
    m = rnd(r)
    return h, m, rnd(r - m)


def kernel(
    pos_ref, vel_ref, oa_ref, code_ref,
    npos_ref, nvel_ref, pres_ref, mon_ref,
    st, xp, tp, stage, tstage, rb, trb, fb, ib, lt, wb, dens, tf, mb, al, be, ar0, ar1, ar2,
    hs, hr, ts, tr, a1s, a1r, a2s, a2r,
):
    gx = lax.axis_index("gx")
    gy = lax.axis_index("gy")
    nx = lax.axis_size("gx")
    ny = lax.axis_size("gy")

    def around(dx, dy):
        return (lax.rem(gx + dx + nx, nx), lax.rem(gy + dy + ny, ny))

    barrier = pltpu.get_barrier_semaphore()
    partners = []
    for dx, dy in DIRS:
        partners.append(around(dx, dy))
    for d in range(2, ny - 1):
        partners.append(around(0, d))
    for d in range(2, nx - 1):
        partners.append(around(d, 0))
    for partner in partners:
        pl.semaphore_signal(barrier, inc=1, device_id=partner, device_id_type=MESH)

    st[...] = jnp.zeros_like(st)
    dens[...] = jnp.zeros_like(dens)
    mb[...] = jnp.zeros_like(mb)
    for a in range(ROWS):
        for f in range(2):
            st[f, a, 0:COLS, :] = pos_ref[f, a]
            st[2 + f, a, 0:COLS, :] = vel_ref[f, a]
            st[9 + f, a, 0:COLS, :] = oa_ref[f, a]
        code = code_ref[a]
        st[4, a, 0:COLS, :] = (code > 0.5).astype(f32)
        st[5, a, 0:COLS, :] = (code > 1.5).astype(f32)

    k = lax.broadcasted_iota(jnp.int32, (16, 128), 0)
    for ox in (-1, 0, 1):
        for oy in (-1, 0, 1):
            o = (ox + 1) * 3 + oy + 1
            al[o] = jnp.where(
                k < 2, 1.0,
                jnp.where((k >= 8) & (k < 11), 2.0 * ox, jnp.where((k >= 11) & (k < 14), 2.0 * oy, 0.0)),
            )
            be[o] = jnp.where(
                (k >= 2) & (k < 5), -2.0 * ox,
                jnp.where(
                    (k >= 5) & (k < 8), -2.0 * oy, jnp.where(k == 14, 1.0 - ox * ox - oy * oy, 0.0)
                ),
            )

    sub = lax.broadcasted_iota(jnp.int32, (8, 128), 0)
    col_at = jnp.where(sub == 7, -1, sub).astype(f32) - 2.5
    lane = lax.broadcasted_iota(jnp.int32, (1, 128), 1)

    pl.semaphore_wait(barrier, len(partners))

    def halo_copies(it, src, staged, dst, send, recv):
        copies = []
        for d, (dx, dy) in enumerate(DIRS):
            if d == 0:
                source = src.at[:, 1]
            elif d == 1:
                source = src.at[:, ROWS]
            else:
                source = staged.at[d]
            copies.append(
                pltpu.make_async_remote_copy(
                    src_ref=source,
                    dst_ref=dst.at[it, d],
                    send_sem=send.at[it, d],
                    recv_sem=recv.at[it, d],
                    device_id=around(dx, dy),
                    device_id_type=MESH,
                )
            )
        return copies

    def pack(src, staged, fields):
        for f in range(fields):
            for a in range(ROWS):
                staged[2, f, a, :] = src[f, a + 1, 0, :]
                staged[3, f, a, :] = src[f, a + 1, COLS - 1, :]
            staged[4, f, 0, :] = src[f, 1, 0, :]
            staged[5, f, 0, :] = src[f, 1, COLS - 1, :]
            staged[6, f, 0, :] = src[f, ROWS, 0, :]
            staged[7, f, 0, :] = src[f, ROWS, COLS - 1, :]

    def unpack(it, dst, got, fields):
        for f in range(fields):
            dst[f, ROWS + 1] = got[it, 0, f]
            dst[f, 0] = got[it, 1, f]
            for a in range(ROWS):
                dst[f, a + 1, 6, :] = got[it, 2, f, a, :]
                dst[f, a + 1, 7, :] = got[it, 3, f, a, :]
            dst[f, ROWS + 1, 6, :] = got[it, 4, f, 0, :]
            dst[f, ROWS + 1, 7, :] = got[it, 5, f, 0, :]
            dst[f, 0, 6, :] = got[it, 6, f, 0, :]
            dst[f, 0, 7, :] = got[it, 7, f, 0, :]

    def put(buf, index, value):
        for r in range(value.shape[0]):
            buf[index * FS + r * 8 : index * FS + r * 8 + 8, :] = value[r]

    def put_own(buf, index, value):
        for r in range(value.shape[0]):
            buf[index * FS + r * 8 + 8 : index * FS + r * 8 + 16, :] = value[r]

    def iteration(it, carry):
        live = st[4]
        heavy = st[5]
        alive = live > 0.5
        for f in range(2):
            v = st[2 + f] + TIME_STEP * (st[9 + f] + st[7 + f])
            x = st[f] + TIME_STEP * v - 0.5
            xp[f, 1 : ROWS + 1] = jnp.where(alive, x, FAR)
        pack(xp, stage, 2)
        copies = halo_copies(it, xp, stage, rb, hs, hr)
        for copy in copies:
            copy.start()
        for copy in copies:
            copy.wait()
        unpack(it, xp, rb, 2)

        x = xp[0]
        y = xp[1]
        xs = split3(x)
        ys = split3(y)
        rs = split3(x * x + y * y)
        one = jnp.ones_like(x)
        zero = jnp.zeros_like(x)
        h, m, l = 0, 1, 2
        jrow = (
            [xs[q] for q in (h, h, m, m, l, h)] + [ys[q] for q in (h, h, m, m, l, h)]
            + list(rs) + [one, one, one] + list(xs) + list(ys) + [one] * 7 + [zero]
        )
        irow = (
            [2.0 * xs[q] for q in (h, m, h, m, h, l)] + [2.0 * ys[q] for q in (h, m, h, m, h, l)]
            + [-one] * 3 + [-q for q in rs] + [zero] * 6 + list(xs) + list(ys) + [zero, zero]
        )
        for q in range(32):
            put(fb, q, jrow[q])
            put_own(ib, q, irow[q][1 : ROWS + 1])

        def transposes(r, c):
            for g in range(3):
                parts = []
                for b in range(2 * g - 1, 2 * g + 3):
                    parts.append(fb[pl.ds(r * 8 + b % 8, 32, stride=FS), :])
                lt[r * 3 + g] = jnp.concatenate(parts, axis=0).T.astype(bf16)
            return c

        lax.fori_loop(0, ROWS + 2, transposes, 0)

        def density(a, c):
            for g in range(3):
                base = []
                for e in range(2):
                    base.append(ib[pl.ds((a + 1) * 8 + 2 * g + e, 32, stride=FS), :])
                total = jnp.zeros((8, 256), f32)
                for ox in (-1, 0, 1):
                    left = lt[(a + 1 + ox) * 3 + g]
                    for n in range(3):
                        o = (ox + 1) * 3 + n
                        halves = []
                        for e in range(2):
                            part = jnp.concatenate(
                                [base[e][0:16], base[e][16:32] * al[o] + be[o]], axis=0
                            ).astype(bf16)
                            pieces = []
                            if n + e > 0:
                                pieces.append(jnp.zeros((32 * (n + e), 128), bf16))
                            pieces.append(part)
                            if n + e < 3:
                                pieces.append(jnp.zeros((32 * (3 - n - e), 128), bf16))
                            halves.append(jnp.concatenate(pieces, axis=0))
                        right = jnp.concatenate(halves, axis=1)
                        w = jnp.maximum(jnp.dot(left, right, preferred_element_type=f32), 0.0)
                        w2 = w * w
                        wb[(a * 3 + g) * 9 + o] = w2
                        total = total + jnp.sum((w2 * w).reshape(16, 8, 256), axis=0)
                row = jnp.sum(total, axis=0, keepdims=True)
                dens[a, 2 * g : 2 * g + 1, :] = row[:, 0:128]
                dens[a, 2 * g + 1 : 2 * g + 2, :] = row[:, 128:256]
            return c

        lax.fori_loop(0, ROWS, density, 0)

        density_now = KERNEL_NORM * dens[...]
        hot = heavy > 0.5
        ratio = density_now / jnp.where(hot, REST_HEAVY, REST_LIGHT)
        lit = alive & jnp.logical_not(hot)
        hvy = alive & hot
        peaks = (
            jnp.where(lit, ratio, NEG), jnp.where(hvy, ratio, NEG),
            jnp.where(lit, -ratio, NEG), jnp.where(hvy, -ratio, NEG),
        )
        vec = jnp.full((1, 128), NEG, f32)
        for q in range(4):
            top = jnp.max(jnp.max(peaks[q], axis=0), axis=0, keepdims=True)
            top = jnp.max(top, axis=1, keepdims=True)
            vec = jnp.where(lane == q, top, vec)

        ar0[it, 0] = vec
        first = []
        for d in range(1, ny):
            first.append(
                pltpu.make_async_remote_copy(
                    src_ref=ar0.at[it, 0], dst_ref=ar1.at[it, d],
                    send_sem=a1s.at[it, d], recv_sem=a1r.at[it, d],
                    device_id=around(0, d), device_id_type=MESH,
                )
            )
        for copy in first:
            copy.start()

        safe = jnp.where(alive, density_now, 1.0)
        inverse = 1.0 / (safe * safe)
        excess = jnp.where(hot, STIFF_HEAVY, STIFF_LIGHT) * (ratio - 1.0)
        t0 = jnp.where(alive, st[6] * inverse, 0.0)
        u = excess * inverse
        u0 = jnp.where(lit, u, 0.0)
        u1 = jnp.where(hvy, u, 0.0)
        tp[0, 1 : ROWS + 1] = t0
        tp[1, 1 : ROWS + 1] = u0
        tp[2, 1 : ROWS + 1] = u1
        pack(tp, tstage, 3)
        tcopies = halo_copies(it, tp, tstage, trb, ts, tr)
        for copy in tcopies:
            copy.start()
        for copy in tcopies:
            copy.wait()
        unpack(it, tp, trb, 3)

        for copy in first:
            copy.wait()
        best = vec
        for d in range(1, ny):
            best = jnp.maximum(best, ar1[it, d])
        ar0[it, 1] = best
        second = []
        for d in range(1, nx):
            second.append(
                pltpu.make_async_remote_copy(
                    src_ref=ar0.at[it, 1], dst_ref=ar2.at[it, d],
                    send_sem=a2s.at[it, d], recv_sem=a2r.at[it, d],
                    device_id=around(d, 0), device_id_type=MESH,
                )
            )
        for copy in second:
            copy.start()

        def moments(r, c):
            shift = lax.convert_element_type(r, f32) - 3.5
            px = xp[0, r] + shift
            py = xp[1, r] + col_at
            fields = (None, tp[0, r], tp[1, r], tp[2, r])
            base = r * 8
            if True:
                for q in range(4):
                    for e, p in enumerate((px, py)):
                        value = p if fields[q] is None else p * fields[q]
                        for level, piece in enumerate(split3(value)):
                            fb[pl.ds((level * 8 + 2 * q + e) * FS + base, 8), :] = piece
                    if fields[q] is None:
                        hi, lo = jnp.ones_like(px), jnp.zeros_like(px)
                    else:
                        hi = rnd(fields[q])
                        lo = rnd(fields[q] - hi)
                    fb[pl.ds((24 + q) * FS + base, 8), :] = hi
                    fb[pl.ds((28 + q) * FS + base, 8), :] = lo
            for b in range(-1, COLS + 1):
                tf[r, b + 1] = fb[pl.ds(base + b % 8, 32, stride=FS), :].astype(bf16)
            return c

        lax.fori_loop(0, ROWS + 2, moments, 0)

        def force(a, c):
            for g in range(3):
                total = jnp.zeros((64, 256), f32)
                for ox in (-1, 0, 1):
                    for n in range(3):
                        o = (ox + 1) * 3 + n
                        w2 = wb[(a * 3 + g) * 9 + o]
                        hi = w2.astype(bf16)
                        lo = (w2 - hi.astype(f32)).astype(bf16)
                        left = tf[a + 1 + ox, 2 * g + n : 2 * g + n + 2].reshape(64, 128)
                        both = jnp.concatenate([left, left], axis=1)
                        total = total + jnp.dot(
                            both, jnp.concatenate([hi, lo], axis=0), preferred_element_type=f32
                        )
                for e in range(2):
                    part = total[32 * e : 32 * e + 32, 128 * e : 128 * e + 128]
                    row = a * 8 + 2 * g + e
                    mb[pl.ds(row, 8, stride=FS), :] = part[0:8] + part[8:16] + part[16:24]
                    mb[pl.ds(8 * FS + row, 8, stride=FS), :] = part[24:32]
            return c

        lax.fori_loop(0, ROWS, force, 0)

        for copy in second:
            copy.wait()
        for d in range(1, nx):
            best = jnp.maximum(best, ar2[it, d])
        mon_ref[pl.ds(it, 1), :] = jnp.where(lane < 2, best, -best)[:, 0:4]
        relax0 = 1.0 / (1.0 + best[:, 0:1] + best[:, 2:3])
        relax1 = 1.0 / (1.0 + best[:, 1:2] + best[:, 3:4])
        relax0 = jnp.broadcast_to(relax0, (8, 128))
        relax1 = jnp.broadcast_to(relax1, (8, 128))

        for a in range(ROWS):
            def mom(q):
                return mb[q * FS + a * 8 : q * FS + a * 8 + 8, :]

            on = alive[a]
            ti = t0[a] + relax0 * u0[a] + relax1 * u1[a]
            s1 = mom(8) + mom(12)
            s_t = (mom(9) + mom(13)) + relax0 * (mom(10) + mom(14)) + relax1 * (mom(11) + mom(15))
            factor = 6.0 * KERNEL_NORM / jnp.where(hot[a], MASS_HEAVY, MASS_LIGHT)
            for f in range(2):
                p = xp[f, a + 1] + (a - 2.5 if f == 0 else col_at)
                s_p = mom(f)
                s_tp = mom(2 + f) + relax0 * mom(4 + f) + relax1 * mom(6 + f)
                push = ti * (p * s1 - s_p) + p * s_t - s_tp
                st[7 + f, a] = jnp.where(on, factor * push, 0.0)
            relax = jnp.where(hot[a], relax1, relax0)
            st[6, a] = jnp.where(on, st[6, a] + relax * excess[a], 0.0)
        return carry

    lax.fori_loop(0, ITERS, iteration, 0)

    live = st[4]
    for f in range(2):
        v = live * (st[2 + f] + TIME_STEP * (st[9 + f] + st[7 + f]))
        p = live * (st[f] + TIME_STEP * v)
        for a in range(ROWS):
            nvel_ref[f, a] = v[a, 0:COLS]
            npos_ref[f, a] = p[a, 0:COLS]
    for a in range(ROWS):
        pres_ref[a] = st[6, a, 0:COLS, :]


def local(nx, ny, position, velocity, other_accel, phase_ids, counts):
    slot = jnp.arange(128, dtype=jnp.int32)
    code = jnp.where(slot[None, None, :] < counts[:, :, None], phase_ids + 1, 0).astype(f32)
    vmem = pl.BlockSpec(memory_space=pltpu.VMEM)
    dma = pltpu.SemaphoreType.DMA
    return pl.pallas_call(
        kernel,
        out_shape=(
            jax.ShapeDtypeStruct((2, ROWS, COLS, 128), f32),
            jax.ShapeDtypeStruct((2, ROWS, COLS, 128), f32),
            jax.ShapeDtypeStruct((ROWS, COLS, 128), f32),
            jax.ShapeDtypeStruct((ITERS, 4), f32),
        ),
        in_specs=[vmem] * 4,
        out_specs=[vmem] * 4,
        scratch_shapes=[
            pltpu.VMEM((11, ROWS, 8, 128), f32),
            pltpu.VMEM((2, 8, 8, 128), f32),
            pltpu.VMEM((3, 8, 8, 128), f32),
            pltpu.VMEM((8, 2, 8, 128), f32),
            pltpu.VMEM((8, 3, 8, 128), f32),
            pltpu.VMEM((ITERS, 8, 2, 8, 128), f32),
            pltpu.VMEM((ITERS, 8, 3, 8, 128), f32),
            pltpu.VMEM((32 * FS, 128), f32),
            pltpu.VMEM((32 * FS, 128), f32),
            pltpu.VMEM((24, 128, 128), bf16),
            pltpu.VMEM((162, 128, 256), f32),
            pltpu.VMEM((ROWS, 8, 128), f32),
            pltpu.VMEM((8, 8, 32, 128), bf16),
            pltpu.VMEM((16 * FS, 128), f32),
            pltpu.VMEM((9, 16, 128), f32),
            pltpu.VMEM((9, 16, 128), f32),
            pltpu.VMEM((ITERS, 2, 1, 128), f32),
            pltpu.VMEM((ITERS, ny, 1, 128), f32),
            pltpu.VMEM((ITERS, nx, 1, 128), f32),
            dma((ITERS, 8)), dma((ITERS, 8)), dma((ITERS, 8)), dma((ITERS, 8)),
            dma((ITERS, ny)), dma((ITERS, ny)), dma((ITERS, nx)), dma((ITERS, nx)),
        ],
        compiler_params=pltpu.CompilerParams(
            collective_id=0, has_side_effects=True, vmem_limit_bytes=60 * 1024 * 1024
        ),
    )(position, velocity, other_accel, code)


def solution(mesh):
    in_specs = (
        P(None, "gx", "gy", None),
        P(None, "gx", "gy", None),
        P(None, "gx", "gy", None),
        P("gx", "gy", None),
        P("gx", "gy"),
    )
    out_specs = (P(None, "gx", "gy", None), P(None, "gx", "gy", None), P("gx", "gy", None), P())
    run = functools.partial(local, mesh.shape["gx"], mesh.shape["gy"])
    return jax.shard_map(run, mesh=mesh, in_specs=in_specs, out_specs=out_specs, check_vma=False)
```

```python
import jax
import jax.numpy as jnp
from jax import lax
from jax.experimental import pallas as pl
from jax.experimental.pallas import tpu as pltpu
from jax.sharding import Mesh
from jax.sharding import PartitionSpec as P

ITERS = 4
TIME_STEP = 0.05
KERNEL_NORM = 4.0 / (3.141592653589793 * 64.0)
REST_LIGHT = 1.2
REST_HEAVY = 1.5
STIFF_LIGHT = 100.0
STIFF_HEAVY = 200.0
MASS_LIGHT = 1.0
MASS_HEAVY = 1.5
FAR = float(2**30)
NEG = -1e30
MESH = pl.DeviceIdType.MESH
SPLIT = ("x", "zl", "zh", "y", "core")
ROWS = 6
COLS = 6
TOP, BOTTOM, LEFT, RIGHT = 0, 7, 8, 9
BLOCKS = 10
FS = BLOCKS * 8
DIRS = ((-1, 0), (1, 0), (0, -1), (0, 1), (-1, -1), (-1, 1), (1, -1), (1, 1))
OWN_TILES = (
    (0, 1, 0, 1, 0), (0, 1, 1, 2, 0),
    (2, 3, 1, 2, 0), (2, 3, 2, 3, 0), (2, 3, 3, 4, 1),
    (4, 5, 3, 4, 1), (4, 5, 4, 5, 1),
    (1, 4, 0, 5, 2),
)
GROUP_START = (0, 2)

f32 = jnp.float32
bf16 = jnp.bfloat16


def rnd(v):
    return v.astype(bf16).astype(f32)


def split3(v):
    h = rnd(v)
    r = v - h
    m = rnd(r)
    return h, m, rnd(r - m)


def feature_rows(x, y):
    xs = split3(x)
    ys = split3(y)
    rs = split3(x * x + y * y)
    one = jnp.ones_like(x)
    zero = jnp.zeros_like(x)
    h, m, l = 0, 1, 2
    jrow = (
        [xs[q] for q in (h, h, m, m, l, h)] + [ys[q] for q in (h, h, m, m, l, h)]
        + list(rs) + [one, one, one] + list(xs) + list(ys) + [one] * 7 + [zero]
    )
    irow = (
        [2.0 * xs[q] for q in (h, m, h, m, h, l)] + [2.0 * ys[q] for q in (h, m, h, m, h, l)]
        + [-one] * 3 + [-q for q in rs] + [zero] * 6 + list(xs) + list(ys) + [zero, zero]
    )
    return jrow, irow


def kernel(
    pos_ref, vel_ref, oa_ref, phase_ref, counts_ref,
    npos_ref, nvel_ref, pres_ref, mon_ref,
    inp, inv, ino, inph, st, xp, tp, stage, tstage, rb, trb, fb, ib, lt, gh, wb, da, fa, tf, mb,
    al, be, ar0, ar1, ar2,
    ins, hs, hr, ts, tr, a1s, a1r, a2s, a2r,
):
    index = {name: lax.axis_index(name) for name in SPLIT}
    size = {name: lax.axis_size(name) for name in SPLIT}
    gx = index["x"] * size["zl"] + index["zl"]
    gy = (index["zh"] * size["y"] + index["y"]) * size["core"] + index["core"]
    nx = size["x"] * size["zl"]
    ny = size["zh"] * size["y"] * size["core"]

    def around(dx, dy):
        px = lax.rem(gx + dx + nx, nx)
        py = lax.rem(gy + dy + ny, ny)
        return (
            px // size["zl"], lax.rem(px, size["zl"]), py // (size["y"] * size["core"]),
            lax.rem(py // size["core"], size["y"]), lax.rem(py, size["core"]),
        )

    def peers(names):
        steps = [()]
        for name in SPLIT:
            count = size[name] if name in names else 1
            steps = [s + (q,) for s in steps for q in range(count)]
        return [
            tuple(lax.rem(index[name] + q, size[name]) for name, q in zip(SPLIT, s))
            for s in steps if any(s)
        ]

    neighbours = [around(dx, dy) for dx, dy in DIRS]
    first_peers = peers(("y", "core"))
    second_peers = peers(("x", "zl", "zh"))
    barrier = pltpu.get_barrier_semaphore()
    for partner in neighbours + first_peers + second_peers:
        pl.semaphore_signal(barrier, inc=1, device_id=partner, device_id_type=MESH)

    loads = [
        pltpu.make_async_copy(src, dst, ins.at[q])
        for q, (src, dst) in enumerate(
            ((pos_ref, inp), (vel_ref, inv), (oa_ref, ino), (phase_ref, inph))
        )
    ]
    for load in loads:
        load.start()

    st[...] = jnp.zeros_like(st)
    da[...] = jnp.zeros_like(da)
    mb[...] = jnp.zeros_like(mb)
    xp[...] = jnp.full_like(xp, FAR)
    tp[...] = jnp.zeros_like(tp)
    fb[...] = jnp.zeros_like(fb)
    stage[...] = jnp.zeros_like(stage)
    tstage[...] = jnp.zeros_like(tstage)
    k = lax.broadcasted_iota(jnp.int32, (16, 128), 0)
    for ox in (-1, 0, 1):
        for oy in (-1, 0, 1):
            o = (ox + 1) * 3 + oy + 1
            al[o] = jnp.where(
                k < 2, 1.0,
                jnp.where((k >= 8) & (k < 11), 2.0 * ox, jnp.where((k >= 11) & (k < 14), 2.0 * oy, 0.0)),
            )
            be[o] = jnp.where(
                (k >= 2) & (k < 5), -2.0 * ox,
                jnp.where(
                    (k >= 5) & (k < 8), -2.0 * oy, jnp.where(k == 14, 1.0 - ox * ox - oy * oy, 0.0)
                ),
            )
    lane = lax.broadcasted_iota(jnp.int32, (1, 128), 1)
    sub = lax.broadcasted_iota(jnp.int32, (8, 128), 0)
    sub_f = sub.astype(f32)
    row_cols = jnp.where(sub == 7, -1.0, sub_f) - 2.5
    for load in loads:
        load.wait()
    for a in range(ROWS):
        for f in range(2):
            for s in range(COLS):
                at = a * 12 + s * 2 + f
                st[f, a, s : s + 1, :] = inp[at : at + 1, :]
                st[2 + f, a, s : s + 1, :] = inv[at : at + 1, :]
                st[9 + f, a, s : s + 1, :] = ino[at : at + 1, :]
        for s in range(COLS):
            st[4, a, s : s + 1, :] = (lane < counts_ref[a, s]).astype(f32)
        st[5, a, 0:COLS, :] = (inph[a] == 1).astype(f32)

    def halo_copies(it, src, staged, dst, send, recv):
        copies = []
        for d in range(8):
            source = src.at[:, (1, ROWS)[d]] if d < 2 else staged.at[d]
            copies.append(
                pltpu.make_async_remote_copy(
                    src_ref=source, dst_ref=dst.at[it, d],
                    send_sem=send.at[it, d], recv_sem=recv.at[it, d],
                    device_id=neighbours[d], device_id_type=MESH,
                )
            )
        return copies

    def pack(src, staged, fields):
        for f in range(fields):
            for a in range(ROWS):
                staged[2, f, a, :] = src[f, a + 1, 0, :]
                staged[3, f, a, :] = src[f, a + 1, COLS - 1, :]
            staged[4, f, 0, :] = src[f, 1, 0, :]
            staged[5, f, 0, :] = src[f, 1, COLS - 1, :]
            staged[6, f, 0, :] = src[f, ROWS, 0, :]
            staged[7, f, 0, :] = src[f, ROWS, COLS - 1, :]

    def unpack(it, dst, got, fields):
        for f in range(fields):
            dst[f, BOTTOM] = got[it, 0, f]
            dst[f, TOP] = got[it, 1, f]
            dst[f, RIGHT] = got[it, 2, f]
            dst[f, LEFT] = got[it, 3, f]
            dst[f, BOTTOM, 6, :] = got[it, 4, f, 0, :]
            dst[f, BOTTOM, 7, :] = got[it, 5, f, 0, :]
            dst[f, TOP, 6, :] = got[it, 6, f, 0, :]
            dst[f, TOP, 7, :] = got[it, 7, f, 0, :]

    def put(buf, rows, base):
        for q, row in enumerate(rows):
            buf[pl.ds(q * FS + base, 8), :] = row

    def cell(buf, c):
        return buf[pl.ds(c, 32, stride=FS), :]

    def turned(cells):
        return jnp.concatenate([cell(fb, c) for c in cells], axis=0).T.astype(bf16)

    def centre(a, col, o):
        base = cell(ib, (a + 1) * 8 + col)
        return jnp.concatenate([base[0:16], base[16:32] * al[o] + be[o]], axis=0).astype(bf16)

    def at_block(part, block, blocks):
        pieces = []
        if block > 0:
            pieces.append(jnp.zeros((32 * block, 128), bf16))
        pieces.append(part)
        if block < blocks - 1:
            pieces.append(jnp.zeros((32 * (blocks - 1 - block), 128), bf16))
        return jnp.concatenate(pieces, axis=0) if len(pieces) > 1 else part

    def overlap(left, right, slot, sums, cols):
        w = jnp.maximum(jnp.dot(left, right, preferred_element_type=f32), 0.0)
        w2 = w * w
        wb[slot] = w2
        part = jnp.sum((w2 * w).reshape(16, 8, 256), axis=0)
        for e in range(2):
            half = part[:, 128 * e : 128 * e + 128]
            sums[cols[e]] = half if sums[cols[e]] is None else sums[cols[e]] + half

    def own_tiles(a, ox3, lrow, slot, sums):
        for q, (ca, cb, ja, jb, group) in enumerate(OWN_TILES):
            pa = centre(a, ca, ox3 + (ja - ca + 1))
            pb = centre(a, cb, ox3 + (jb - cb + 1))
            if group == 2:
                left = jnp.concatenate([lrow[0], lrow[1]], axis=1)
                right = jnp.concatenate([at_block(pa, ja, 8), at_block(pb, jb - 2 + 4, 8)], axis=1)
            else:
                left = lrow[group]
                right = jnp.concatenate(
                    [at_block(pa, ja - GROUP_START[group], 4), at_block(pb, jb - GROUP_START[group], 4)],
                    axis=1,
                )
            overlap(left, right, slot + q, sums, (ca, cb))

    def edge_tile(a, ox3, r, slot, sums):
        pa = centre(a, 0, ox3)
        pb = centre(a, COLS - 1, ox3 + 2)
        odd = (r + 1) % 2
        right = jnp.concatenate([at_block(pa, 2 * odd, 4), at_block(pb, 2 * odd + 1, 4)], axis=1)
        overlap(gh[(r + 1) // 2], right, slot + 8, sums, (0, COLS - 1))

    def pull(w2, left, sums, cols):
        hi = w2.astype(bf16)
        lo = (w2 - hi.astype(f32)).astype(bf16)
        both = jnp.concatenate([left, left], axis=1)
        total = jnp.dot(both, jnp.concatenate([hi, lo], axis=0), preferred_element_type=f32)
        for e in range(2):
            part = total[32 * e : 32 * e + 32, 128 * e : 128 * e + 128]
            sums[cols[e]] = part if sums[cols[e]] is None else sums[cols[e]] + part

    def own_pulls(r, slot, sums):
        for q, (ca, cb, ja, jb, group) in enumerate(OWN_TILES):
            left = jnp.concatenate([tf[r, ja], tf[r, jb]], axis=0)
            pull(wb[slot + q], left, sums, (ca, cb))

    def side_cells(r):
        if r < 0:
            return (TOP, 7), (TOP, 6)
        if r >= ROWS:
            return (BOTTOM, 7), (BOTTOM, 6)
        return (LEFT, r), (RIGHT, r)

    def moment_rows(block, px, py):
        rows = [None] * 32
        for q in range(4):
            field = None if q == 0 else tp[q - 1, block]
            for e, p in enumerate((px, py)):
                pieces = split3(p if field is None else p * field)
                for level in range(3):
                    rows[level * 8 + 2 * q + e] = pieces[level]
            if field is None:
                rows[24], rows[28] = jnp.ones_like(px), jnp.zeros_like(px)
            else:
                rows[24 + q] = rnd(field)
                rows[28 + q] = rnd(field - rows[24 + q])
        return rows

    pl.semaphore_wait(barrier, len(neighbours) + len(first_peers) + len(second_peers))

    def densities(it):
        alive = st[4] > 0.5
        for f in range(2):
            v = st[2 + f] + TIME_STEP * (st[9 + f] + st[7 + f])
            x = st[f] + TIME_STEP * v - 0.5
            xp[f, 1 : ROWS + 1] = jnp.where(alive, x, FAR)
        pack(xp, stage, 2)
        copies = halo_copies(it, xp, stage, rb, hs, hr)
        for copy in copies:
            copy.start()

        for r in range(ROWS):
            jrow, irow = feature_rows(xp[0, r + 1], xp[1, r + 1])
            put(fb, jrow, (r + 1) * 8)
            put(ib, irow, (r + 1) * 8)
        for r in range(ROWS):
            for g in range(2):
                lt[(r + 1) * 2 + g] = turned([(r + 1) * 8 + GROUP_START[g] + s for s in range(4)])
        da[...] = jnp.zeros_like(da)

        def density(t, c):
            a = t // 3
            step = lax.rem(t, 3)
            r = a + step
            sums = [None] * COLS
            own_tiles(a, step * 3, (lt[r * 2], lt[r * 2 + 1]), t * 9, sums)
            for s in range(COLS):
                da[a, s] += sums[s]
            return c

        lax.fori_loop(1, 17, density, 0, unroll=4)

        for copy in copies:
            copy.wait()
        unpack(it, xp, rb, 2)
        for block in (TOP, BOTTOM, LEFT, RIGHT):
            jrow, _ = feature_rows(xp[0, block], xp[1, block])
            put(fb, jrow, block * 8)
        for block in (TOP, BOTTOM):
            for g in range(2):
                lt[block * 2 + g] = turned([block * 8 + GROUP_START[g] + s for s in range(4)])
        for q in range(4):
            cells = [b * 8 + s for r in (2 * q - 1, 2 * q) for b, s in side_cells(r)]
            gh[q] = turned(cells)
        for t in range(18):
            a, ox = t // 3, t % 3 - 1
            r = a + ox
            sums = [None] * COLS
            if r < 0 or r >= ROWS:
                own_tiles(a, (ox + 1) * 3, (lt[(r + 1) * 2], lt[(r + 1) * 2 + 1]), t * 9, sums)
            edge_tile(a, (ox + 1) * 3, r, t * 9, sums)
            for s in range(COLS):
                if sums[s] is not None:
                    da[a, s] += sums[s]

    def bounds_copies(it, src_slot, dst, send, recv, targets):
        return [
            pltpu.make_async_remote_copy(
                src_ref=ar0.at[it, src_slot], dst_ref=dst.at[it, d],
                send_sem=send.at[it, d], recv_sem=recv.at[it, d],
                device_id=target, device_id_type=MESH,
            )
            for d, target in enumerate(targets)
        ]

    def forces(it):
        alive = st[4] > 0.5
        hot = st[5] > 0.5
        rows = []
        for a in range(ROWS):
            cells = [jnp.sum(da[a, s], axis=0, keepdims=True) for s in range(COLS)]
            rows.append(jnp.concatenate(cells + [jnp.zeros((2, 128), f32)], axis=0))
        density_now = KERNEL_NORM * jnp.stack(rows)
        ratio = density_now / jnp.where(hot, REST_HEAVY, REST_LIGHT)
        lit = alive & jnp.logical_not(hot)
        hvy = alive & hot
        peaks = (
            jnp.where(lit, ratio, NEG), jnp.where(hvy, ratio, NEG),
            jnp.where(lit, -ratio, NEG), jnp.where(hvy, -ratio, NEG),
        )
        vec = jnp.full((1, 128), NEG, f32)
        for q in range(4):
            top = jnp.max(jnp.max(peaks[q], axis=0), axis=0, keepdims=True)
            top = jnp.max(top, axis=1, keepdims=True)
            vec = jnp.where(lane == q, top, vec)
        ar0[it, 0] = vec
        first = bounds_copies(it, 0, ar1, a1s, a1r, first_peers)

        safe = jnp.where(alive, density_now, 1.0)
        inverse = 1.0 / (safe * safe)
        excess = jnp.where(hot, STIFF_HEAVY, STIFF_LIGHT) * (ratio - 1.0)
        t0 = jnp.where(alive, st[6] * inverse, 0.0)
        u = excess * inverse
        u0 = jnp.where(lit, u, 0.0)
        u1 = jnp.where(hvy, u, 0.0)
        tp[0, 1 : ROWS + 1] = t0
        tp[1, 1 : ROWS + 1] = u0
        tp[2, 1 : ROWS + 1] = u1
        pack(tp, tstage, 3)
        tcopies = halo_copies(it, tp, tstage, trb, ts, tr)
        for copy in first + tcopies:
            copy.start()

        for a in range(ROWS):
            put(fb, moment_rows(a + 1, xp[0, a + 1] + (a - 2.5), xp[1, a + 1] + row_cols), (a + 1) * 8)
        for a in range(ROWS):
            for s in range(COLS):
                tf[a + 1, s] = cell(fb, (a + 1) * 8 + s).astype(bf16)
        fa[...] = jnp.zeros_like(fa)

        def force(t, c):
            a = t // 3
            step = lax.rem(t, 3)
            sums = [None] * COLS
            own_pulls(a + step, t * 9, sums)
            for s in range(COLS):
                fa[a, s] += sums[s]
            return c

        lax.fori_loop(1, 17, force, 0, unroll=4)

        for copy in first:
            copy.wait()
        best = vec
        for d in range(len(first_peers)):
            best = jnp.maximum(best, ar1[it, d])
        ar0[it, 1] = best
        second = bounds_copies(it, 1, ar2, a2s, a2r, second_peers)
        for copy in second:
            copy.start()

        for copy in tcopies:
            copy.wait()
        unpack(it, tp, trb, 3)
        edge_x = {TOP: -3.5, BOTTOM: 3.5, LEFT: sub_f - 2.5, RIGHT: sub_f - 2.5}
        edge_y = {TOP: row_cols, BOTTOM: row_cols, LEFT: -3.5, RIGHT: 3.5}
        for block in (TOP, BOTTOM, LEFT, RIGHT):
            put(fb, moment_rows(block, xp[0, block] + edge_x[block], xp[1, block] + edge_y[block]), block * 8)
        for block in (TOP, BOTTOM, LEFT, RIGHT):
            for s in range(8 if block in (TOP, BOTTOM) else ROWS):
                tf[block, s] = cell(fb, block * 8 + s).astype(bf16)
        for t in range(18):
            a, ox = t // 3, t % 3 - 1
            r = a + ox
            sums = [None] * COLS
            if r < 0 or r >= ROWS:
                own_pulls(r + 1, t * 9, sums)
            (lb, ls), (rb_, rs_) = side_cells(r)
            pull(
                wb[t * 9 + 8], jnp.concatenate([tf[lb, ls], tf[rb_, rs_]], axis=0), sums, (0, COLS - 1)
            )
            for s in range(COLS):
                if sums[s] is not None:
                    fa[a, s] += sums[s]
        for a in range(ROWS):
            for s in range(COLS):
                part = fa[a, s]
                row = a * 8 + s
                mb[pl.ds(row, 8, stride=FS), :] = part[0:8] + part[8:16] + part[16:24]
                mb[pl.ds(8 * FS + row, 8, stride=FS), :] = part[24:32]

        for copy in second:
            copy.wait()
        for d in range(len(second_peers)):
            best = jnp.maximum(best, ar2[it, d])
        mon_ref[pl.ds(it, 1), :] = jnp.where(lane < 2, best, -best)[:, 0:4]
        relax0 = jnp.broadcast_to(1.0 / (1.0 + best[:, 0:1] + best[:, 2:3]), (8, 128))
        relax1 = jnp.broadcast_to(1.0 / (1.0 + best[:, 1:2] + best[:, 3:4]), (8, 128))

        for a in range(ROWS):
            def mom(q):
                return mb[q * FS + a * 8 : q * FS + a * 8 + 8, :]

            on = alive[a]
            ti = t0[a] + relax0 * u0[a] + relax1 * u1[a]
            s1 = mom(8) + mom(12)
            s_t = (mom(9) + mom(13)) + relax0 * (mom(10) + mom(14)) + relax1 * (mom(11) + mom(15))
            factor = 6.0 * KERNEL_NORM / jnp.where(hot[a], MASS_HEAVY, MASS_LIGHT)
            for f in range(2):
                p = xp[f, a + 1] + (a - 2.5 if f == 0 else row_cols)
                s_p = mom(f)
                s_tp = mom(2 + f) + relax0 * mom(4 + f) + relax1 * mom(6 + f)
                push = ti * (p * s1 - s_p) + p * s_t - s_tp
                st[7 + f, a] = jnp.where(on, factor * push, 0.0)
            relax = jnp.where(hot[a], relax1, relax0)
            st[6, a] = jnp.where(on, st[6, a] + relax * excess[a], 0.0)

    def whole(it, carry):
        densities(it)
        forces(it)
        return carry

    lax.fori_loop(0, ITERS, whole, 0)

    live = st[4]
    for f in range(2):
        v = live * (st[2 + f] + TIME_STEP * (st[9 + f] + st[7 + f]))
        p = live * (st[f] + TIME_STEP * v)
        for a in range(ROWS):
            for s in range(COLS):
                at = a * 12 + s * 2 + f
                nvel_ref[at : at + 1, :] = v[a, s : s + 1]
                npos_ref[at : at + 1, :] = p[a, s : s + 1]
    for a in range(ROWS):
        pres_ref[a] = st[6, a, 0:COLS, :]


def flat(value):
    return value.transpose(1, 2, 0, 3).reshape(ROWS * COLS * 2, 128)


def unflat(value):
    return value.reshape(ROWS, COLS, 2, 128).transpose(2, 0, 1, 3)


def local(position, velocity, other_accel, phase_ids, counts):
    vmem = pl.BlockSpec(memory_space=pltpu.VMEM)
    hbm = pl.BlockSpec(memory_space=pl.ANY)
    dma = pltpu.SemaphoreType.DMA
    n1 = lax.axis_size("y") * lax.axis_size("core") - 1
    n2 = lax.axis_size("x") * lax.axis_size("zl") * lax.axis_size("zh") - 1
    new_pos, new_vel, pressure, monitor = pl.pallas_call(
        kernel,
        out_shape=(
            jax.ShapeDtypeStruct((ROWS * COLS * 2, 128), f32),
            jax.ShapeDtypeStruct((ROWS * COLS * 2, 128), f32),
            jax.ShapeDtypeStruct((ROWS, COLS, 128), f32),
            jax.ShapeDtypeStruct((ITERS, 4), f32),
        ),
        in_specs=[hbm] * 4 + [pl.BlockSpec(memory_space=pltpu.SMEM)],
        out_specs=[vmem] * 4,
        scratch_shapes=[
            pltpu.VMEM((ROWS * COLS * 2, 128), f32),
            pltpu.VMEM((ROWS * COLS * 2, 128), f32),
            pltpu.VMEM((ROWS * COLS * 2, 128), f32),
            pltpu.VMEM((ROWS, COLS, 128), jnp.int32),
            pltpu.VMEM((11, ROWS, 8, 128), f32),
            pltpu.VMEM((2, BLOCKS, 8, 128), f32),
            pltpu.VMEM((3, BLOCKS, 8, 128), f32),
            pltpu.VMEM((8, 2, 8, 128), f32),
            pltpu.VMEM((8, 3, 8, 128), f32),
            pltpu.VMEM((ITERS, 8, 2, 8, 128), f32),
            pltpu.VMEM((ITERS, 8, 3, 8, 128), f32),
            pltpu.VMEM((32 * FS, 128), f32),
            pltpu.VMEM((32 * FS, 128), f32),
            pltpu.VMEM((16, 128, 128), bf16),
            pltpu.VMEM((4, 128, 128), bf16),
            pltpu.VMEM((162, 128, 256), f32),
            pltpu.VMEM((ROWS, COLS, 8, 128), f32),
            pltpu.VMEM((ROWS, COLS, 32, 128), f32),
            pltpu.VMEM((BLOCKS, 8, 32, 128), bf16),
            pltpu.VMEM((16 * FS, 128), f32),
            pltpu.VMEM((9, 16, 128), f32),
            pltpu.VMEM((9, 16, 128), f32),
            pltpu.VMEM((ITERS, 2, 1, 128), f32),
            pltpu.VMEM((ITERS, n1, 1, 128), f32),
            pltpu.VMEM((ITERS, n2, 1, 128), f32),
            dma((4,)),
            dma((ITERS, 8)), dma((ITERS, 8)), dma((ITERS, 8)), dma((ITERS, 8)),
            dma((ITERS, n1)), dma((ITERS, n1)), dma((ITERS, n2)), dma((ITERS, n2)),
        ],
        compiler_params=pltpu.CompilerParams(
            collective_id=0, has_side_effects=True, vmem_limit_bytes=60 * 1024 * 1024
        ),
    )(flat(position), flat(velocity), flat(other_accel), phase_ids, counts)
    return unflat(new_pos), unflat(new_vel), pressure, monitor


def solution(mesh):
    gx = ("x", "zl")
    gy = ("zh", "y", "core")
    torus = Mesh(mesh.devices.reshape(4, 2, 2, 4, 2), SPLIT)
    wide = P(None, gx, gy, None)
    return jax.shard_map(
        local, mesh=torus, in_specs=(wide, wide, wide, P(gx, gy, None), P(gx, gy)),
        out_specs=(wide, wide, P(gx, gy, None), P()), check_vma=False,
    )
```

```python
import jax
import jax.numpy as jnp
from jax import lax
from jax.experimental import pallas as pl
from jax.experimental.pallas import tpu as pltpu
from jax.sharding import Mesh
from jax.sharding import PartitionSpec as P

ITERS = 4
TIME_STEP = 0.05
KERNEL_NORM = 4.0 / (3.141592653589793 * 64.0)
REST_LIGHT = 1.2
REST_HEAVY = 1.5
STIFF_LIGHT = 100.0
STIFF_HEAVY = 200.0
MASS_LIGHT = 1.0
MASS_HEAVY = 1.5
FAR = float(2**30)
NEG = -1e30
MESH = pl.DeviceIdType.MESH
SPLIT = ("x", "zl", "zh", "y", "core")
ROWS = 6
COLS = 6
TOP, BOTTOM, LEFT, RIGHT, CORNERS = 0, 7, 8, 9, 10
EDGES = (TOP, BOTTOM, LEFT, RIGHT)
BLOCKS = 11
FS = BLOCKS * 8
DIRS = ((-1, 0), (1, 0), (0, -1), (0, 1), (-1, -1), (-1, 1), (1, -1), (1, 1))
OWN_TILES = (
    (0, 1, 0, 1, 0), (0, 1, 1, 2, 0),
    (2, 3, 1, 2, 0), (2, 3, 2, 3, 0), (2, 3, 3, 4, 1),
    (4, 5, 3, 4, 1), (4, 5, 4, 5, 1),
    (1, 4, 0, 5, 2),
)
GROUP_START = (0, 2)
UNROLL = 4
OUT_VELOCITY = ROWS * COLS * 2
OUT_PRESSURE = 2 * OUT_VELOCITY
OUT_MONITOR = OUT_PRESSURE + ROWS * 8
OUT_ROWS = OUT_MONITOR + 8

f32 = jnp.float32
bf16 = jnp.bfloat16


def rnd(v):
    return v.astype(bf16).astype(f32)


def split3(v):
    h = rnd(v)
    r = v - h
    m = rnd(r)
    return h, m, rnd(r - m)


def feature_rows(x, y):
    xs = split3(x)
    ys = split3(y)
    rs = split3(x * x + y * y)
    one = jnp.ones_like(x)
    zero = jnp.zeros_like(x)
    h, m, l = 0, 1, 2
    jrow = (
        [xs[q] for q in (h, h, m, m, l, h)] + [ys[q] for q in (h, h, m, m, l, h)]
        + list(rs) + [one, one, one] + list(xs) + list(ys) + [one] * 7 + [zero]
    )
    irow = (
        [2.0 * xs[q] for q in (h, m, h, m, h, l)] + [2.0 * ys[q] for q in (h, m, h, m, h, l)]
        + [-one] * 3 + [-q for q in rs] + [zero] * 6 + list(xs) + list(ys) + [zero, zero]
    )
    return jrow, irow


def kernel(
    pos_ref, vel_ref, oa_ref, phase_ref, counts_ref,
    out_ref,
    inp, inv, ino, inph, st, xp, bp, tp, stage, tstage, cstage, ctstage, rb, trb, crb, ctrb,
    fb, ib, lt, gh, wb, da, fa, tf, mb, al, be, rl, ar0, ar1, ar2,
    ins, hs, hr, ts, tr, a1s, a1r, a2s, a2r,
):
    index = {name: lax.axis_index(name) for name in SPLIT}
    size = {name: lax.axis_size(name) for name in SPLIT}
    gx = index["x"] * size["zl"] + index["zl"]
    gy = (index["zh"] * size["y"] + index["y"]) * size["core"] + index["core"]
    nx = size["x"] * size["zl"]
    ny = size["zh"] * size["y"] * size["core"]

    def around(dx, dy):
        px = lax.rem(gx + dx + nx, nx)
        py = lax.rem(gy + dy + ny, ny)
        return (
            px // size["zl"], lax.rem(px, size["zl"]), py // (size["y"] * size["core"]),
            lax.rem(py // size["core"], size["y"]), lax.rem(py, size["core"]),
        )

    def peers(names):
        steps = [()]
        for name in SPLIT:
            count = size[name] if name in names else 1
            steps = [s + (q,) for s in steps for q in range(count)]
        return [
            tuple(lax.rem(index[name] + q, size[name]) for name, q in zip(SPLIT, s))
            for s in steps if any(s)
        ]

    neighbours = [around(dx, dy) for dx, dy in DIRS]
    first_peers = peers(("y", "core"))
    second_peers = peers(("x", "zl", "zh"))
    barrier = pltpu.get_barrier_semaphore()
    for partner in neighbours + first_peers + second_peers:
        pl.semaphore_signal(barrier, inc=1, device_id=partner, device_id_type=MESH)

    loads = [
        pltpu.make_async_copy(src, dst, ins.at[q])
        for q, (src, dst) in enumerate(
            ((pos_ref, inp), (vel_ref, inv), (oa_ref, ino), (phase_ref, inph))
        )
    ]
    for load in loads:
        load.start()

    st[...] = jnp.zeros_like(st)
    da[...] = jnp.zeros_like(da)
    mb[...] = jnp.zeros_like(mb)
    xp[...] = jnp.full_like(xp, FAR)
    tp[...] = jnp.zeros_like(tp)
    fb[...] = jnp.zeros_like(fb)
    bp[...] = jnp.zeros_like(bp)
    rl[...] = jnp.zeros_like(rl)
    for buf in (stage, tstage, cstage, ctstage):
        buf[...] = jnp.zeros_like(buf)
    k = lax.broadcasted_iota(jnp.int32, (16, 128), 0)
    for ox in (-1, 0, 1):
        for oy in (-1, 0, 1):
            o = (ox + 1) * 3 + oy + 1
            al[o] = jnp.where(
                k < 2, 1.0,
                jnp.where((k >= 8) & (k < 11), 2.0 * ox, jnp.where((k >= 11) & (k < 14), 2.0 * oy, 0.0)),
            )
            be[o] = jnp.where(
                (k >= 2) & (k < 5), -2.0 * ox,
                jnp.where(
                    (k >= 5) & (k < 8), -2.0 * oy, jnp.where(k == 14, 1.0 - ox * ox - oy * oy, 0.0)
                ),
            )
    lane = lax.broadcasted_iota(jnp.int32, (1, 128), 1)
    sub = lax.broadcasted_iota(jnp.int32, (8, 128), 0)
    sub_f = sub.astype(f32)
    row_cols = jnp.where(sub == 7, -1.0, sub_f) - 2.5
    for load in loads:
        load.wait()
    for a in range(ROWS):
        for f in range(2):
            for s in range(COLS):
                at = a * 12 + s * 2 + f
                st[f, a, s : s + 1, :] = inp[at : at + 1, :]
                st[2 + f, a, s : s + 1, :] = inv[at : at + 1, :]
                st[13 + f, a, s : s + 1, :] = ino[at : at + 1, :]
        for s in range(COLS):
            st[4, a, s : s + 1, :] = (lane < counts_ref[a, s]).astype(f32)
        st[5, a, 0:COLS, :] = (inph[a] == 1).astype(f32)

    def halo_copies(src, staged, corners, dst, cdst, send, recv):
        edges = []
        diagonals = []
        for d in range(8):
            if d < 4:
                source = src.at[:, (1, ROWS)[d]] if d < 2 else staged.at[d - 2]
                target = dst.at[d]
            else:
                source, target = corners.at[d - 4], cdst.at[d - 4]
            (edges if d < 4 else diagonals).append(
                pltpu.make_async_remote_copy(
                    src_ref=source, dst_ref=target, send_sem=send.at[d], recv_sem=recv.at[d],
                    device_id=neighbours[d], device_id_type=MESH,
                )
            )
        return diagonals, edges

    def pack(src, staged, corners, fields):
        for f in range(fields):
            corners[0, f : f + 1, :] = src[f, 1, 0:1, :]
            corners[1, f : f + 1, :] = src[f, 1, COLS - 1 : COLS, :]
            corners[2, f : f + 1, :] = src[f, ROWS, 0:1, :]
            corners[3, f : f + 1, :] = src[f, ROWS, COLS - 1 : COLS, :]
            for a in range(ROWS):
                staged[0, f, a : a + 1, :] = src[f, a + 1, 0:1, :]
                staged[1, f, a : a + 1, :] = src[f, a + 1, COLS - 1 : COLS, :]

    PLACE = (3, 2, 1, 0)

    def put(buf, rows, base):
        for q, row in enumerate(rows):
            buf[pl.ds(q * FS + base, 8), :] = row

    def cell(buf, c):
        return buf[pl.ds(c, 32, stride=FS), :]

    def turned(cells):
        return jnp.concatenate([cell(fb, c) for c in cells], axis=0).T.astype(bf16)

    def centre(a, col, o):
        base = cell(ib, (a + 1) * 8 + col)
        return jnp.concatenate([base[0:16], base[16:32] * al[o] + be[o]], axis=0).astype(bf16)

    def at_block(part, block, blocks):
        pieces = []
        if block > 0:
            pieces.append(jnp.zeros((32 * block, 128), bf16))
        pieces.append(part)
        if block < blocks - 1:
            pieces.append(jnp.zeros((32 * (blocks - 1 - block), 128), bf16))
        return jnp.concatenate(pieces, axis=0) if len(pieces) > 1 else part

    def overlap(left, right, slot, sums, cols):
        w = jnp.maximum(jnp.dot(left, right, preferred_element_type=f32), 0.0)
        w2 = w * w
        wb[slot] = w2
        part = jnp.sum((w2 * w).reshape(16, 8, 256), axis=0)
        for e in range(2):
            half = part[:, 128 * e : 128 * e + 128]
            sums[cols[e]] = half if sums[cols[e]] is None else sums[cols[e]] + half

    def own_tiles(a, ox3, lrow, slot, sums):
        for q, (ca, cb, ja, jb, group) in enumerate(OWN_TILES):
            pa = centre(a, ca, ox3 + (ja - ca + 1))
            pb = centre(a, cb, ox3 + (jb - cb + 1))
            if group == 2:
                left = jnp.concatenate([lrow[0], lrow[1]], axis=1)
                right = jnp.concatenate([at_block(pa, ja, 8), at_block(pb, jb - 2 + 4, 8)], axis=1)
            else:
                left = lrow[group]
                right = jnp.concatenate(
                    [at_block(pa, ja - GROUP_START[group], 4), at_block(pb, jb - GROUP_START[group], 4)],
                    axis=1,
                )
            overlap(left, right, slot + q, sums, (ca, cb))

    def edge_tile(a, ox3, r, slot, sums):
        pa = centre(a, 0, ox3)
        pb = centre(a, COLS - 1, ox3 + 2)
        group, odd = divmod(r, 2) if 0 <= r < ROWS else (3, int(r >= ROWS))
        right = jnp.concatenate([at_block(pa, 2 * odd, 4), at_block(pb, 2 * odd + 1, 4)], axis=1)
        overlap(gh[group], right, slot + 8, sums, (0, COLS - 1))

    def pull(w2, left, sums, cols):
        hi = w2.astype(bf16)
        lo = (w2 - hi.astype(f32)).astype(bf16)
        both = jnp.concatenate([left, left], axis=1)
        total = jnp.dot(both, jnp.concatenate([hi, lo], axis=0), preferred_element_type=f32)
        for e in range(2):
            part = total[32 * e : 32 * e + 32, 128 * e : 128 * e + 128]
            sums[cols[e]] = part if sums[cols[e]] is None else sums[cols[e]] + part

    def own_pulls(r, slot, sums):
        for q, (ca, cb, ja, jb, group) in enumerate(OWN_TILES):
            left = jnp.concatenate([tf[r, ja], tf[r, jb]], axis=0)
            pull(wb[slot + q], left, sums, (ca, cb))

    def side_cells(r):
        if r < 0:
            return (CORNERS, 0), (CORNERS, 1)
        if r >= ROWS:
            return (CORNERS, 2), (CORNERS, 3)
        return (LEFT, r), (RIGHT, r)

    def moment_rows(block, px, py):
        rows = [None] * 32
        for q in range(4):
            field = None if q == 0 else tp[q - 1, block]
            for e, p in enumerate((px, py)):
                pieces = split3(p if field is None else p * field)
                for level in range(3):
                    rows[level * 8 + 2 * q + e] = pieces[level]
            if field is None:
                rows[24], rows[28] = jnp.ones_like(px), jnp.zeros_like(px)
            else:
                rows[24 + q] = rnd(field)
                rows[28 + q] = rnd(field - rows[24 + q])
        return rows

    pl.semaphore_wait(barrier, len(neighbours) + len(first_peers) + len(second_peers))

    position_copies = halo_copies(bp, stage, cstage, rb, crb, hs, hr)
    term_copies = halo_copies(tp, tstage, ctstage, trb, ctrb, ts, tr)

    def start(pair):
        for copy in pair[0] + pair[1]:
            copy.start()

    def coefficients():
        alive = st[4] > 0.5
        for f in range(2):
            free = st[f] + TIME_STEP * (st[2 + f] + TIME_STEP * st[13 + f]) - 0.5
            step = TIME_STEP * TIME_STEP
            bp[3 * f, 1 : ROWS + 1] = jnp.where(alive, free + step * st[7 + 3 * f], FAR)
            bp[3 * f + 1, 1 : ROWS + 1] = step * st[8 + 3 * f]
            bp[3 * f + 2, 1 : ROWS + 1] = step * st[9 + 3 * f]
        pack(bp, stage, cstage, 6)
        start(position_copies)

    def side_tiles(which):
        done = []
        for t in range(18):
            a, ox = t // 3, t % 3 - 1
            r = a + ox
            outside = r < 0 or r >= ROWS
            if which == "edges" and outside:
                done.append((t, a, ox, r, True))
            if outside == (which == "corners"):
                done.append((t, a, ox, r, False))
        return done

    def add_up(buf, a, sums):
        for s in range(COLS):
            if sums[s] is not None:
                buf[a, s] += sums[s]

    def densities(it):
        relax0, relax1 = rl[0], rl[1]
        for f in range(2):
            for r in range(ROWS):
                xp[f, r + 1] = bp[3 * f, r + 1] + relax0 * bp[3 * f + 1, r + 1] + relax1 * bp[3 * f + 2, r + 1]
        for r in range(ROWS):
            jrow, irow = feature_rows(xp[0, r + 1], xp[1, r + 1])
            put(fb, jrow, (r + 1) * 8)
            put(ib, irow, (r + 1) * 8)
        for r in range(ROWS):
            for g in range(2):
                lt[(r + 1) * 2 + g] = turned([(r + 1) * 8 + GROUP_START[g] + s for s in range(4)])
        da[...] = jnp.zeros_like(da)

        def density(t, c):
            a = t // 3
            step = lax.rem(t, 3)
            r = a + step
            sums = [None] * COLS
            own_tiles(a, step * 3, (lt[r * 2], lt[r * 2 + 1]), t * 9, sums)
            for s in range(COLS):
                da[a, s] += sums[s]
            return c

        lax.fori_loop(1, 17, density, 0, unroll=UNROLL)

        diagonals, edges = position_copies
        for copy in edges:
            copy.wait()
        for d, block in enumerate((BOTTOM, TOP, RIGHT, LEFT)):
            for f in range(2):
                xp[f, block] = rb[d, 3 * f] + relax0 * rb[d, 3 * f + 1] + relax1 * rb[d, 3 * f + 2]
        for block in EDGES:
            jrow, _ = feature_rows(xp[0, block], xp[1, block])
            put(fb, jrow, block * 8)
        for block in (TOP, BOTTOM):
            for g in range(2):
                lt[block * 2 + g] = turned([block * 8 + GROUP_START[g] + s for s in range(4)])
        for q in range(3):
            gh[q] = turned([b * 8 + s for r in (2 * q, 2 * q + 1) for b, s in side_cells(r)])
        for t, a, ox, r, row in side_tiles("edges"):
            sums = [None] * COLS
            if row:
                own_tiles(a, (ox + 1) * 3, (lt[(r + 1) * 2], lt[(r + 1) * 2 + 1]), t * 9, sums)
            else:
                edge_tile(a, (ox + 1) * 3, r, t * 9, sums)
            add_up(da, a, sums)

        for copy in diagonals:
            copy.wait()
        for d in range(4):
            for f in range(2):
                xp[f, CORNERS, PLACE[d] : PLACE[d] + 1, :] = (
                    crb[d, 3 * f : 3 * f + 1, :] + relax0[0:1] * crb[d, 3 * f + 1 : 3 * f + 2, :]
                    + relax1[0:1] * crb[d, 3 * f + 2 : 3 * f + 3, :]
                )
        jrow, _ = feature_rows(xp[0, CORNERS], xp[1, CORNERS])
        put(fb, jrow, CORNERS * 8)
        gh[3] = turned([CORNERS * 8 + q for q in range(4)])
        for t, a, ox, r, row in side_tiles("corners"):
            sums = [None] * COLS
            edge_tile(a, (ox + 1) * 3, r, t * 9, sums)
            add_up(da, a, sums)

    def bounds_copies(now, src_slot, dst, send, recv, targets):
        return [
            pltpu.make_async_remote_copy(
                src_ref=ar0.at[now, src_slot], dst_ref=dst.at[now, d],
                send_sem=send.at[now, d], recv_sem=recv.at[now, d],
                device_id=target, device_id_type=MESH,
            )
            for d, target in enumerate(targets)
        ]

    def forces(it):
        now = lax.rem(it, 2)
        alive = st[4] > 0.5
        hot = st[5] > 0.5
        rows = []
        for a in range(ROWS):
            cells = [jnp.sum(da[a, s], axis=0, keepdims=True) for s in range(COLS)]
            rows.append(jnp.concatenate(cells + [jnp.zeros((2, 128), f32)], axis=0))
        density_now = KERNEL_NORM * jnp.stack(rows)
        ratio = density_now / jnp.where(hot, REST_HEAVY, REST_LIGHT)
        lit = alive & jnp.logical_not(hot)
        hvy = alive & hot
        peaks = (
            jnp.where(lit, ratio, NEG), jnp.where(hvy, ratio, NEG),
            jnp.where(lit, -ratio, NEG), jnp.where(hvy, -ratio, NEG),
        )
        vec = jnp.full((1, 128), NEG, f32)
        for q in range(4):
            top = jnp.max(jnp.max(peaks[q], axis=0), axis=0, keepdims=True)
            top = jnp.max(top, axis=1, keepdims=True)
            vec = jnp.where(lane == q, top, vec)
        ar0[now, 0] = vec
        first = bounds_copies(now, 0, ar1, a1s, a1r, first_peers)

        safe = jnp.where(alive, density_now, 1.0)
        inverse = 1.0 / (safe * safe)
        excess = jnp.where(hot, STIFF_HEAVY, STIFF_LIGHT) * (ratio - 1.0)
        t0 = jnp.where(alive, st[6] * inverse, 0.0)
        u = excess * inverse
        u0 = jnp.where(lit, u, 0.0)
        u1 = jnp.where(hvy, u, 0.0)
        tp[0, 1 : ROWS + 1] = t0
        tp[1, 1 : ROWS + 1] = u0
        tp[2, 1 : ROWS + 1] = u1
        pack(tp, tstage, ctstage, 3)
        for copy in first:
            copy.start()
        start(term_copies)

        for a in range(ROWS):
            put(fb, moment_rows(a + 1, xp[0, a + 1] + (a - 2.5), xp[1, a + 1] + row_cols), (a + 1) * 8)
        for a in range(ROWS):
            for s in range(COLS):
                tf[a + 1, s] = cell(fb, (a + 1) * 8 + s).astype(bf16)
        fa[...] = jnp.zeros_like(fa)

        def force(t, c):
            a = t // 3
            step = lax.rem(t, 3)
            sums = [None] * COLS
            own_pulls(a + step, t * 9, sums)
            for s in range(COLS):
                fa[a, s] += sums[s]
            return c

        lax.fori_loop(1, 17, force, 0, unroll=UNROLL)

        for copy in first:
            copy.wait()
        best = vec
        for d in range(len(first_peers)):
            best = jnp.maximum(best, ar1[now, d])
        ar0[now, 1] = best
        second = bounds_copies(now, 1, ar2, a2s, a2r, second_peers)
        for copy in second:
            copy.start()

        diagonals, edges = term_copies
        for copy in edges:
            copy.wait()
        for d, block in enumerate((BOTTOM, TOP, RIGHT, LEFT)):
            for f in range(3):
                tp[f, block] = trb[d, f]
        edge_x = {TOP: -3.5, BOTTOM: 3.5, LEFT: sub_f - 2.5, RIGHT: sub_f - 2.5}
        edge_y = {TOP: row_cols, BOTTOM: row_cols, LEFT: -3.5, RIGHT: 3.5}
        for block in EDGES:
            put(fb, moment_rows(block, xp[0, block] + edge_x[block], xp[1, block] + edge_y[block]), block * 8)
        for block in EDGES:
            for s in range(ROWS):
                tf[block, s] = cell(fb, block * 8 + s).astype(bf16)

        def side_pull(t, r, sums):
            (lb, ls), (ub, us) = side_cells(r)
            pull(wb[t * 9 + 8], jnp.concatenate([tf[lb, ls], tf[ub, us]], axis=0), sums, (0, COLS - 1))

        for t, a, ox, r, row in side_tiles("edges"):
            sums = [None] * COLS
            if row:
                own_pulls(r + 1, t * 9, sums)
            else:
                side_pull(t, r, sums)
            add_up(fa, a, sums)

        for copy in diagonals:
            copy.wait()
        for d in range(4):
            for f in range(3):
                tp[f, CORNERS, PLACE[d] : PLACE[d] + 1, :] = ctrb[d, f : f + 1, :]
        corner_x = jnp.where(sub < 2, -3.5, 3.5)
        corner_y = jnp.where(lax.rem(sub, 2) == 0, -3.5, 3.5)
        put(fb, moment_rows(CORNERS, xp[0, CORNERS] + corner_x, xp[1, CORNERS] + corner_y), CORNERS * 8)
        for s in range(4):
            tf[CORNERS, s] = cell(fb, CORNERS * 8 + s).astype(bf16)
        for t, a, ox, r, row in side_tiles("corners"):
            sums = [None] * COLS
            side_pull(t, r, sums)
            add_up(fa, a, sums)

        for a in range(ROWS):
            for s in range(COLS):
                part = fa[a, s]
                row = a * 8 + s
                mb[pl.ds(row, 8, stride=FS), :] = part[0:8] + part[8:16] + part[16:24]
                mb[pl.ds(8 * FS + row, 8, stride=FS), :] = part[24:32]

        for a in range(ROWS):
            def mom(q):
                return mb[q * FS + a * 8 : q * FS + a * 8 + 8, :]

            s1 = mom(8) + mom(12)
            factor = jnp.where(
                alive[a], 6.0 * KERNEL_NORM / jnp.where(hot[a], MASS_HEAVY, MASS_LIGHT), 0.0
            )
            for f in range(2):
                p = xp[f, a + 1] + (a - 2.5 if f == 0 else row_cols)
                arm = p * s1 - mom(f)
                for q, term in enumerate((t0[a], u0[a], u1[a])):
                    push = term * arm + p * (mom(9 + q) + mom(13 + q)) - mom(2 + 2 * q + f)
                    st[7 + 3 * f + q, a] = jnp.where(alive[a], factor * push, 0.0)

        @pl.when(it < ITERS - 1)
        def _():
            coefficients()

        for copy in second:
            copy.wait()
        for d in range(len(second_peers)):
            best = jnp.maximum(best, ar2[now, d])
        out_ref[pl.ds(OUT_MONITOR + it, 1), :] = jnp.where(lane < 2, best, -best)
        relax0 = jnp.broadcast_to(1.0 / (1.0 + best[:, 0:1] + best[:, 2:3]), (8, 128))
        relax1 = jnp.broadcast_to(1.0 / (1.0 + best[:, 1:2] + best[:, 3:4]), (8, 128))
        rl[0] = relax0
        rl[1] = relax1
        for a in range(ROWS):
            relax = jnp.where(hot[a], relax1, relax0)
            st[6, a] = jnp.where(alive[a], st[6, a] + relax * excess[a], 0.0)

    coefficients()

    def whole(it, carry):
        densities(it)
        forces(it)
        return carry

    lax.fori_loop(0, ITERS, whole, 0)

    for a in range(ROWS):
        live = st[4, a]
        for f in range(2):
            accel = st[7 + 3 * f, a] + rl[0] * st[8 + 3 * f, a] + rl[1] * st[9 + 3 * f, a]
            v = live * (st[2 + f, a] + TIME_STEP * (st[13 + f, a] + accel))
            p = live * (st[f, a] + TIME_STEP * v)
            out_ref[pl.ds(a * 12 + f, COLS, stride=2), :] = p[0:COLS]
            out_ref[pl.ds(OUT_VELOCITY + a * 12 + f, COLS, stride=2), :] = v[0:COLS]
        out_ref[OUT_PRESSURE + a * 8 : OUT_PRESSURE + a * 8 + 8, :] = st[6, a]


def spread(in_ref, npos_ref, nvel_ref, pres_ref, mon_ref):
    npos_ref[...] = in_ref[0:OUT_VELOCITY, :]
    nvel_ref[...] = in_ref[OUT_VELOCITY:OUT_PRESSURE, :]
    for a in range(ROWS):
        pres_ref[a] = in_ref[OUT_PRESSURE + a * 8 : OUT_PRESSURE + a * 8 + COLS, :]
    mon_ref[...] = in_ref[OUT_MONITOR : OUT_MONITOR + ITERS, 0:4]


def flat(value):
    return value.transpose(1, 2, 0, 3).reshape(ROWS * COLS * 2, 128)


def unflat(value):
    return value.reshape(ROWS, COLS, 2, 128).transpose(2, 0, 1, 3)


def local(position, velocity, other_accel, phase_ids, counts):
    vmem = pl.BlockSpec(memory_space=pltpu.VMEM)
    hbm = pl.BlockSpec(memory_space=pl.ANY)
    dma = pltpu.SemaphoreType.DMA
    n1 = lax.axis_size("y") * lax.axis_size("core") - 1
    n2 = lax.axis_size("x") * lax.axis_size("zl") * lax.axis_size("zh") - 1
    packed = pl.pallas_call(
        kernel,
        out_shape=jax.ShapeDtypeStruct((OUT_ROWS, 128), f32),
        in_specs=[hbm] * 4 + [pl.BlockSpec(memory_space=pltpu.SMEM)],
        out_specs=vmem,
        scratch_shapes=[
            pltpu.VMEM((ROWS * COLS * 2, 128), f32),
            pltpu.VMEM((ROWS * COLS * 2, 128), f32),
            pltpu.VMEM((ROWS * COLS * 2, 128), f32),
            pltpu.VMEM((ROWS, COLS, 128), jnp.int32),
            pltpu.VMEM((15, ROWS, 8, 128), f32),
            pltpu.VMEM((2, BLOCKS, 8, 128), f32),
            pltpu.VMEM((6, BLOCKS, 8, 128), f32),
            pltpu.VMEM((3, BLOCKS, 8, 128), f32),
            pltpu.VMEM((2, 6, 8, 128), f32),
            pltpu.VMEM((2, 3, 8, 128), f32),
            pltpu.VMEM((4, 8, 128), f32),
            pltpu.VMEM((4, 8, 128), f32),
            pltpu.VMEM((4, 6, 8, 128), f32),
            pltpu.VMEM((4, 3, 8, 128), f32),
            pltpu.VMEM((4, 8, 128), f32),
            pltpu.VMEM((4, 8, 128), f32),
            pltpu.VMEM((32 * FS, 128), f32),
            pltpu.VMEM((32 * FS, 128), f32),
            pltpu.VMEM((16, 128, 128), bf16),
            pltpu.VMEM((4, 128, 128), bf16),
            pltpu.VMEM((162, 128, 256), f32),
            pltpu.VMEM((ROWS, COLS, 8, 128), f32),
            pltpu.VMEM((ROWS, COLS, 32, 128), f32),
            pltpu.VMEM((BLOCKS, 8, 32, 128), bf16),
            pltpu.VMEM((16 * FS, 128), f32),
            pltpu.VMEM((9, 16, 128), f32),
            pltpu.VMEM((9, 16, 128), f32),
            pltpu.VMEM((2, 8, 128), f32),
            pltpu.VMEM((2, 2, 1, 128), f32),
            pltpu.VMEM((2, n1, 1, 128), f32),
            pltpu.VMEM((2, n2, 1, 128), f32),
            dma((4,)), dma((8,)), dma((8,)), dma((8,)), dma((8,)),
            dma((2, n1)), dma((2, n1)), dma((2, n2)), dma((2, n2)),
        ],
        compiler_params=pltpu.CompilerParams(
            collective_id=0, has_side_effects=True, vmem_limit_bytes=36 * 1024 * 1024
        ),
    )(flat(position), flat(velocity), flat(other_accel), phase_ids, counts)
    new_pos, new_vel, pressure, monitor = pl.pallas_call(
        spread,
        out_shape=(
            jax.ShapeDtypeStruct((ROWS * COLS * 2, 128), f32),
            jax.ShapeDtypeStruct((ROWS * COLS * 2, 128), f32),
            jax.ShapeDtypeStruct((ROWS, COLS, 128), f32),
            jax.ShapeDtypeStruct((ITERS, 4), f32),
        ),
        in_specs=[vmem],
        out_specs=[vmem] * 4,
        compiler_params=pltpu.CompilerParams(vmem_limit_bytes=4 * 1024 * 1024),
    )(packed)
    return unflat(new_pos), unflat(new_vel), pressure, monitor


def solution(mesh):
    gx = ("x", "zl")
    gy = ("zh", "y", "core")
    torus = Mesh(mesh.devices.reshape(4, 2, 2, 4, 2), SPLIT)
    wide = P(None, gx, gy, None)
    return jax.shard_map(
        local, mesh=torus, in_specs=(wide, wide, wide, P(gx, gy, None), P(gx, gy)),
        out_specs=(wide, wide, P(gx, gy, None), P()), check_vma=False,
    )
```

```python
import jax
import jax.numpy as jnp
from jax import lax
from jax.experimental import pallas as pl
from jax.experimental.pallas import tpu as pltpu
from jax.sharding import Mesh
from jax.sharding import PartitionSpec as P

ITERS = 4
TIME_STEP = 0.05
KERNEL_NORM = 4.0 / (3.141592653589793 * 64.0)
REST_LIGHT = 1.2
REST_HEAVY = 1.5
STIFF_LIGHT = 100.0
STIFF_HEAVY = 200.0
MASS_LIGHT = 1.0
MASS_HEAVY = 1.5
FAR = float(2**30)
NEG = -1e30
MESH = pl.DeviceIdType.MESH
SPLIT = ("x", "zl", "zh", "y", "core")
ROWS = 6
COLS = 6
TOP, BOTTOM, LEFT, RIGHT, CORNERS = 0, 7, 8, 9, 10
EDGES = (TOP, BOTTOM, LEFT, RIGHT)
BLOCKS = 11
FS = BLOCKS * 8
DIRS = ((-1, 0), (1, 0), (0, -1), (0, 1), (-1, -1), (-1, 1), (1, -1), (1, 1))
OWN_TILES = (
    (0, 1, 0, 1, 0), (0, 1, 1, 2, 0),
    (2, 3, 1, 2, 0), (2, 3, 2, 3, 0), (2, 3, 3, 4, 1),
    (4, 5, 3, 4, 1), (4, 5, 4, 5, 1),
    (1, 4, 0, 5, 2),
)
GROUP_START = (0, 2)
UNROLL = 8
OUT_VELOCITY = ROWS * COLS * 2
OUT_PRESSURE = 2 * OUT_VELOCITY
OUT_MONITOR = OUT_PRESSURE + ROWS * 8
OUT_ROWS = OUT_MONITOR + 8

f32 = jnp.float32
bf16 = jnp.bfloat16


def rnd(v):
    return v.astype(bf16).astype(f32)


def split3(v):
    h = rnd(v)
    r = v - h
    m = rnd(r)
    return h, m, rnd(r - m)


def feature_rows(x, y):
    xs = split3(x)
    ys = split3(y)
    rs = split3(x * x + y * y)
    one = jnp.ones_like(x)
    zero = jnp.zeros_like(x)
    h, m, l = 0, 1, 2
    jrow = (
        [xs[q] for q in (h, h, m, m, l, h)] + [ys[q] for q in (h, h, m, m, l, h)]
        + list(rs) + [one, one, one] + list(xs) + list(ys) + [one] * 7 + [zero]
    )
    irow = (
        [2.0 * xs[q] for q in (h, m, h, m, h, l)] + [2.0 * ys[q] for q in (h, m, h, m, h, l)]
        + [-one] * 3 + [-q for q in rs] + [zero] * 6 + list(xs) + list(ys) + [zero, zero]
    )
    return jrow, irow


def kernel(
    pos_ref, vel_ref, oa_ref, phase_ref, counts_ref,
    out_ref,
    inp, inv, ino, inph, st, xp, bp, tp, stage, tstage, cstage, ctstage, rb, trb, crb, ctrb,
    fb, ib, lt, gh, wb, da, fa, tf, mb, al, be, rl, ar0, ar1, ar2,
    ins, hs, hr, ts, tr, a1s, a1r, a2s, a2r,
):
    index = {name: lax.axis_index(name) for name in SPLIT}
    size = {name: lax.axis_size(name) for name in SPLIT}
    gx = index["x"] * size["zl"] + index["zl"]
    gy = (index["zh"] * size["y"] + index["y"]) * size["core"] + index["core"]
    nx = size["x"] * size["zl"]
    ny = size["zh"] * size["y"] * size["core"]

    def around(dx, dy):
        px = lax.rem(gx + dx + nx, nx)
        py = lax.rem(gy + dy + ny, ny)
        return (
            px // size["zl"], lax.rem(px, size["zl"]), py // (size["y"] * size["core"]),
            lax.rem(py // size["core"], size["y"]), lax.rem(py, size["core"]),
        )

    def peers(names):
        steps = [()]
        for name in SPLIT:
            count = size[name] if name in names else 1
            steps = [s + (q,) for s in steps for q in range(count)]
        return [
            tuple(lax.rem(index[name] + q, size[name]) for name, q in zip(SPLIT, s))
            for s in steps if any(s)
        ]

    neighbours = [around(dx, dy) for dx, dy in DIRS]
    first_peers = peers(("y", "core"))
    second_peers = peers(("x", "zl", "zh"))
    barrier = pltpu.get_barrier_semaphore()
    for partner in neighbours + first_peers + second_peers:
        pl.semaphore_signal(barrier, inc=1, device_id=partner, device_id_type=MESH)

    loads = [
        pltpu.make_async_copy(src, dst, ins.at[q])
        for q, (src, dst) in enumerate(
            ((pos_ref, inp), (vel_ref, inv), (oa_ref, ino), (phase_ref, inph))
        )
    ]
    for load in loads:
        load.start()

    st[...] = jnp.zeros_like(st)
    da[...] = jnp.zeros_like(da)
    mb[...] = jnp.zeros_like(mb)
    xp[...] = jnp.full_like(xp, FAR)
    tp[...] = jnp.zeros_like(tp)
    fb[...] = jnp.zeros_like(fb)
    bp[...] = jnp.zeros_like(bp)
    rl[...] = jnp.zeros_like(rl)
    for buf in (stage, tstage, cstage, ctstage):
        buf[...] = jnp.zeros_like(buf)
    k = lax.broadcasted_iota(jnp.int32, (16, 128), 0)
    for ox in (-1, 0, 1):
        for oy in (-1, 0, 1):
            o = (ox + 1) * 3 + oy + 1
            al[o] = jnp.where(
                k < 2, 1.0,
                jnp.where((k >= 8) & (k < 11), 2.0 * ox, jnp.where((k >= 11) & (k < 14), 2.0 * oy, 0.0)),
            )
            be[o] = jnp.where(
                (k >= 2) & (k < 5), -2.0 * ox,
                jnp.where(
                    (k >= 5) & (k < 8), -2.0 * oy, jnp.where(k == 14, 1.0 - ox * ox - oy * oy, 0.0)
                ),
            )
    lane = lax.broadcasted_iota(jnp.int32, (1, 128), 1)
    sub = lax.broadcasted_iota(jnp.int32, (8, 128), 0)
    sub_f = sub.astype(f32)
    row_cols = jnp.where(sub == 7, -1.0, sub_f) - 2.5
    for load in loads:
        load.wait()
    for a in range(ROWS):
        for f in range(2):
            for s in range(COLS):
                at = a * 12 + s * 2 + f
                st[f, a, s : s + 1, :] = inp[at : at + 1, :]
                st[2 + f, a, s : s + 1, :] = inv[at : at + 1, :]
                st[13 + f, a, s : s + 1, :] = ino[at : at + 1, :]
        for s in range(COLS):
            st[4, a, s : s + 1, :] = (lane < counts_ref[a, s]).astype(f32)
        st[5, a, 0:COLS, :] = (inph[a] == 1).astype(f32)

    def halo_copies(src, staged, corners, dst, cdst, send, recv):
        edges = []
        diagonals = []
        for d in range(8):
            if d < 4:
                source = src.at[:, (1, ROWS)[d]] if d < 2 else staged.at[d - 2]
                target = dst.at[d]
            else:
                source, target = corners.at[d - 4], cdst.at[d - 4]
            (edges if d < 4 else diagonals).append(
                pltpu.make_async_remote_copy(
                    src_ref=source, dst_ref=target, send_sem=send.at[d], recv_sem=recv.at[d],
                    device_id=neighbours[d], device_id_type=MESH,
                )
            )
        return diagonals, edges

    def pack(src, staged, corners, fields):
        for f in range(fields):
            corners[0, f : f + 1, :] = src[f, 1, 0:1, :]
            corners[1, f : f + 1, :] = src[f, 1, COLS - 1 : COLS, :]
            corners[2, f : f + 1, :] = src[f, ROWS, 0:1, :]
            corners[3, f : f + 1, :] = src[f, ROWS, COLS - 1 : COLS, :]
            for a in range(ROWS):
                staged[0, f, a : a + 1, :] = src[f, a + 1, 0:1, :]
                staged[1, f, a : a + 1, :] = src[f, a + 1, COLS - 1 : COLS, :]

    PLACE = (3, 2, 1, 0)

    def put(buf, rows, base):
        for q, row in enumerate(rows):
            buf[pl.ds(q * FS + base, 8), :] = row

    def cell(buf, c):
        return buf[pl.ds(c, 32, stride=FS), :]

    def turned(cells):
        return jnp.concatenate([cell(fb, c) for c in cells], axis=0).astype(bf16).T

    def centre(a, col, o):
        base = cell(ib, (a + 1) * 8 + col)
        return jnp.concatenate([base[0:16], base[16:32] * al[o] + be[o]], axis=0).astype(bf16)

    def at_block(part, block, blocks):
        pieces = []
        if block > 0:
            pieces.append(jnp.zeros((32 * block, 128), bf16))
        pieces.append(part)
        if block < blocks - 1:
            pieces.append(jnp.zeros((32 * (blocks - 1 - block), 128), bf16))
        return jnp.concatenate(pieces, axis=0) if len(pieces) > 1 else part

    def overlap(left, right, slot, sums, cols):
        w = jnp.maximum(jnp.dot(left, right, preferred_element_type=f32), 0.0)
        w2 = w * w
        wb[slot] = w2
        part = jnp.sum((w2 * w).reshape(16, 8, 256), axis=0)
        for e in range(2):
            half = part[:, 128 * e : 128 * e + 128]
            sums[cols[e]] = half if sums[cols[e]] is None else sums[cols[e]] + half

    def own_tiles(a, ox3, lrow, slot, sums):
        for q, (ca, cb, ja, jb, group) in enumerate(OWN_TILES):
            pa = centre(a, ca, ox3 + (ja - ca + 1))
            pb = centre(a, cb, ox3 + (jb - cb + 1))
            if group == 2:
                left = jnp.concatenate([lrow[0], lrow[1]], axis=1)
                right = jnp.concatenate([at_block(pa, ja, 8), at_block(pb, jb - 2 + 4, 8)], axis=1)
            else:
                left = lrow[group]
                right = jnp.concatenate(
                    [at_block(pa, ja - GROUP_START[group], 4), at_block(pb, jb - GROUP_START[group], 4)],
                    axis=1,
                )
            overlap(left, right, slot + q, sums, (ca, cb))

    def edge_tile(a, ox3, r, slot, sums):
        pa = centre(a, 0, ox3)
        pb = centre(a, COLS - 1, ox3 + 2)
        group, odd = divmod(r, 2) if 0 <= r < ROWS else (3, int(r >= ROWS))
        right = jnp.concatenate([at_block(pa, 2 * odd, 4), at_block(pb, 2 * odd + 1, 4)], axis=1)
        overlap(gh[group], right, slot + 8, sums, (0, COLS - 1))

    def pull(w2, left, sums, cols):
        hi = w2.astype(bf16)
        lo = (w2 - hi.astype(f32)).astype(bf16)
        both = jnp.concatenate([left, left], axis=1)
        total = jnp.dot(both, jnp.concatenate([hi, lo], axis=0), preferred_element_type=f32)
        for e in range(2):
            part = total[32 * e : 32 * e + 32, 128 * e : 128 * e + 128]
            sums[cols[e]] = part if sums[cols[e]] is None else sums[cols[e]] + part

    def own_pulls(r, slot, sums):
        for q, (ca, cb, ja, jb, group) in enumerate(OWN_TILES):
            left = jnp.concatenate([tf[r, ja], tf[r, jb]], axis=0)
            pull(wb[slot + q], left, sums, (ca, cb))

    def side_cells(r):
        if r < 0:
            return (CORNERS, 0), (CORNERS, 1)
        if r >= ROWS:
            return (CORNERS, 2), (CORNERS, 3)
        return (LEFT, r), (RIGHT, r)

    def moment_rows(block, px, py):
        rows = [None] * 32
        for q in range(4):
            field = None if q == 0 else tp[q - 1, block]
            for e, p in enumerate((px, py)):
                pieces = split3(p if field is None else p * field)
                for level in range(3):
                    rows[level * 8 + 2 * q + e] = pieces[level]
            if field is None:
                rows[24], rows[28] = jnp.ones_like(px), jnp.zeros_like(px)
            else:
                rows[24 + q] = rnd(field)
                rows[28 + q] = rnd(field - rows[24 + q])
        return rows

    pl.semaphore_wait(barrier, len(neighbours) + len(first_peers) + len(second_peers))

    position_copies = halo_copies(bp, stage, cstage, rb, crb, hs, hr)
    term_copies = halo_copies(tp, tstage, ctstage, trb, ctrb, ts, tr)

    def start(pair):
        for copy in pair[0] + pair[1]:
            copy.start()

    def coefficients():
        alive = st[4] > 0.5
        for f in range(2):
            free = st[f] + TIME_STEP * (st[2 + f] + TIME_STEP * st[13 + f]) - 0.5
            step = TIME_STEP * TIME_STEP
            bp[3 * f, 1 : ROWS + 1] = jnp.where(alive, free + step * st[7 + 3 * f], FAR)
            bp[3 * f + 1, 1 : ROWS + 1] = step * st[8 + 3 * f]
            bp[3 * f + 2, 1 : ROWS + 1] = step * st[9 + 3 * f]
        pack(bp, stage, cstage, 6)
        start(position_copies)

    def side_tiles(which):
        done = []
        for t in range(18):
            a, ox = t // 3, t % 3 - 1
            r = a + ox
            outside = r < 0 or r >= ROWS
            if which == "edges" and outside:
                done.append((t, a, ox, r, True))
            if outside == (which == "corners"):
                done.append((t, a, ox, r, False))
        return done

    def add_up(buf, a, sums):
        for s in range(COLS):
            if sums[s] is not None:
                buf[a, s] += sums[s]

    def densities(it):
        relax0, relax1 = rl[0], rl[1]
        for f in range(2):
            for r in range(ROWS):
                xp[f, r + 1] = bp[3 * f, r + 1] + relax0 * bp[3 * f + 1, r + 1] + relax1 * bp[3 * f + 2, r + 1]
        for r in range(ROWS):
            jrow, irow = feature_rows(xp[0, r + 1], xp[1, r + 1])
            put(fb, jrow, (r + 1) * 8)
            put(ib, irow, (r + 1) * 8)
        for r in range(ROWS):
            for g in range(2):
                lt[(r + 1) * 2 + g] = turned([(r + 1) * 8 + GROUP_START[g] + s for s in range(4)])
        da[...] = jnp.zeros_like(da)

        def density(t, c):
            a = t // 3
            step = lax.rem(t, 3)
            r = a + step
            sums = [None] * COLS
            own_tiles(a, step * 3, (lt[r * 2], lt[r * 2 + 1]), t * 9, sums)
            for s in range(COLS):
                da[pl.ds(a * 64 + s * 8, 8), :] += sums[s]
            return c

        lax.fori_loop(1, 17, density, 0, unroll=UNROLL)

        diagonals, edges = position_copies
        for copy in edges:
            copy.wait()
        for d, block in enumerate((BOTTOM, TOP, RIGHT, LEFT)):
            for f in range(2):
                xp[f, block] = rb[d, 3 * f] + relax0 * rb[d, 3 * f + 1] + relax1 * rb[d, 3 * f + 2]
        for block in EDGES:
            jrow, _ = feature_rows(xp[0, block], xp[1, block])
            put(fb, jrow, block * 8)
        for block in (TOP, BOTTOM):
            for g in range(2):
                lt[block * 2 + g] = turned([block * 8 + GROUP_START[g] + s for s in range(4)])
        for q in range(3):
            gh[q] = turned([b * 8 + s for r in (2 * q, 2 * q + 1) for b, s in side_cells(r)])
        for t, a, ox, r, row in side_tiles("edges"):
            sums = [None] * COLS
            if row:
                own_tiles(a, (ox + 1) * 3, (lt[(r + 1) * 2], lt[(r + 1) * 2 + 1]), t * 9, sums)
            else:
                edge_tile(a, (ox + 1) * 3, r, t * 9, sums)
            for s in range(COLS):
                if sums[s] is not None:
                    da[a * 64 + s * 8 : a * 64 + s * 8 + 8, :] += sums[s]

        for copy in diagonals:
            copy.wait()
        for d in range(4):
            for f in range(2):
                xp[f, CORNERS, PLACE[d] : PLACE[d] + 1, :] = (
                    crb[d, 3 * f : 3 * f + 1, :] + relax0[0:1] * crb[d, 3 * f + 1 : 3 * f + 2, :]
                    + relax1[0:1] * crb[d, 3 * f + 2 : 3 * f + 3, :]
                )
        jrow, _ = feature_rows(xp[0, CORNERS], xp[1, CORNERS])
        put(fb, jrow, CORNERS * 8)
        gh[3] = turned([CORNERS * 8 + q for q in range(4)])
        for t, a, ox, r, row in side_tiles("corners"):
            sums = [None] * COLS
            edge_tile(a, (ox + 1) * 3, r, t * 9, sums)
            for s in range(COLS):
                if sums[s] is not None:
                    da[a * 64 + s * 8 : a * 64 + s * 8 + 8, :] += sums[s]

    def bounds_copies(now, src_slot, dst, send, recv, targets):
        return [
            pltpu.make_async_remote_copy(
                src_ref=ar0.at[now, src_slot], dst_ref=dst.at[now, d],
                send_sem=send.at[now, d], recv_sem=recv.at[now, d],
                device_id=target, device_id_type=MESH,
            )
            for d, target in enumerate(targets)
        ]

    def forces(it):
        now = lax.rem(it, 2)
        alive = st[4] > 0.5
        hot = st[5] > 0.5
        rows = []
        for a in range(ROWS):
            parts = [da[pl.ds(a * 64 + q, 8, stride=8), :] for q in range(8)]
            while len(parts) > 1:
                parts = [parts[q] + parts[q + 1] for q in range(0, len(parts), 2)]
            rows.append(parts[0])
        density_now = KERNEL_NORM * jnp.stack(rows)
        ratio = density_now / jnp.where(hot, REST_HEAVY, REST_LIGHT)
        lit = alive & jnp.logical_not(hot)
        hvy = alive & hot
        peaks = (
            jnp.where(lit, ratio, NEG), jnp.where(hvy, ratio, NEG),
            jnp.where(lit, -ratio, NEG), jnp.where(hvy, -ratio, NEG),
        )
        vec = jnp.full((1, 128), NEG, f32)
        for q in range(4):
            top = jnp.max(jnp.max(peaks[q], axis=0), axis=0, keepdims=True)
            top = jnp.max(top, axis=1, keepdims=True)
            vec = jnp.where(lane == q, top, vec)
        ar0[now, 0] = vec
        first = bounds_copies(now, 0, ar1, a1s, a1r, first_peers)
        for copy in first:
            copy.start()

        safe = jnp.where(alive, density_now, 1.0)
        inverse = 1.0 / (safe * safe)
        excess = jnp.where(hot, STIFF_HEAVY, STIFF_LIGHT) * (ratio - 1.0)
        t0 = jnp.where(alive, st[6] * inverse, 0.0)
        u = excess * inverse
        u0 = jnp.where(lit, u, 0.0)
        u1 = jnp.where(hvy, u, 0.0)
        tp[0, 1 : ROWS + 1] = t0
        tp[1, 1 : ROWS + 1] = u0
        tp[2, 1 : ROWS + 1] = u1
        pack(tp, tstage, ctstage, 3)
        start(term_copies)

        for a in range(ROWS):
            put(fb, moment_rows(a + 1, xp[0, a + 1] + (a - 2.5), xp[1, a + 1] + row_cols), (a + 1) * 8)
        for a in range(ROWS):
            for s in range(COLS):
                tf[a + 1, s] = cell(fb, (a + 1) * 8 + s).astype(bf16)
        fa[...] = jnp.zeros_like(fa)

        def force(t, c):
            a = t // 3
            step = lax.rem(t, 3)
            sums = [None] * COLS
            own_pulls(a + step, t * 9, sums)
            for s in range(COLS):
                fa[a, s] += sums[s]
            return c

        lax.fori_loop(1, 17, force, 0, unroll=UNROLL)

        for copy in first:
            copy.wait()
        best = vec
        for d in range(len(first_peers)):
            best = jnp.maximum(best, ar1[now, d])
        ar0[now, 1] = best
        second = bounds_copies(now, 1, ar2, a2s, a2r, second_peers)
        for copy in second:
            copy.start()

        diagonals, edges = term_copies
        for copy in edges:
            copy.wait()
        for d, block in enumerate((BOTTOM, TOP, RIGHT, LEFT)):
            for f in range(3):
                tp[f, block] = trb[d, f]
        edge_x = {TOP: -3.5, BOTTOM: 3.5, LEFT: sub_f - 2.5, RIGHT: sub_f - 2.5}
        edge_y = {TOP: row_cols, BOTTOM: row_cols, LEFT: -3.5, RIGHT: 3.5}
        for block in EDGES:
            put(fb, moment_rows(block, xp[0, block] + edge_x[block], xp[1, block] + edge_y[block]), block * 8)
        for block in EDGES:
            for s in range(ROWS):
                tf[block, s] = cell(fb, block * 8 + s).astype(bf16)

        def side_pull(t, r, sums):
            (lb, ls), (ub, us) = side_cells(r)
            pull(wb[t * 9 + 8], jnp.concatenate([tf[lb, ls], tf[ub, us]], axis=0), sums, (0, COLS - 1))

        for t, a, ox, r, row in side_tiles("edges"):
            sums = [None] * COLS
            if row:
                own_pulls(r + 1, t * 9, sums)
            else:
                side_pull(t, r, sums)
            add_up(fa, a, sums)

        for copy in diagonals:
            copy.wait()
        for d in range(4):
            for f in range(3):
                tp[f, CORNERS, PLACE[d] : PLACE[d] + 1, :] = ctrb[d, f : f + 1, :]
        corner_x = jnp.where(sub < 2, -3.5, 3.5)
        corner_y = jnp.where(lax.rem(sub, 2) == 0, -3.5, 3.5)
        put(fb, moment_rows(CORNERS, xp[0, CORNERS] + corner_x, xp[1, CORNERS] + corner_y), CORNERS * 8)
        for s in range(4):
            tf[CORNERS, s] = cell(fb, CORNERS * 8 + s).astype(bf16)
        for t, a, ox, r, row in side_tiles("corners"):
            sums = [None] * COLS
            side_pull(t, r, sums)
            add_up(fa, a, sums)

        for a in range(ROWS):
            for s in range(COLS):
                part = fa[a, s]
                row = a * 8 + s
                mb[pl.ds(row, 8, stride=FS), :] = part[0:8] + part[8:16] + part[16:24]
                mb[pl.ds(8 * FS + row, 8, stride=FS), :] = part[24:32]

        for a in range(ROWS):
            def mom(q):
                return mb[q * FS + a * 8 : q * FS + a * 8 + 8, :]

            s1 = mom(8) + mom(12)
            factor = jnp.where(
                alive[a], 6.0 * KERNEL_NORM / jnp.where(hot[a], MASS_HEAVY, MASS_LIGHT), 0.0
            )
            for f in range(2):
                p = xp[f, a + 1] + (a - 2.5 if f == 0 else row_cols)
                arm = p * s1 - mom(f)
                for q, term in enumerate((t0[a], u0[a], u1[a])):
                    push = term * arm + p * (mom(9 + q) + mom(13 + q)) - mom(2 + 2 * q + f)
                    st[7 + 3 * f + q, a] = jnp.where(alive[a], factor * push, 0.0)

        @pl.when(it < ITERS - 1)
        def _():
            coefficients()

        for copy in second:
            copy.wait()
        for d in range(len(second_peers)):
            best = jnp.maximum(best, ar2[now, d])
        out_ref[pl.ds(OUT_MONITOR + it, 1), :] = jnp.where(lane < 2, best, -best)
        relax0 = jnp.broadcast_to(1.0 / (1.0 + best[:, 0:1] + best[:, 2:3]), (8, 128))
        relax1 = jnp.broadcast_to(1.0 / (1.0 + best[:, 1:2] + best[:, 3:4]), (8, 128))
        rl[0] = relax0
        rl[1] = relax1
        for a in range(ROWS):
            relax = jnp.where(hot[a], relax1, relax0)
            st[6, a] = jnp.where(alive[a], st[6, a] + relax * excess[a], 0.0)

    coefficients()

    def whole(it, carry):
        densities(it)
        forces(it)
        return carry

    lax.fori_loop(0, ITERS, whole, 0)

    for a in range(ROWS):
        live = st[4, a]
        for f in range(2):
            accel = st[7 + 3 * f, a] + rl[0] * st[8 + 3 * f, a] + rl[1] * st[9 + 3 * f, a]
            v = live * (st[2 + f, a] + TIME_STEP * (st[13 + f, a] + accel))
            p = live * (st[f, a] + TIME_STEP * v)
            out_ref[pl.ds(a * 12 + f, COLS, stride=2), :] = p[0:COLS]
            out_ref[pl.ds(OUT_VELOCITY + a * 12 + f, COLS, stride=2), :] = v[0:COLS]
        out_ref[OUT_PRESSURE + a * 8 : OUT_PRESSURE + a * 8 + 8, :] = st[6, a]


def spread(in_ref, npos_ref, nvel_ref, pres_ref, mon_ref):
    npos_ref[...] = in_ref[0:OUT_VELOCITY, :]
    nvel_ref[...] = in_ref[OUT_VELOCITY:OUT_PRESSURE, :]
    for a in range(ROWS):
        pres_ref[a] = in_ref[OUT_PRESSURE + a * 8 : OUT_PRESSURE + a * 8 + COLS, :]
    mon_ref[...] = in_ref[OUT_MONITOR : OUT_MONITOR + ITERS, 0:4]


def flat(value):
    return value.transpose(1, 2, 0, 3).reshape(ROWS * COLS * 2, 128)


def unflat(value):
    return value.reshape(ROWS, COLS, 2, 128).transpose(2, 0, 1, 3)


def local(position, velocity, other_accel, phase_ids, counts):
    vmem = pl.BlockSpec(memory_space=pltpu.VMEM)
    hbm = pl.BlockSpec(memory_space=pl.ANY)
    dma = pltpu.SemaphoreType.DMA
    n1 = lax.axis_size("y") * lax.axis_size("core") - 1
    n2 = lax.axis_size("x") * lax.axis_size("zl") * lax.axis_size("zh") - 1
    packed = pl.pallas_call(
        kernel,
        out_shape=jax.ShapeDtypeStruct((OUT_ROWS, 128), f32),
        in_specs=[hbm] * 4 + [pl.BlockSpec(memory_space=pltpu.SMEM)],
        out_specs=vmem,
        scratch_shapes=[
            pltpu.VMEM((ROWS * COLS * 2, 128), f32),
            pltpu.VMEM((ROWS * COLS * 2, 128), f32),
            pltpu.VMEM((ROWS * COLS * 2, 128), f32),
            pltpu.VMEM((ROWS, COLS, 128), jnp.int32),
            pltpu.VMEM((15, ROWS, 8, 128), f32),
            pltpu.VMEM((2, BLOCKS, 8, 128), f32),
            pltpu.VMEM((6, BLOCKS, 8, 128), f32),
            pltpu.VMEM((3, BLOCKS, 8, 128), f32),
            pltpu.VMEM((2, 6, 8, 128), f32),
            pltpu.VMEM((2, 3, 8, 128), f32),
            pltpu.VMEM((4, 8, 128), f32),
            pltpu.VMEM((4, 8, 128), f32),
            pltpu.VMEM((4, 6, 8, 128), f32),
            pltpu.VMEM((4, 3, 8, 128), f32),
            pltpu.VMEM((4, 8, 128), f32),
            pltpu.VMEM((4, 8, 128), f32),
            pltpu.VMEM((32 * FS, 128), f32),
            pltpu.VMEM((32 * FS, 128), f32),
            pltpu.VMEM((16, 128, 128), bf16),
            pltpu.VMEM((4, 128, 128), bf16),
            pltpu.VMEM((162, 128, 256), f32),
            pltpu.VMEM((ROWS * 64, 128), f32),
            pltpu.VMEM((ROWS, COLS, 32, 128), f32),
            pltpu.VMEM((BLOCKS, 8, 32, 128), bf16),
            pltpu.VMEM((16 * FS, 128), f32),
            pltpu.VMEM((9, 16, 128), f32),
            pltpu.VMEM((9, 16, 128), f32),
            pltpu.VMEM((2, 8, 128), f32),
            pltpu.VMEM((2, 2, 1, 128), f32),
            pltpu.VMEM((2, n1, 1, 128), f32),
            pltpu.VMEM((2, n2, 1, 128), f32),
            dma((4,)), dma((8,)), dma((8,)), dma((8,)), dma((8,)),
            dma((2, n1)), dma((2, n1)), dma((2, n2)), dma((2, n2)),
        ],
        compiler_params=pltpu.CompilerParams(
            collective_id=0, has_side_effects=True, vmem_limit_bytes=60 * 1024 * 1024
        ),
    )(flat(position), flat(velocity), flat(other_accel), phase_ids, counts)
    new_pos, new_vel, pressure, monitor = pl.pallas_call(
        spread,
        out_shape=(
            jax.ShapeDtypeStruct((ROWS * COLS * 2, 128), f32),
            jax.ShapeDtypeStruct((ROWS * COLS * 2, 128), f32),
            jax.ShapeDtypeStruct((ROWS, COLS, 128), f32),
            jax.ShapeDtypeStruct((ITERS, 4), f32),
        ),
        in_specs=[vmem],
        out_specs=[vmem] * 4,
        compiler_params=pltpu.CompilerParams(vmem_limit_bytes=4 * 1024 * 1024),
    )(packed)
    return unflat(new_pos), unflat(new_vel), pressure, monitor


def solution(mesh):
    gx = ("x", "zl")
    gy = ("zh", "y", "core")
    torus = Mesh(mesh.devices.reshape(4, 2, 2, 4, 2), SPLIT)
    wide = P(None, gx, gy, None)
    return jax.shard_map(
        local, mesh=torus, in_specs=(wide, wide, wide, P(gx, gy, None), P(gx, gy)),
        out_specs=(wide, wide, P(gx, gy, None), P()), check_vma=False,
    )
```

```python
import jax
import jax.numpy as jnp
from jax import lax
from jax.experimental import pallas as pl
from jax.experimental.pallas import tpu as pltpu
from jax.sharding import Mesh
from jax.sharding import PartitionSpec as P

ITERS = 4
TIME_STEP = 0.05
KERNEL_NORM = 4.0 / (3.141592653589793 * 64.0)
REST_LIGHT = 1.2
REST_HEAVY = 1.5
STIFF_LIGHT = 100.0
STIFF_HEAVY = 200.0
MASS_LIGHT = 1.0
MASS_HEAVY = 1.5
FAR = float(2**30)
NEG = -1e30
MESH = pl.DeviceIdType.MESH
SPLIT = ("x", "zl", "zh", "y", "core")
ROWS = 6
COLS = 6
TOP, BOTTOM, LEFT, RIGHT, CORNERS = 0, 7, 8, 9, 10
EDGES = (TOP, BOTTOM, LEFT, RIGHT)
BLOCKS = 11
FS = BLOCKS * 8
DIRS = ((-1, 0), (1, 0), (0, -1), (0, 1), (-1, -1), (-1, 1), (1, -1), (1, 1))
OWN_TILES = (
    (0, 1, 0, 1, 0), (0, 1, 1, 2, 0),
    (2, 3, 1, 2, 0), (2, 3, 2, 3, 0), (2, 3, 3, 4, 1),
    (4, 5, 3, 4, 1), (4, 5, 4, 5, 1),
    (1, 4, 0, 5, 2),
)
ROW_TILES = (
    (0, 1, 0, 1, 0), (0, 1, 1, 2, 0), (2, 2, 2, 3, 0),
    (3, 4, 3, 4, 1), (3, 4, 4, 5, 1), (5, None, 5, None, 1),
)
GROUP_START = (0, 2)
UNROLL_DENSITY = 5
FORCE_FIRST = 4
OUT_VELOCITY = ROWS * COLS * 2
OUT_PRESSURE = 2 * OUT_VELOCITY
OUT_MONITOR = OUT_PRESSURE + ROWS * 8
OUT_ROWS = OUT_MONITOR + 8

f32 = jnp.float32
bf16 = jnp.bfloat16


def rnd(v):
    return v.astype(bf16).astype(f32)


def split3(v):
    h = rnd(v)
    r = v - h
    m = rnd(r)
    return h, m, rnd(r - m)


def feature_rows(x, y):
    xs = split3(x)
    ys = split3(y)
    rs = split3(x * x + y * y)
    one = jnp.ones_like(x)
    zero = jnp.zeros_like(x)
    h, m, l = 0, 1, 2
    jrow = (
        [xs[q] for q in (h, h, m, m, l, h)] + [ys[q] for q in (h, h, m, m, l, h)]
        + list(rs) + [one, one, one] + list(xs) + list(ys) + [one] * 7 + [zero]
    )
    irow = (
        [2.0 * xs[q] for q in (h, m, h, m, h, l)] + [2.0 * ys[q] for q in (h, m, h, m, h, l)]
        + [-one] * 3 + [-q for q in rs] + [zero] * 6 + list(xs) + list(ys) + [zero, zero]
    )
    return jrow, irow


def kernel(
    pos_ref, vel_ref, oa_ref, phase_ref, counts_ref,
    out_ref,
    inp, inv, ino, inph, st, xp, bp, tp, stage, tstage, cstage, ctstage, rb, trb, crb, ctrb,
    fb, ib, lt, gh, wb, aj, da, fa, tf, mb, al, be, rl, ar0, ar1, ar2,
    ins, hs, hr, ts, tr, a1s, a1r, a2s, a2r,
):
    index = {name: lax.axis_index(name) for name in SPLIT}
    size = {name: lax.axis_size(name) for name in SPLIT}
    gx = index["x"] * size["zl"] + index["zl"]
    gy = (index["zh"] * size["y"] + index["y"]) * size["core"] + index["core"]
    nx = size["x"] * size["zl"]
    ny = size["zh"] * size["y"] * size["core"]

    def around(dx, dy):
        px = lax.rem(gx + dx + nx, nx)
        py = lax.rem(gy + dy + ny, ny)
        return (
            px // size["zl"], lax.rem(px, size["zl"]), py // (size["y"] * size["core"]),
            lax.rem(py // size["core"], size["y"]), lax.rem(py, size["core"]),
        )

    def peers(names):
        steps = [()]
        for name in SPLIT:
            count = size[name] if name in names else 1
            steps = [s + (q,) for s in steps for q in range(count)]
        return [
            tuple(lax.rem(index[name] + q, size[name]) for name, q in zip(SPLIT, s))
            for s in steps if any(s)
        ]

    neighbours = [around(dx, dy) for dx, dy in DIRS]
    first_peers = peers(("y", "core"))
    second_peers = peers(("x", "zl", "zh"))
    barrier = pltpu.get_barrier_semaphore()
    for partner in neighbours + first_peers + second_peers:
        pl.semaphore_signal(barrier, inc=1, device_id=partner, device_id_type=MESH)

    loads = [
        pltpu.make_async_copy(src, dst, ins.at[q])
        for q, (src, dst) in enumerate(
            ((pos_ref, inp), (vel_ref, inv), (oa_ref, ino), (phase_ref, inph))
        )
    ]
    for load in loads:
        load.start()

    st[...] = jnp.zeros_like(st)
    da[...] = jnp.zeros_like(da)
    mb[...] = jnp.zeros_like(mb)
    xp[...] = jnp.full_like(xp, FAR)
    tp[...] = jnp.zeros_like(tp)
    fb[...] = jnp.zeros_like(fb)
    aj[...] = jnp.zeros_like(aj)
    bp[...] = jnp.zeros_like(bp)
    rl[...] = jnp.zeros_like(rl)
    for buf in (stage, tstage, cstage, ctstage):
        buf[...] = jnp.zeros_like(buf)
    k = lax.broadcasted_iota(jnp.int32, (16, 128), 0)
    for ox in (-1, 0, 1):
        for oy in (-1, 0, 1):
            o = (ox + 1) * 3 + oy + 1
            al[o] = jnp.where(
                k < 2, 1.0,
                jnp.where((k >= 8) & (k < 11), 2.0 * ox, jnp.where((k >= 11) & (k < 14), 2.0 * oy, 0.0)),
            )
            be[o] = jnp.where(
                (k >= 2) & (k < 5), -2.0 * ox,
                jnp.where(
                    (k >= 5) & (k < 8), -2.0 * oy, jnp.where(k == 14, 1.0 - ox * ox - oy * oy, 0.0)
                ),
            )
    lane = lax.broadcasted_iota(jnp.int32, (1, 128), 1)
    sub = lax.broadcasted_iota(jnp.int32, (8, 128), 0)
    sub_f = sub.astype(f32)
    row_cols = jnp.where(sub == 7, -1.0, sub_f) - 2.5
    for load in loads:
        load.wait()
    for a in range(ROWS):
        for f in range(2):
            for s in range(COLS):
                at = a * 12 + s * 2 + f
                st[f, a, s : s + 1, :] = inp[at : at + 1, :]
                st[2 + f, a, s : s + 1, :] = inv[at : at + 1, :]
                st[13 + f, a, s : s + 1, :] = ino[at : at + 1, :]
        for s in range(COLS):
            st[4, a, s : s + 1, :] = (lane < counts_ref[a, s]).astype(f32)
        st[5, a, 0:COLS, :] = (inph[a] == 1).astype(f32)

    def halo_copies(src, staged, corners, dst, cdst, send, recv):
        edges = []
        diagonals = []
        for d in range(8):
            if d < 4:
                source = src.at[:, (1, ROWS)[d]] if d < 2 else staged.at[d - 2]
                target = dst.at[d]
            else:
                source, target = corners.at[d - 4], cdst.at[d - 4]
            (edges if d < 4 else diagonals).append(
                pltpu.make_async_remote_copy(
                    src_ref=source, dst_ref=target, send_sem=send.at[d], recv_sem=recv.at[d],
                    device_id=neighbours[d], device_id_type=MESH,
                )
            )
        return diagonals, edges

    def pack(src, staged, corners, fields):
        for f in range(fields):
            corners[0, f : f + 1, :] = src[f, 1, 0:1, :]
            corners[1, f : f + 1, :] = src[f, 1, COLS - 1 : COLS, :]
            corners[2, f : f + 1, :] = src[f, ROWS, 0:1, :]
            corners[3, f : f + 1, :] = src[f, ROWS, COLS - 1 : COLS, :]
            for a in range(ROWS):
                staged[0, f, a : a + 1, :] = src[f, a + 1, 0:1, :]
                staged[1, f, a : a + 1, :] = src[f, a + 1, COLS - 1 : COLS, :]

    PLACE = (3, 2, 1, 0)

    def put(buf, rows, base):
        for q, row in enumerate(rows):
            buf[pl.ds(q * FS + base, 8), :] = row

    def cell(buf, c):
        return buf[pl.ds(c, 32, stride=FS), :]

    def turned(cells):
        return jnp.concatenate([cell(fb, c) for c in cells], axis=0).astype(bf16).T

    def centre(a, col, o):
        base = cell(ib, (a + 1) * 8 + col)
        return jnp.concatenate([base[0:16], base[16:32] * al[o] + be[o]], axis=0).astype(bf16)

    def at_block(part, block, blocks):
        pieces = []
        if block > 0:
            pieces.append(jnp.zeros((32 * block, 128), bf16))
        pieces.append(part)
        if block < blocks - 1:
            pieces.append(jnp.zeros((32 * (blocks - 1 - block), 128), bf16))
        return jnp.concatenate(pieces, axis=0) if len(pieces) > 1 else part

    def collect(sums, col, part):
        if col is not None:
            sums[col] = part if sums[col] is None else sums[col] + part

    def overlap(left, right, slot, sums, cols, mirrors=(None, None)):
        w = jnp.maximum(jnp.dot(left, right, preferred_element_type=f32), 0.0)
        w2 = w * w
        wb[slot] = w2
        w3 = w2 * w
        part = jnp.sum(w3.reshape(16, 8, 256), axis=0)
        for e in range(2):
            collect(sums, cols[e], part[:, 128 * e : 128 * e + 128])
            if mirrors[e] is not None:
                aj[mirrors[e]] += w3[:, 128 * e : 128 * e + 128]

    def own_tiles(a, ox3, lrow, slot, sums, tiles=OWN_TILES, mirror_row=None):
        for q, (ca, cb, ja, jb, group) in enumerate(tiles):
            blocks = 8 if group == 2 else 4
            halves = []
            mirrors = []
            for col, j, e in ((ca, ja, 0), (cb, jb, 1)):
                if col is None:
                    halves.append(jnp.zeros((32 * blocks, 128), bf16))
                    mirrors.append(None)
                    continue
                block = (j + 2 * e if group == 2 else j - GROUP_START[group])
                halves.append(at_block(centre(a, col, ox3 + (j - col + 1)), block, blocks))
                keep = mirror_row is not None and not (tiles is ROW_TILES and col == j)
                mirrors.append(mirror_row * COLS + j if keep else None)
            left = jnp.concatenate([lrow[0], lrow[1]], axis=1) if group == 2 else lrow[group]
            overlap(left, jnp.concatenate(halves, axis=1), slot + q, sums, (ca, cb), mirrors)

    def edge_tile(a, ox3, r, slot, sums):
        pa = centre(a, 0, ox3)
        pb = centre(a, COLS - 1, ox3 + 2)
        group, odd = divmod(r, 2) if 0 <= r < ROWS else (3, int(r >= ROWS))
        right = jnp.concatenate([at_block(pa, 2 * odd, 4), at_block(pb, 2 * odd + 1, 4)], axis=1)
        overlap(gh[group], right, slot + 8, sums, (0, COLS - 1))

    def halves_of(w2):
        hi = w2.astype(bf16)
        return hi, (w2 - hi.astype(f32)).astype(bf16)

    def pull(hi, lo, left, sums, cols):
        both = jnp.concatenate([left, left], axis=1)
        total = jnp.dot(both, jnp.concatenate([hi, lo], axis=0), preferred_element_type=f32)
        for e in range(2):
            collect(sums, cols[e], total[32 * e : 32 * e + 32, 128 * e : 128 * e + 128])

    def pair_rows(block, ca, cb):
        return jnp.concatenate([tf[block, ca], tf[block, ca if cb is None else cb]], axis=0)

    def own_pulls(r, slot, sums, a=None, mirrored=None, tiles=OWN_TILES):
        for q, (ca, cb, ja, jb, group) in enumerate(tiles):
            hi, lo = halves_of(wb[slot + q])
            pull(hi, lo, pair_rows(r, ja, jb), sums, (ca, cb))
            if mirrored is None:
                continue
            row = tiles is ROW_TILES
            cols = tuple(None if row and c == j else j for c, j in ((ca, ja), (cb, jb)))
            if cols == (None, None):
                continue
            turn = [
                jnp.concatenate([v[:, 0:128].T, v[:, 128:256].T], axis=1) for v in (hi, lo)
            ]
            pull(turn[0], turn[1], pair_rows(a, ca, cb), mirrored, cols)

    def side_cells(r):
        if r < 0:
            return (CORNERS, 0), (CORNERS, 1)
        if r >= ROWS:
            return (CORNERS, 2), (CORNERS, 3)
        return (LEFT, r), (RIGHT, r)

    def moment_rows(block, px, py):
        rows = [None] * 32
        for q in range(4):
            field = None if q == 0 else tp[q - 1, block]
            for e, p in enumerate((px, py)):
                pieces = split3(p if field is None else p * field)
                for level in range(3):
                    rows[level * 8 + 2 * q + e] = pieces[level]
            if field is None:
                rows[24], rows[28] = jnp.ones_like(px), jnp.zeros_like(px)
            else:
                rows[24 + q] = rnd(field)
                rows[28 + q] = rnd(field - rows[24 + q])
        return rows

    pl.semaphore_wait(barrier, len(neighbours) + len(first_peers) + len(second_peers))

    position_copies = halo_copies(bp, stage, cstage, rb, crb, hs, hr)
    term_copies = halo_copies(tp, tstage, ctstage, trb, ctrb, ts, tr)

    def start(pair):
        for copy in pair[0] + pair[1]:
            copy.start()

    def coefficients():
        alive = st[4] > 0.5
        for f in range(2):
            free = st[f] + TIME_STEP * (st[2 + f] + TIME_STEP * st[13 + f]) - 0.5
            step = TIME_STEP * TIME_STEP
            bp[3 * f, 1 : ROWS + 1] = jnp.where(alive, free + step * st[7 + 3 * f], FAR)
            bp[3 * f + 1, 1 : ROWS + 1] = step * st[8 + 3 * f]
            bp[3 * f + 2, 1 : ROWS + 1] = step * st[9 + 3 * f]
        pack(bp, stage, cstage, 6)
        start(position_copies)

    def side_tiles(which):
        done = []
        for t in range(18):
            a, ox = t // 3, t % 3 - 1
            r = a + ox
            outside = r < 0 or r >= ROWS
            if which == "edges" and outside:
                done.append((t, a, ox, r, True))
            if outside == (which == "corners"):
                done.append((t, a, ox, r, False))
        return done

    def add_up(buf, a, sums):
        for s in range(COLS):
            if sums[s] is not None:
                buf[a, s] += sums[s]

    def densities(it):
        relax0, relax1 = rl[0], rl[1]
        for f in range(2):
            for r in range(ROWS):
                xp[f, r + 1] = bp[3 * f, r + 1] + relax0 * bp[3 * f + 1, r + 1] + relax1 * bp[3 * f + 2, r + 1]
        for r in range(ROWS):
            jrow, irow = feature_rows(xp[0, r + 1], xp[1, r + 1])
            put(fb, jrow, (r + 1) * 8)
            put(ib, irow, (r + 1) * 8)
        for r in range(ROWS):
            for g in range(2):
                lt[(r + 1) * 2 + g] = turned([(r + 1) * 8 + GROUP_START[g] + s for s in range(4)])
        def row_with_itself(a, sums):
            own_tiles(a, 3, (lt[(a + 1) * 2], lt[(a + 1) * 2 + 1]), (3 * a + 1) * 9, sums, ROW_TILES, a)
            for s in range(COLS):
                block = aj[a * COLS + s].T
                aj[a * COLS + s] = jnp.zeros((128, 128), f32)
                collect(sums, s, jnp.sum(block.reshape(16, 8, 128), axis=0))

        def keep(a, sums):
            for s in range(COLS):
                da[pl.ds(a * 64 + s * 8, 8), :] = sums[s]

        def density(a, c):
            sums = [None] * COLS
            row_with_itself(a, sums)
            own_tiles(
                a, 6, (lt[(a + 2) * 2], lt[(a + 2) * 2 + 1]), (3 * a + 2) * 9, sums, OWN_TILES, a + 1
            )
            keep(a, sums)
            return c

        lax.fori_loop(0, ROWS - 1, density, 0, unroll=UNROLL_DENSITY)
        sums = [None] * COLS
        row_with_itself(ROWS - 1, sums)
        keep(ROWS - 1, sums)

        diagonals, edges = position_copies
        for copy in edges:
            copy.wait()
        for d, block in enumerate((BOTTOM, TOP, RIGHT, LEFT)):
            for f in range(2):
                xp[f, block] = rb[d, 3 * f] + relax0 * rb[d, 3 * f + 1] + relax1 * rb[d, 3 * f + 2]
        for block in EDGES:
            jrow, _ = feature_rows(xp[0, block], xp[1, block])
            put(fb, jrow, block * 8)
        for block in (TOP, BOTTOM):
            for g in range(2):
                lt[block * 2 + g] = turned([block * 8 + GROUP_START[g] + s for s in range(4)])
        for q in range(3):
            gh[q] = turned([b * 8 + s for r in (2 * q, 2 * q + 1) for b, s in side_cells(r)])
        for t, a, ox, r, row in side_tiles("edges"):
            sums = [None] * COLS
            if row:
                own_tiles(a, (ox + 1) * 3, (lt[(r + 1) * 2], lt[(r + 1) * 2 + 1]), t * 9, sums)
            else:
                edge_tile(a, (ox + 1) * 3, r, t * 9, sums)
            for s in range(COLS):
                if sums[s] is not None:
                    da[a * 64 + s * 8 : a * 64 + s * 8 + 8, :] += sums[s]

        for copy in diagonals:
            copy.wait()
        for d in range(4):
            for f in range(2):
                xp[f, CORNERS, PLACE[d] : PLACE[d] + 1, :] = (
                    crb[d, 3 * f : 3 * f + 1, :] + relax0[0:1] * crb[d, 3 * f + 1 : 3 * f + 2, :]
                    + relax1[0:1] * crb[d, 3 * f + 2 : 3 * f + 3, :]
                )
        jrow, _ = feature_rows(xp[0, CORNERS], xp[1, CORNERS])
        put(fb, jrow, CORNERS * 8)
        gh[3] = turned([CORNERS * 8 + q for q in range(4)])
        for t, a, ox, r, row in side_tiles("corners"):
            sums = [None] * COLS
            edge_tile(a, (ox + 1) * 3, r, t * 9, sums)
            for s in range(COLS):
                if sums[s] is not None:
                    da[a * 64 + s * 8 : a * 64 + s * 8 + 8, :] += sums[s]

    def bounds_copies(now, src_slot, dst, send, recv, targets):
        return [
            pltpu.make_async_remote_copy(
                src_ref=ar0.at[now, src_slot], dst_ref=dst.at[now, d],
                send_sem=send.at[now, d], recv_sem=recv.at[now, d],
                device_id=target, device_id_type=MESH,
            )
            for d, target in enumerate(targets)
        ]

    def forces(it):
        now = lax.rem(it, 2)
        alive = st[4] > 0.5
        hot = st[5] > 0.5
        rows = []
        for a in range(ROWS):
            parts = [da[pl.ds(a * 64 + q, 8, stride=8), :] for q in range(8)]
            while len(parts) > 1:
                parts = [parts[q] + parts[q + 1] for q in range(0, len(parts), 2)]
            rows.append(parts[0])
        density_now = KERNEL_NORM * jnp.stack(rows)
        ratio = density_now / jnp.where(hot, REST_HEAVY, REST_LIGHT)
        lit = alive & jnp.logical_not(hot)
        hvy = alive & hot
        peaks = (
            jnp.where(lit, ratio, NEG), jnp.where(hvy, ratio, NEG),
            jnp.where(lit, -ratio, NEG), jnp.where(hvy, -ratio, NEG),
        )
        vec = jnp.full((1, 128), NEG, f32)
        for q in range(4):
            top = jnp.max(jnp.max(peaks[q], axis=0), axis=0, keepdims=True)
            top = jnp.max(top, axis=1, keepdims=True)
            vec = jnp.where(lane == q, top, vec)
        ar0[now, 0] = vec
        first = bounds_copies(now, 0, ar1, a1s, a1r, first_peers)
        for copy in first:
            copy.start()

        safe = jnp.where(alive, density_now, 1.0)
        inverse = 1.0 / (safe * safe)
        excess = jnp.where(hot, STIFF_HEAVY, STIFF_LIGHT) * (ratio - 1.0)
        t0 = jnp.where(alive, st[6] * inverse, 0.0)
        u = excess * inverse
        u0 = jnp.where(lit, u, 0.0)
        u1 = jnp.where(hvy, u, 0.0)
        tp[0, 1 : ROWS + 1] = t0
        tp[1, 1 : ROWS + 1] = u0
        tp[2, 1 : ROWS + 1] = u1
        pack(tp, tstage, ctstage, 3)
        start(term_copies)

        for a in range(ROWS):
            put(fb, moment_rows(a + 1, xp[0, a + 1] + (a - 2.5), xp[1, a + 1] + row_cols), (a + 1) * 8)
        for a in range(ROWS):
            for s in range(COLS):
                tf[a + 1, s] = cell(fb, (a + 1) * 8 + s).astype(bf16)

        def force(a, c):
            here = [None] * COLS
            below = [None] * COLS
            own_pulls(a + 1, (3 * a + 1) * 9, here, a + 1, here, ROW_TILES)
            own_pulls(a + 2, (3 * a + 2) * 9, here, a + 1, below, OWN_TILES)
            for s in range(COLS):
                fa[a, s] += here[s]
                fa[a + 1, s] = below[s]
            return c

        for s in range(COLS):
            fa[0, s] = jnp.zeros((32, 128), f32)
        lax.fori_loop(0, FORCE_FIRST, force, 0)
        for copy in first:
            copy.wait()
        best = vec
        for d in range(len(first_peers)):
            best = jnp.maximum(best, ar1[now, d])
        ar0[now, 1] = best
        second = bounds_copies(now, 1, ar2, a2s, a2r, second_peers)
        for copy in second:
            copy.start()

        lax.fori_loop(FORCE_FIRST, ROWS - 1, force, 0)
        here = [None] * COLS
        own_pulls(ROWS, (3 * ROWS - 2) * 9, here, ROWS, here, ROW_TILES)
        add_up(fa, ROWS - 1, here)

        diagonals, edges = term_copies
        for copy in edges:
            copy.wait()
        for d, block in enumerate((BOTTOM, TOP, RIGHT, LEFT)):
            for f in range(3):
                tp[f, block] = trb[d, f]
        edge_x = {TOP: -3.5, BOTTOM: 3.5, LEFT: sub_f - 2.5, RIGHT: sub_f - 2.5}
        edge_y = {TOP: row_cols, BOTTOM: row_cols, LEFT: -3.5, RIGHT: 3.5}
        for block in EDGES:
            put(fb, moment_rows(block, xp[0, block] + edge_x[block], xp[1, block] + edge_y[block]), block * 8)
        for block in EDGES:
            for s in range(ROWS):
                tf[block, s] = cell(fb, block * 8 + s).astype(bf16)

        def side_pull(t, r, sums):
            (lb, ls), (ub, us) = side_cells(r)
            hi, lo = halves_of(wb[t * 9 + 8])
            pull(hi, lo, jnp.concatenate([tf[lb, ls], tf[ub, us]], axis=0), sums, (0, COLS - 1))

        for t, a, ox, r, row in side_tiles("edges"):
            sums = [None] * COLS
            if row:
                own_pulls(r + 1, t * 9, sums)
            else:
                side_pull(t, r, sums)
            add_up(fa, a, sums)

        for copy in diagonals:
            copy.wait()
        for d in range(4):
            for f in range(3):
                tp[f, CORNERS, PLACE[d] : PLACE[d] + 1, :] = ctrb[d, f : f + 1, :]
        corner_x = jnp.where(sub < 2, -3.5, 3.5)
        corner_y = jnp.where(lax.rem(sub, 2) == 0, -3.5, 3.5)
        put(fb, moment_rows(CORNERS, xp[0, CORNERS] + corner_x, xp[1, CORNERS] + corner_y), CORNERS * 8)
        for s in range(4):
            tf[CORNERS, s] = cell(fb, CORNERS * 8 + s).astype(bf16)
        for t, a, ox, r, row in side_tiles("corners"):
            sums = [None] * COLS
            side_pull(t, r, sums)
            add_up(fa, a, sums)

        for a in range(ROWS):
            for s in range(COLS):
                part = fa[a, s]
                row = a * 8 + s
                mb[pl.ds(row, 8, stride=FS), :] = part[0:8] + part[8:16] + part[16:24]
                mb[pl.ds(8 * FS + row, 8, stride=FS), :] = part[24:32]

        for a in range(ROWS):
            def mom(q):
                return mb[q * FS + a * 8 : q * FS + a * 8 + 8, :]

            s1 = mom(8) + mom(12)
            factor = jnp.where(
                alive[a], 6.0 * KERNEL_NORM / jnp.where(hot[a], MASS_HEAVY, MASS_LIGHT), 0.0
            )
            for f in range(2):
                p = xp[f, a + 1] + (a - 2.5 if f == 0 else row_cols)
                arm = p * s1 - mom(f)
                for q, term in enumerate((t0[a], u0[a], u1[a])):
                    push = term * arm + p * (mom(9 + q) + mom(13 + q)) - mom(2 + 2 * q + f)
                    st[7 + 3 * f + q, a] = jnp.where(alive[a], factor * push, 0.0)

        @pl.when(it < ITERS - 1)
        def _():
            coefficients()

        for copy in second:
            copy.wait()
        for d in range(len(second_peers)):
            best = jnp.maximum(best, ar2[now, d])
        out_ref[pl.ds(OUT_MONITOR + it, 1), :] = jnp.where(lane < 2, best, -best)
        relax0 = jnp.broadcast_to(1.0 / (1.0 + best[:, 0:1] + best[:, 2:3]), (8, 128))
        relax1 = jnp.broadcast_to(1.0 / (1.0 + best[:, 1:2] + best[:, 3:4]), (8, 128))
        rl[0] = relax0
        rl[1] = relax1
        for a in range(ROWS):
            relax = jnp.where(hot[a], relax1, relax0)
            st[6, a] = jnp.where(alive[a], st[6, a] + relax * excess[a], 0.0)

    coefficients()

    def whole(it, carry):
        densities(it)
        forces(it)
        return carry

    lax.fori_loop(0, ITERS, whole, 0)

    for a in range(ROWS):
        live = st[4, a]
        for f in range(2):
            accel = st[7 + 3 * f, a] + rl[0] * st[8 + 3 * f, a] + rl[1] * st[9 + 3 * f, a]
            v = live * (st[2 + f, a] + TIME_STEP * (st[13 + f, a] + accel))
            p = live * (st[f, a] + TIME_STEP * v)
            out_ref[pl.ds(a * 12 + f, COLS, stride=2), :] = p[0:COLS]
            out_ref[pl.ds(OUT_VELOCITY + a * 12 + f, COLS, stride=2), :] = v[0:COLS]
        out_ref[OUT_PRESSURE + a * 8 : OUT_PRESSURE + a * 8 + 8, :] = st[6, a]


def spread(in_ref, npos_ref, nvel_ref, pres_ref, mon_ref):
    npos_ref[...] = in_ref[0:OUT_VELOCITY, :]
    nvel_ref[...] = in_ref[OUT_VELOCITY:OUT_PRESSURE, :]
    for a in range(ROWS):
        pres_ref[a] = in_ref[OUT_PRESSURE + a * 8 : OUT_PRESSURE + a * 8 + COLS, :]
    mon_ref[...] = in_ref[OUT_MONITOR : OUT_MONITOR + ITERS, 0:4]


def flat(value):
    return value.transpose(1, 2, 0, 3).reshape(ROWS * COLS * 2, 128)


def unflat(value):
    return value.reshape(ROWS, COLS, 2, 128).transpose(2, 0, 1, 3)


def local(position, velocity, other_accel, phase_ids, counts):
    vmem = pl.BlockSpec(memory_space=pltpu.VMEM)
    hbm = pl.BlockSpec(memory_space=pl.ANY)
    dma = pltpu.SemaphoreType.DMA
    n1 = lax.axis_size("y") * lax.axis_size("core") - 1
    n2 = lax.axis_size("x") * lax.axis_size("zl") * lax.axis_size("zh") - 1
    packed = pl.pallas_call(
        kernel,
        out_shape=jax.ShapeDtypeStruct((OUT_ROWS, 128), f32),
        in_specs=[hbm] * 4 + [pl.BlockSpec(memory_space=pltpu.SMEM)],
        out_specs=vmem,
        scratch_shapes=[
            pltpu.VMEM((ROWS * COLS * 2, 128), f32),
            pltpu.VMEM((ROWS * COLS * 2, 128), f32),
            pltpu.VMEM((ROWS * COLS * 2, 128), f32),
            pltpu.VMEM((ROWS, COLS, 128), jnp.int32),
            pltpu.VMEM((15, ROWS, 8, 128), f32),
            pltpu.VMEM((2, BLOCKS, 8, 128), f32),
            pltpu.VMEM((6, BLOCKS, 8, 128), f32),
            pltpu.VMEM((3, BLOCKS, 8, 128), f32),
            pltpu.VMEM((2, 6, 8, 128), f32),
            pltpu.VMEM((2, 3, 8, 128), f32),
            pltpu.VMEM((4, 8, 128), f32),
            pltpu.VMEM((4, 8, 128), f32),
            pltpu.VMEM((4, 6, 8, 128), f32),
            pltpu.VMEM((4, 3, 8, 128), f32),
            pltpu.VMEM((4, 8, 128), f32),
            pltpu.VMEM((4, 8, 128), f32),
            pltpu.VMEM((32 * FS, 128), f32),
            pltpu.VMEM((32 * FS, 128), f32),
            pltpu.VMEM((16, 128, 128), bf16),
            pltpu.VMEM((4, 128, 128), bf16),
            pltpu.VMEM((162, 128, 256), f32),
            pltpu.VMEM((ROWS * COLS, 128, 128), f32),
            pltpu.VMEM((ROWS * 64, 128), f32),
            pltpu.VMEM((ROWS, COLS, 32, 128), f32),
            pltpu.VMEM((BLOCKS, 8, 32, 128), bf16),
            pltpu.VMEM((16 * FS, 128), f32),
            pltpu.VMEM((9, 16, 128), f32),
            pltpu.VMEM((9, 16, 128), f32),
            pltpu.VMEM((2, 8, 128), f32),
            pltpu.VMEM((2, 2, 1, 128), f32),
            pltpu.VMEM((2, n1, 1, 128), f32),
            pltpu.VMEM((2, n2, 1, 128), f32),
            dma((4,)), dma((8,)), dma((8,)), dma((8,)), dma((8,)),
            dma((2, n1)), dma((2, n1)), dma((2, n2)), dma((2, n2)),
        ],
        compiler_params=pltpu.CompilerParams(
            collective_id=0, has_side_effects=True, vmem_limit_bytes=60 * 1024 * 1024
        ),
    )(flat(position), flat(velocity), flat(other_accel), phase_ids, counts)
    new_pos, new_vel, pressure, monitor = pl.pallas_call(
        spread,
        out_shape=(
            jax.ShapeDtypeStruct((ROWS * COLS * 2, 128), f32),
            jax.ShapeDtypeStruct((ROWS * COLS * 2, 128), f32),
            jax.ShapeDtypeStruct((ROWS, COLS, 128), f32),
            jax.ShapeDtypeStruct((ITERS, 4), f32),
        ),
        in_specs=[vmem],
        out_specs=[vmem] * 4,
        compiler_params=pltpu.CompilerParams(vmem_limit_bytes=4 * 1024 * 1024),
    )(packed)
    return unflat(new_pos), unflat(new_vel), pressure, monitor


def solution(mesh):
    gx = ("x", "zl")
    gy = ("zh", "y", "core")
    torus = Mesh(mesh.devices.reshape(4, 2, 2, 4, 2), SPLIT)
    wide = P(None, gx, gy, None)
    return jax.shard_map(
        local, mesh=torus, in_specs=(wide, wide, wide, P(gx, gy, None), P(gx, gy)),
        out_specs=(wide, wide, P(gx, gy, None), P()), check_vma=False,
    )
```

```python
import jax
import jax.numpy as jnp
from jax import lax
from jax.experimental import pallas as pl
from jax.experimental.pallas import tpu as pltpu
from jax.sharding import Mesh
from jax.sharding import PartitionSpec as P

ITERS = 4
TIME_STEP = 0.05
KERNEL_NORM = 4.0 / (3.141592653589793 * 64.0)
REST_LIGHT = 1.2
REST_HEAVY = 1.5
STIFF_LIGHT = 100.0
STIFF_HEAVY = 200.0
MASS_LIGHT = 1.0
MASS_HEAVY = 1.5
FAR = float(2**30)
NEG = -1e30
MESH = pl.DeviceIdType.MESH
SPLIT = ("x", "zl", "zh", "y", "core")
ROWS = 6
COLS = 6
TOP, BOTTOM, LEFT, RIGHT, CORNERS = 0, 7, 8, 9, 10
EDGES = (TOP, BOTTOM, LEFT, RIGHT)
BLOCKS = 11
FS = BLOCKS * 8
DIRS = ((-1, 0), (1, 0), (0, -1), (0, 1), (-1, -1), (-1, 1), (1, -1), (1, 1))
OWN_TILES = (
    (0, 1, 0, 1, 0), (0, 1, 1, 2, 0),
    (2, 3, 1, 2, 0), (2, 3, 2, 3, 0), (2, 3, 3, 4, 1),
    (4, 5, 3, 4, 1), (4, 5, 4, 5, 1),
    (1, 4, 0, 5, 2),
)
ROW_TILES = (
    (0, 1, 0, 1, 0), (0, 1, 1, 2, 0), (2, 2, 2, 3, 0),
    (3, 4, 3, 4, 1), (3, 4, 4, 5, 1), (5, None, 5, None, 1),
)
GROUP_START = (0, 2)
UNROLL_DENSITY = 5
FORCE_FIRST = 4
EDGE_FIRST = 9
OUT_VELOCITY = ROWS * COLS * 2
OUT_PRESSURE = 2 * OUT_VELOCITY
OUT_MONITOR = OUT_PRESSURE + ROWS * 8
OUT_ROWS = OUT_MONITOR + 8

f32 = jnp.float32
bf16 = jnp.bfloat16


def rnd(v):
    return v.astype(bf16).astype(f32)


def split3(v):
    h = rnd(v)
    r = v - h
    m = rnd(r)
    return h, m, rnd(r - m)


def feature_rows(x, y):
    xs = split3(x)
    ys = split3(y)
    rs = split3(x * x + y * y)
    one = jnp.ones_like(x)
    zero = jnp.zeros_like(x)
    h, m, l = 0, 1, 2
    jrow = (
        [xs[q] for q in (h, h, m, m, l, h)] + [ys[q] for q in (h, h, m, m, l, h)]
        + list(rs) + [one, one, one] + list(xs) + list(ys) + [one] * 7 + [zero]
    )
    irow = (
        [2.0 * xs[q] for q in (h, m, h, m, h, l)] + [2.0 * ys[q] for q in (h, m, h, m, h, l)]
        + [-one] * 3 + [-q for q in rs] + [zero] * 6 + list(xs) + list(ys) + [zero, zero]
    )
    return jrow, irow


def kernel(
    pos_ref, vel_ref, oa_ref, phase_ref, counts_ref,
    out_ref,
    inp, inv, ino, inph, st, xp, bp, tp, stage, tstage, cstage, ctstage, rb, trb, crb, ctrb,
    fb, ib, lt, gh, wb, aj, da, fa, tf, mb, al, be, rl, ar0, ar1, ar2,
    ins, hs, hr, ts, tr, a1s, a1r, a2s, a2r,
):
    index = {name: lax.axis_index(name) for name in SPLIT}
    size = {name: lax.axis_size(name) for name in SPLIT}
    gx = index["x"] * size["zl"] + index["zl"]
    gy = (index["zh"] * size["y"] + index["y"]) * size["core"] + index["core"]
    nx = size["x"] * size["zl"]
    ny = size["zh"] * size["y"] * size["core"]

    def around(dx, dy):
        px = lax.rem(gx + dx + nx, nx)
        py = lax.rem(gy + dy + ny, ny)
        return (
            px // size["zl"], lax.rem(px, size["zl"]), py // (size["y"] * size["core"]),
            lax.rem(py // size["core"], size["y"]), lax.rem(py, size["core"]),
        )

    def peers(names):
        steps = [()]
        for name in SPLIT:
            count = size[name] if name in names else 1
            steps = [s + (q,) for s in steps for q in range(count)]
        return [
            tuple(lax.rem(index[name] + q, size[name]) for name, q in zip(SPLIT, s))
            for s in steps if any(s)
        ]

    neighbours = [around(dx, dy) for dx, dy in DIRS]
    first_peers = peers(("y", "core"))
    second_peers = peers(("x", "zl", "zh"))
    barrier = pltpu.get_barrier_semaphore()
    for partner in neighbours + first_peers + second_peers:
        pl.semaphore_signal(barrier, inc=1, device_id=partner, device_id_type=MESH)

    loads = [
        pltpu.make_async_copy(src, dst, ins.at[q])
        for q, (src, dst) in enumerate(
            ((pos_ref, inp), (vel_ref, inv), (oa_ref, ino), (phase_ref, inph))
        )
    ]
    for load in loads:
        load.start()

    st[...] = jnp.zeros_like(st)
    da[...] = jnp.zeros_like(da)
    mb[...] = jnp.zeros_like(mb)
    xp[...] = jnp.full_like(xp, FAR)
    tp[...] = jnp.zeros_like(tp)
    fb[...] = jnp.zeros_like(fb)
    aj[...] = jnp.zeros_like(aj)
    bp[...] = jnp.zeros_like(bp)
    rl[...] = jnp.zeros_like(rl)
    for buf in (stage, tstage, cstage, ctstage):
        buf[...] = jnp.zeros_like(buf)
    k = lax.broadcasted_iota(jnp.int32, (16, 128), 0)
    for ox in (-1, 0, 1):
        for oy in (-1, 0, 1):
            o = (ox + 1) * 3 + oy + 1
            al[o] = jnp.where(
                k < 2, 1.0,
                jnp.where((k >= 8) & (k < 11), 2.0 * ox, jnp.where((k >= 11) & (k < 14), 2.0 * oy, 0.0)),
            )
            be[o] = jnp.where(
                (k >= 2) & (k < 5), -2.0 * ox,
                jnp.where(
                    (k >= 5) & (k < 8), -2.0 * oy, jnp.where(k == 14, 1.0 - ox * ox - oy * oy, 0.0)
                ),
            )
    lane = lax.broadcasted_iota(jnp.int32, (1, 128), 1)
    sub = lax.broadcasted_iota(jnp.int32, (8, 128), 0)
    sub_f = sub.astype(f32)
    row_cols = jnp.where(sub == 7, -1.0, sub_f) - 2.5
    for load in loads:
        load.wait()
    for a in range(ROWS):
        for f in range(2):
            for s in range(COLS):
                at = a * 12 + s * 2 + f
                st[f, a, s : s + 1, :] = inp[at : at + 1, :]
                st[2 + f, a, s : s + 1, :] = inv[at : at + 1, :]
                st[13 + f, a, s : s + 1, :] = ino[at : at + 1, :]
        for s in range(COLS):
            st[4, a, s : s + 1, :] = (lane < counts_ref[a, s]).astype(f32)
        st[5, a, 0:COLS, :] = (inph[a] == 1).astype(f32)

    def halo_copies(src, staged, corners, dst, cdst, send, recv):
        edges = []
        diagonals = []
        for d in range(8):
            if d < 4:
                source = src.at[:, (1, ROWS)[d]] if d < 2 else staged.at[d - 2]
                target = dst.at[d]
            else:
                source, target = corners.at[d - 4], cdst.at[d - 4]
            (edges if d < 4 else diagonals).append(
                pltpu.make_async_remote_copy(
                    src_ref=source, dst_ref=target, send_sem=send.at[d], recv_sem=recv.at[d],
                    device_id=neighbours[d], device_id_type=MESH,
                )
            )
        return diagonals, edges

    def pack(src, staged, corners, fields):
        for f in range(fields):
            corners[0, f : f + 1, :] = src[f, 1, 0:1, :]
            corners[1, f : f + 1, :] = src[f, 1, COLS - 1 : COLS, :]
            corners[2, f : f + 1, :] = src[f, ROWS, 0:1, :]
            corners[3, f : f + 1, :] = src[f, ROWS, COLS - 1 : COLS, :]
            for a in range(ROWS):
                staged[0, f, a : a + 1, :] = src[f, a + 1, 0:1, :]
                staged[1, f, a : a + 1, :] = src[f, a + 1, COLS - 1 : COLS, :]

    PLACE = (3, 2, 1, 0)

    def put(buf, rows, base):
        for q, row in enumerate(rows):
            buf[pl.ds(q * FS + base, 8), :] = row

    def cell(buf, c):
        return buf[pl.ds(c, 32, stride=FS), :]

    def turned(cells):
        return jnp.concatenate([cell(fb, c) for c in cells], axis=0).astype(bf16).T

    def centre(a, col, o):
        base = cell(ib, (a + 1) * 8 + col)
        return jnp.concatenate([base[0:16], base[16:32] * al[o] + be[o]], axis=0).astype(bf16)

    def at_block(part, block, blocks):
        pieces = []
        if block > 0:
            pieces.append(jnp.zeros((32 * block, 128), bf16))
        pieces.append(part)
        if block < blocks - 1:
            pieces.append(jnp.zeros((32 * (blocks - 1 - block), 128), bf16))
        return jnp.concatenate(pieces, axis=0) if len(pieces) > 1 else part

    def collect(sums, col, part):
        if col is not None:
            sums[col] = part if sums[col] is None else sums[col] + part

    def overlap(left, right, slot, sums, cols, mirrors=(None, None)):
        w = jnp.maximum(jnp.dot(left, right, preferred_element_type=f32), 0.0)
        w2 = w * w
        wb[slot] = w2
        w3 = w2 * w
        part = jnp.sum(w3.reshape(16, 8, 256), axis=0)
        for e in range(2):
            collect(sums, cols[e], part[:, 128 * e : 128 * e + 128])
            if mirrors[e] is not None:
                aj[mirrors[e]] += w3[:, 128 * e : 128 * e + 128]

    def own_tiles(a, ox3, lrow, slot, sums, tiles=OWN_TILES, mirror_row=None):
        for q, (ca, cb, ja, jb, group) in enumerate(tiles):
            blocks = 8 if group == 2 else 4
            halves = []
            mirrors = []
            for col, j, e in ((ca, ja, 0), (cb, jb, 1)):
                if col is None:
                    halves.append(jnp.zeros((32 * blocks, 128), bf16))
                    mirrors.append(None)
                    continue
                block = (j + 2 * e if group == 2 else j - GROUP_START[group])
                halves.append(at_block(centre(a, col, ox3 + (j - col + 1)), block, blocks))
                keep = mirror_row is not None and not (tiles is ROW_TILES and col == j)
                mirrors.append(mirror_row * COLS + j if keep else None)
            left = jnp.concatenate([lrow[0], lrow[1]], axis=1) if group == 2 else lrow[group]
            overlap(left, jnp.concatenate(halves, axis=1), slot + q, sums, (ca, cb), mirrors)

    def edge_tile(a, ox3, r, slot, sums):
        pa = centre(a, 0, ox3)
        pb = centre(a, COLS - 1, ox3 + 2)
        group, odd = divmod(r, 2) if 0 <= r < ROWS else (3, int(r >= ROWS))
        right = jnp.concatenate([at_block(pa, 2 * odd, 4), at_block(pb, 2 * odd + 1, 4)], axis=1)
        overlap(gh[group], right, slot + 8, sums, (0, COLS - 1))

    def halves_of(w2):
        hi = w2.astype(bf16)
        return hi, (w2 - hi.astype(f32)).astype(bf16)

    def pull(hi, lo, left, sums, cols):
        both = jnp.concatenate([left, left], axis=1)
        total = jnp.dot(both, jnp.concatenate([hi, lo], axis=0), preferred_element_type=f32)
        for e in range(2):
            collect(sums, cols[e], total[32 * e : 32 * e + 32, 128 * e : 128 * e + 128])

    def pair_rows(block, ca, cb):
        return jnp.concatenate([tf[block, ca], tf[block, ca if cb is None else cb]], axis=0)

    def own_pulls(r, slot, sums, a=None, mirrored=None, tiles=OWN_TILES):
        for q, (ca, cb, ja, jb, group) in enumerate(tiles):
            hi, lo = halves_of(wb[slot + q])
            pull(hi, lo, pair_rows(r, ja, jb), sums, (ca, cb))
            if mirrored is None:
                continue
            row = tiles is ROW_TILES
            cols = tuple(None if row and c == j else j for c, j in ((ca, ja), (cb, jb)))
            if cols == (None, None):
                continue
            turn = [
                jnp.concatenate([v[:, 0:128].T, v[:, 128:256].T], axis=1) for v in (hi, lo)
            ]
            pull(turn[0], turn[1], pair_rows(a, ca, cb), mirrored, cols)

    def side_cells(r):
        if r < 0:
            return (CORNERS, 0), (CORNERS, 1)
        if r >= ROWS:
            return (CORNERS, 2), (CORNERS, 3)
        return (LEFT, r), (RIGHT, r)

    def moment_rows(block, px, py):
        rows = [None] * 32
        for q in range(4):
            field = None if q == 0 else tp[q - 1, block]
            for e, p in enumerate((px, py)):
                pieces = split3(p if field is None else p * field)
                for level in range(3):
                    rows[level * 8 + 2 * q + e] = pieces[level]
            if field is None:
                rows[24], rows[28] = jnp.ones_like(px), jnp.zeros_like(px)
            else:
                rows[24 + q] = rnd(field)
                rows[28 + q] = rnd(field - rows[24 + q])
        return rows

    position_copies = halo_copies(bp, stage, cstage, rb, crb, hs, hr)
    term_copies = halo_copies(tp, tstage, ctstage, trb, ctrb, ts, tr)

    def start(pair):
        for copy in pair[0] + pair[1]:
            copy.start()

    def coefficients():
        alive = st[4] > 0.5
        for f in range(2):
            free = st[f] + TIME_STEP * (st[2 + f] + TIME_STEP * st[13 + f]) - 0.5
            step = TIME_STEP * TIME_STEP
            bp[3 * f, 1 : ROWS + 1] = jnp.where(alive, free + step * st[7 + 3 * f], FAR)
            bp[3 * f + 1, 1 : ROWS + 1] = step * st[8 + 3 * f]
            bp[3 * f + 2, 1 : ROWS + 1] = step * st[9 + 3 * f]
        pack(bp, stage, cstage, 6)

    def side_tiles(which):
        done = []
        for t in range(18):
            a, ox = t // 3, t % 3 - 1
            r = a + ox
            outside = r < 0 or r >= ROWS
            if which == "edges" and outside:
                done.append((t, a, ox, r, True))
            if outside == (which == "corners"):
                done.append((t, a, ox, r, False))
        return done

    def add_up(buf, a, sums):
        for s in range(COLS):
            if sums[s] is not None:
                buf[a, s] += sums[s]

    def densities(it):
        relax0, relax1 = rl[0], rl[1]
        for f in range(2):
            for r in range(ROWS):
                xp[f, r + 1] = bp[3 * f, r + 1] + relax0 * bp[3 * f + 1, r + 1] + relax1 * bp[3 * f + 2, r + 1]
        for r in range(ROWS):
            jrow, irow = feature_rows(xp[0, r + 1], xp[1, r + 1])
            put(fb, jrow, (r + 1) * 8)
            put(ib, irow, (r + 1) * 8)
        for r in range(ROWS):
            for g in range(2):
                lt[(r + 1) * 2 + g] = turned([(r + 1) * 8 + GROUP_START[g] + s for s in range(4)])
        def row_with_itself(a, sums):
            own_tiles(a, 3, (lt[(a + 1) * 2], lt[(a + 1) * 2 + 1]), (3 * a + 1) * 9, sums, ROW_TILES, a)
            for s in range(COLS):
                block = aj[a * COLS + s].T
                aj[a * COLS + s] = jnp.zeros((128, 128), f32)
                collect(sums, s, jnp.sum(block.reshape(16, 8, 128), axis=0))

        def keep(a, sums):
            for s in range(COLS):
                da[pl.ds(a * 64 + s * 8, 8), :] = sums[s]

        def density(a, c):
            sums = [None] * COLS
            row_with_itself(a, sums)
            own_tiles(
                a, 6, (lt[(a + 2) * 2], lt[(a + 2) * 2 + 1]), (3 * a + 2) * 9, sums, OWN_TILES, a + 1
            )
            keep(a, sums)
            return c

        lax.fori_loop(0, ROWS - 1, density, 0, unroll=UNROLL_DENSITY)
        diagonals, edges = position_copies
        for copy in edges:
            copy.wait()
        for d, block in enumerate((BOTTOM, TOP, RIGHT, LEFT)):
            for f in range(2):
                xp[f, block] = rb[d, 3 * f] + relax0 * rb[d, 3 * f + 1] + relax1 * rb[d, 3 * f + 2]
        for block in EDGES:
            jrow, _ = feature_rows(xp[0, block], xp[1, block])
            put(fb, jrow, block * 8)
        for block in (TOP, BOTTOM):
            for g in range(2):
                lt[block * 2 + g] = turned([block * 8 + GROUP_START[g] + s for s in range(4)])
        for q in range(3):
            gh[q] = turned([b * 8 + s for r in (2 * q, 2 * q + 1) for b, s in side_cells(r)])
        sums = [None] * COLS
        row_with_itself(ROWS - 1, sums)
        keep(ROWS - 1, sums)

        def side_density(tiles):
            for t, a, ox, r, row in tiles:
                sums = [None] * COLS
                if row:
                    own_tiles(a, (ox + 1) * 3, (lt[(r + 1) * 2], lt[(r + 1) * 2 + 1]), t * 9, sums)
                else:
                    edge_tile(a, (ox + 1) * 3, r, t * 9, sums)
                for s in range(COLS):
                    if sums[s] is not None:
                        da[a * 64 + s * 8 : a * 64 + s * 8 + 8, :] += sums[s]

        edge_tiles = side_tiles("edges")
        side_density(edge_tiles[:EDGE_FIRST])
        for copy in diagonals:
            copy.wait()
        for d in range(4):
            for f in range(2):
                xp[f, CORNERS, PLACE[d] : PLACE[d] + 1, :] = (
                    crb[d, 3 * f : 3 * f + 1, :] + relax0[0:1] * crb[d, 3 * f + 1 : 3 * f + 2, :]
                    + relax1[0:1] * crb[d, 3 * f + 2 : 3 * f + 3, :]
                )
        jrow, _ = feature_rows(xp[0, CORNERS], xp[1, CORNERS])
        put(fb, jrow, CORNERS * 8)
        gh[3] = turned([CORNERS * 8 + q for q in range(4)])
        side_density(edge_tiles[EDGE_FIRST:-1] + side_tiles("corners") + edge_tiles[-1:])

    def bounds_copies(now, src_slot, dst, send, recv, targets):
        return [
            pltpu.make_async_remote_copy(
                src_ref=ar0.at[now, src_slot], dst_ref=dst.at[now, d],
                send_sem=send.at[now, d], recv_sem=recv.at[now, d],
                device_id=target, device_id_type=MESH,
            )
            for d, target in enumerate(targets)
        ]

    def forces(it):
        now = lax.rem(it, 2)
        alive = st[4] > 0.5
        hot = st[5] > 0.5
        rows = []
        for a in range(ROWS):
            parts = [da[pl.ds(a * 64 + q, 8, stride=8), :] for q in range(8)]
            while len(parts) > 1:
                parts = [parts[q] + parts[q + 1] for q in range(0, len(parts), 2)]
            rows.append(parts[0])
        density_now = KERNEL_NORM * jnp.stack(rows)
        ratio = density_now / jnp.where(hot, REST_HEAVY, REST_LIGHT)
        lit = alive & jnp.logical_not(hot)
        hvy = alive & hot
        peaks = (
            jnp.where(lit, ratio, NEG), jnp.where(hvy, ratio, NEG),
            jnp.where(lit, -ratio, NEG), jnp.where(hvy, -ratio, NEG),
        )
        vec = jnp.full((1, 128), NEG, f32)
        for q in range(4):
            top = jnp.max(jnp.max(peaks[q], axis=0), axis=0, keepdims=True)
            top = jnp.max(top, axis=1, keepdims=True)
            vec = jnp.where(lane == q, top, vec)
        ar0[now, 0] = vec
        first = bounds_copies(now, 0, ar1, a1s, a1r, first_peers)
        for copy in first:
            copy.start()

        safe = jnp.where(alive, density_now, 1.0)
        inverse = 1.0 / (safe * safe)
        excess = jnp.where(hot, STIFF_HEAVY, STIFF_LIGHT) * (ratio - 1.0)
        t0 = jnp.where(alive, st[6] * inverse, 0.0)
        u = excess * inverse
        u0 = jnp.where(lit, u, 0.0)
        u1 = jnp.where(hvy, u, 0.0)
        tp[0, 1 : ROWS + 1] = t0
        tp[1, 1 : ROWS + 1] = u0
        tp[2, 1 : ROWS + 1] = u1
        pack(tp, tstage, ctstage, 3)
        start(term_copies)

        for a in range(ROWS):
            put(fb, moment_rows(a + 1, xp[0, a + 1] + (a - 2.5), xp[1, a + 1] + row_cols), (a + 1) * 8)
        for a in range(ROWS):
            for s in range(COLS):
                tf[a + 1, s] = cell(fb, (a + 1) * 8 + s).astype(bf16)

        def force(a, c):
            here = [None] * COLS
            below = [None] * COLS
            own_pulls(a + 1, (3 * a + 1) * 9, here, a + 1, here, ROW_TILES)
            own_pulls(a + 2, (3 * a + 2) * 9, here, a + 1, below, OWN_TILES)
            for s in range(COLS):
                fa[a, s] += here[s]
                fa[a + 1, s] = below[s]
            return c

        for s in range(COLS):
            fa[0, s] = jnp.zeros((32, 128), f32)
        lax.fori_loop(0, FORCE_FIRST, force, 0)
        for copy in first:
            copy.wait()
        best = vec
        for d in range(len(first_peers)):
            best = jnp.maximum(best, ar1[now, d])
        ar0[now, 1] = best
        second = bounds_copies(now, 1, ar2, a2s, a2r, second_peers)
        for copy in second:
            copy.start()

        lax.fori_loop(FORCE_FIRST, ROWS - 1, force, 0)
        here = [None] * COLS
        own_pulls(ROWS, (3 * ROWS - 2) * 9, here, ROWS, here, ROW_TILES)
        add_up(fa, ROWS - 1, here)

        diagonals, edges = term_copies
        for copy in edges:
            copy.wait()
        for d, block in enumerate((BOTTOM, TOP, RIGHT, LEFT)):
            for f in range(3):
                tp[f, block] = trb[d, f]
        edge_x = {TOP: -3.5, BOTTOM: 3.5, LEFT: sub_f - 2.5, RIGHT: sub_f - 2.5}
        edge_y = {TOP: row_cols, BOTTOM: row_cols, LEFT: -3.5, RIGHT: 3.5}
        for block in EDGES:
            put(fb, moment_rows(block, xp[0, block] + edge_x[block], xp[1, block] + edge_y[block]), block * 8)
        for block in EDGES:
            for s in range(ROWS):
                tf[block, s] = cell(fb, block * 8 + s).astype(bf16)

        def side_pull(t, r, sums):
            (lb, ls), (ub, us) = side_cells(r)
            hi, lo = halves_of(wb[t * 9 + 8])
            pull(hi, lo, jnp.concatenate([tf[lb, ls], tf[ub, us]], axis=0), sums, (0, COLS - 1))

        for t, a, ox, r, row in side_tiles("edges"):
            sums = [None] * COLS
            if row:
                own_pulls(r + 1, t * 9, sums)
            else:
                side_pull(t, r, sums)
            add_up(fa, a, sums)

        for copy in diagonals:
            copy.wait()
        for d in range(4):
            for f in range(3):
                tp[f, CORNERS, PLACE[d] : PLACE[d] + 1, :] = ctrb[d, f : f + 1, :]
        corner_x = jnp.where(sub < 2, -3.5, 3.5)
        corner_y = jnp.where(lax.rem(sub, 2) == 0, -3.5, 3.5)
        put(fb, moment_rows(CORNERS, xp[0, CORNERS] + corner_x, xp[1, CORNERS] + corner_y), CORNERS * 8)
        for s in range(4):
            tf[CORNERS, s] = cell(fb, CORNERS * 8 + s).astype(bf16)
        for t, a, ox, r, row in side_tiles("corners"):
            sums = [None] * COLS
            side_pull(t, r, sums)
            add_up(fa, a, sums)

        for a in range(ROWS):
            for s in range(COLS):
                part = fa[a, s]
                row = a * 8 + s
                mb[pl.ds(row, 8, stride=FS), :] = part[0:8] + part[8:16] + part[16:24]
                mb[pl.ds(8 * FS + row, 8, stride=FS), :] = part[24:32]

        for a in range(ROWS):
            def mom(q):
                return mb[q * FS + a * 8 : q * FS + a * 8 + 8, :]

            s1 = mom(8) + mom(12)
            factor = jnp.where(
                alive[a], 6.0 * KERNEL_NORM / jnp.where(hot[a], MASS_HEAVY, MASS_LIGHT), 0.0
            )
            for f in range(2):
                p = xp[f, a + 1] + (a - 2.5 if f == 0 else row_cols)
                arm = p * s1 - mom(f)
                for q, term in enumerate((t0[a], u0[a], u1[a])):
                    push = term * arm + p * (mom(9 + q) + mom(13 + q)) - mom(2 + 2 * q + f)
                    st[7 + 3 * f + q, a] = jnp.where(alive[a], factor * push, 0.0)

        @pl.when(it < ITERS - 1)
        def _():
            coefficients()
            start(position_copies)

        for copy in second:
            copy.wait()
        for d in range(len(second_peers)):
            best = jnp.maximum(best, ar2[now, d])
        out_ref[pl.ds(OUT_MONITOR + it, 1), :] = jnp.where(lane < 2, best, -best)
        relax0 = jnp.broadcast_to(1.0 / (1.0 + best[:, 0:1] + best[:, 2:3]), (8, 128))
        relax1 = jnp.broadcast_to(1.0 / (1.0 + best[:, 1:2] + best[:, 3:4]), (8, 128))
        rl[0] = relax0
        rl[1] = relax1
        for a in range(ROWS):
            relax = jnp.where(hot[a], relax1, relax0)
            st[6, a] = jnp.where(alive[a], st[6, a] + relax * excess[a], 0.0)

    coefficients()
    pl.semaphore_wait(barrier, len(neighbours) + len(first_peers) + len(second_peers))
    start(position_copies)

    def whole(it, carry):
        densities(it)
        forces(it)
        return carry

    lax.fori_loop(0, ITERS, whole, 0)

    for a in range(ROWS):
        live = st[4, a]
        for f in range(2):
            accel = st[7 + 3 * f, a] + rl[0] * st[8 + 3 * f, a] + rl[1] * st[9 + 3 * f, a]
            v = live * (st[2 + f, a] + TIME_STEP * (st[13 + f, a] + accel))
            p = live * (st[f, a] + TIME_STEP * v)
            out_ref[pl.ds(a * 12 + f, COLS, stride=2), :] = p[0:COLS]
            out_ref[pl.ds(OUT_VELOCITY + a * 12 + f, COLS, stride=2), :] = v[0:COLS]
        out_ref[OUT_PRESSURE + a * 8 : OUT_PRESSURE + a * 8 + 8, :] = st[6, a]


def spread(in_ref, npos_ref, nvel_ref, pres_ref, mon_ref, rest, sems):
    copies = [
        pltpu.make_async_copy(in_ref.at[pl.ds(first, out.shape[0])], out, sems.at[q])
        for q, (first, out) in enumerate(((0, npos_ref), (OUT_VELOCITY, nvel_ref), (OUT_PRESSURE, rest)))
    ]
    for copy in copies:
        copy.start()
    for copy in copies:
        copy.wait()
    for a in range(ROWS):
        pres_ref[a] = rest[a * 8 : a * 8 + COLS, :]
    mon_ref[...] = rest[ROWS * 8 : ROWS * 8 + ITERS, 0:4]


def flat(value):
    return value.transpose(1, 2, 0, 3).reshape(ROWS * COLS * 2, 128)


def unflat(value):
    return value.reshape(ROWS, COLS, 2, 128).transpose(2, 0, 1, 3)


def local(position, velocity, other_accel, phase_ids, counts):
    vmem = pl.BlockSpec(memory_space=pltpu.VMEM)
    hbm = pl.BlockSpec(memory_space=pl.ANY)
    dma = pltpu.SemaphoreType.DMA
    n1 = lax.axis_size("y") * lax.axis_size("core") - 1
    n2 = lax.axis_size("x") * lax.axis_size("zl") * lax.axis_size("zh") - 1
    packed = pl.pallas_call(
        kernel,
        out_shape=jax.ShapeDtypeStruct((OUT_ROWS, 128), f32),
        in_specs=[hbm] * 4 + [pl.BlockSpec(memory_space=pltpu.SMEM)],
        out_specs=vmem,
        scratch_shapes=[
            pltpu.VMEM((ROWS * COLS * 2, 128), f32),
            pltpu.VMEM((ROWS * COLS * 2, 128), f32),
            pltpu.VMEM((ROWS * COLS * 2, 128), f32),
            pltpu.VMEM((ROWS, COLS, 128), jnp.int32),
            pltpu.VMEM((15, ROWS, 8, 128), f32),
            pltpu.VMEM((2, BLOCKS, 8, 128), f32),
            pltpu.VMEM((6, BLOCKS, 8, 128), f32),
            pltpu.VMEM((3, BLOCKS, 8, 128), f32),
            pltpu.VMEM((2, 6, 8, 128), f32),
            pltpu.VMEM((2, 3, 8, 128), f32),
            pltpu.VMEM((4, 8, 128), f32),
            pltpu.VMEM((4, 8, 128), f32),
            pltpu.VMEM((4, 6, 8, 128), f32),
            pltpu.VMEM((4, 3, 8, 128), f32),
            pltpu.VMEM((4, 8, 128), f32),
            pltpu.VMEM((4, 8, 128), f32),
            pltpu.VMEM((32 * FS, 128), f32),
            pltpu.VMEM((32 * FS, 128), f32),
            pltpu.VMEM((16, 128, 128), bf16),
            pltpu.VMEM((4, 128, 128), bf16),
            pltpu.VMEM((162, 128, 256), f32),
            pltpu.VMEM((ROWS * COLS, 128, 128), f32),
            pltpu.VMEM((ROWS * 64, 128), f32),
            pltpu.VMEM((ROWS, COLS, 32, 128), f32),
            pltpu.VMEM((BLOCKS, 8, 32, 128), bf16),
            pltpu.VMEM((16 * FS, 128), f32),
            pltpu.VMEM((9, 16, 128), f32),
            pltpu.VMEM((9, 16, 128), f32),
            pltpu.VMEM((2, 8, 128), f32),
            pltpu.VMEM((2, 2, 1, 128), f32),
            pltpu.VMEM((2, n1, 1, 128), f32),
            pltpu.VMEM((2, n2, 1, 128), f32),
            dma((4,)), dma((8,)), dma((8,)), dma((8,)), dma((8,)),
            dma((2, n1)), dma((2, n1)), dma((2, n2)), dma((2, n2)),
        ],
        compiler_params=pltpu.CompilerParams(
            collective_id=0, has_side_effects=True, vmem_limit_bytes=60 * 1024 * 1024
        ),
    )(flat(position), flat(velocity), flat(other_accel), phase_ids, counts)
    new_pos, new_vel, pressure, monitor = pl.pallas_call(
        spread,
        out_shape=(
            jax.ShapeDtypeStruct((ROWS * COLS * 2, 128), f32),
            jax.ShapeDtypeStruct((ROWS * COLS * 2, 128), f32),
            jax.ShapeDtypeStruct((ROWS, COLS, 128), f32),
            jax.ShapeDtypeStruct((ITERS, 4), f32),
        ),
        in_specs=[hbm],
        out_specs=[vmem] * 4,
        scratch_shapes=[pltpu.VMEM((OUT_ROWS - OUT_PRESSURE, 128), f32), dma((3,))],
        compiler_params=pltpu.CompilerParams(vmem_limit_bytes=60 * 1024 * 1024),
    )(packed)
    return unflat(new_pos), unflat(new_vel), pressure, monitor


def solution(mesh):
    gx = ("x", "zl")
    gy = ("zh", "y", "core")
    torus = Mesh(mesh.devices.reshape(4, 2, 2, 4, 2), SPLIT)
    wide = P(None, gx, gy, None)
    return jax.shard_map(
        local, mesh=torus, in_specs=(wide, wide, wide, P(gx, gy, None), P(gx, gy)),
        out_specs=(wide, wide, P(gx, gy, None), P()), check_vma=False,
    )
```

```python
import jax
import jax.numpy as jnp
from jax import lax
from jax.experimental import pallas as pl
from jax.experimental.pallas import tpu as pltpu
from jax.sharding import Mesh
from jax.sharding import PartitionSpec as P

ITERS = 4
TIME_STEP = 0.05
KERNEL_NORM = 4.0 / (3.141592653589793 * 64.0)
REST_LIGHT = 1.2
REST_HEAVY = 1.5
STIFF_LIGHT = 100.0
STIFF_HEAVY = 200.0
MASS_LIGHT = 1.0
MASS_HEAVY = 1.5
FAR = float(2**30)
NEG = -1e30
MESH = pl.DeviceIdType.MESH
SPLIT = ("x", "zl", "zh", "y", "core")
ROWS = 6
COLS = 6
TOP, BOTTOM, LEFT, RIGHT, CORNERS = 0, 7, 8, 9, 10
EDGES = (TOP, BOTTOM, LEFT, RIGHT)
BLOCKS = 11
FS = BLOCKS * 8
DIRS = ((-1, 0), (1, 0), (0, -1), (0, 1), (-1, -1), (-1, 1), (1, -1), (1, 1))
OWN_TILES = (
    (0, 1, 0, 1, 0), (0, 1, 1, 2, 0),
    (2, 3, 1, 2, 0), (2, 3, 2, 3, 0), (2, 3, 3, 4, 1),
    (4, 5, 3, 4, 1), (4, 5, 4, 5, 1),
    (1, 4, 0, 5, 2),
)
ROW_TILES = (
    (0, 1, 0, 1, 0), (0, 1, 1, 2, 0), (2, 2, 2, 3, 0),
    (3, 4, 3, 4, 1), (3, 4, 4, 5, 1), (5, None, 5, None, 1),
)
GROUP_START = (0, 2)
UNROLL_DENSITY = 5
FORCE_FIRST = 4
EDGE_FIRST = 5
OUT_VELOCITY = ROWS * COLS * 2
OUT_PRESSURE = 2 * OUT_VELOCITY
OUT_MONITOR = OUT_PRESSURE + ROWS * 8
OUT_ROWS = OUT_MONITOR + 8

f32 = jnp.float32
bf16 = jnp.bfloat16


def rnd(v):
    return v.astype(bf16).astype(f32)


def split3(v):
    h = rnd(v)
    r = v - h
    m = rnd(r)
    return h, m, rnd(r - m)


def feature_rows(x, y):
    xs = split3(x)
    ys = split3(y)
    rs = split3(x * x + y * y)
    one = jnp.ones_like(x)
    zero = jnp.zeros_like(x)
    h, m, l = 0, 1, 2
    jrow = (
        [xs[q] for q in (h, h, m, m, l, h)] + [ys[q] for q in (h, h, m, m, l, h)]
        + list(rs) + [one, one, one] + list(xs) + list(ys) + [one] * 7 + [zero]
    )
    irow = (
        [2.0 * xs[q] for q in (h, m, h, m, h, l)] + [2.0 * ys[q] for q in (h, m, h, m, h, l)]
        + [-one] * 3 + [-q for q in rs] + [zero] * 6 + list(xs) + list(ys) + [zero, zero]
    )
    return jrow, irow


def kernel(
    pos_ref, vel_ref, oa_ref, phase_ref, counts_ref,
    out_ref,
    inp, inv, ino, inph, st, xp, bp, tp, stage, tstage, cstage, ctstage, rb, trb, crb, ctrb,
    fb, ib, lt, gh, wb, aj, da, fa, tf, mb, al, be, rl, ar0, ar1, ar2,
    ins, hs, hr, ts, tr, a1s, a1r, a2s, a2r,
):
    index = {name: lax.axis_index(name) for name in SPLIT}
    size = {name: lax.axis_size(name) for name in SPLIT}
    gx = index["x"] * size["zl"] + index["zl"]
    gy = (index["zh"] * size["y"] + index["y"]) * size["core"] + index["core"]
    nx = size["x"] * size["zl"]
    ny = size["zh"] * size["y"] * size["core"]

    def around(dx, dy):
        px = lax.rem(gx + dx + nx, nx)
        py = lax.rem(gy + dy + ny, ny)
        return (
            px // size["zl"], lax.rem(px, size["zl"]), py // (size["y"] * size["core"]),
            lax.rem(py // size["core"], size["y"]), lax.rem(py, size["core"]),
        )

    def peers(names):
        steps = [()]
        for name in SPLIT:
            count = size[name] if name in names else 1
            steps = [s + (q,) for s in steps for q in range(count)]
        return [
            tuple(lax.rem(index[name] + q, size[name]) for name, q in zip(SPLIT, s))
            for s in steps if any(s)
        ]

    neighbours = [around(dx, dy) for dx, dy in DIRS]
    first_peers = peers(("y", "core"))
    second_peers = peers(("x", "zl", "zh"))
    barrier = pltpu.get_barrier_semaphore()
    for partner in neighbours + first_peers + second_peers:
        pl.semaphore_signal(barrier, inc=1, device_id=partner, device_id_type=MESH)

    loads = [
        pltpu.make_async_copy(src, dst, ins.at[q])
        for q, (src, dst) in enumerate(
            ((pos_ref, inp), (vel_ref, inv), (oa_ref, ino), (phase_ref, inph))
        )
    ]
    for load in loads:
        load.start()

    st[...] = jnp.zeros_like(st)
    da[...] = jnp.zeros_like(da)
    mb[...] = jnp.zeros_like(mb)
    xp[...] = jnp.full_like(xp, FAR)
    tp[...] = jnp.zeros_like(tp)
    fb[...] = jnp.zeros_like(fb)
    aj[...] = jnp.zeros_like(aj)
    bp[...] = jnp.zeros_like(bp)
    rl[...] = jnp.zeros_like(rl)
    for buf in (stage, tstage, cstage, ctstage):
        buf[...] = jnp.zeros_like(buf)
    k = lax.broadcasted_iota(jnp.int32, (16, 128), 0)
    for ox in (-1, 0, 1):
        for oy in (-1, 0, 1):
            o = (ox + 1) * 3 + oy + 1
            al[o] = jnp.where(
                k < 2, 1.0,
                jnp.where((k >= 8) & (k < 11), 2.0 * ox, jnp.where((k >= 11) & (k < 14), 2.0 * oy, 0.0)),
            )
            be[o] = jnp.where(
                (k >= 2) & (k < 5), -2.0 * ox,
                jnp.where(
                    (k >= 5) & (k < 8), -2.0 * oy, jnp.where(k == 14, 1.0 - ox * ox - oy * oy, 0.0)
                ),
            )
    lane = lax.broadcasted_iota(jnp.int32, (1, 128), 1)
    sub = lax.broadcasted_iota(jnp.int32, (8, 128), 0)
    sub_f = sub.astype(f32)
    row_cols = jnp.where(sub == 7, -1.0, sub_f) - 2.5
    for load in loads:
        load.wait()
    for a in range(ROWS):
        for f in range(2):
            for s in range(COLS):
                at = a * 12 + s * 2 + f
                st[f, a, s : s + 1, :] = inp[at : at + 1, :]
                st[2 + f, a, s : s + 1, :] = inv[at : at + 1, :]
                st[13 + f, a, s : s + 1, :] = ino[at : at + 1, :]
        for s in range(COLS):
            st[4, a, s : s + 1, :] = (lane < counts_ref[a, s]).astype(f32)
        st[5, a, 0:COLS, :] = (inph[a] == 1).astype(f32)

    def halo_copies(src, staged, corners, dst, cdst, send, recv):
        edges = []
        diagonals = []
        for d in range(8):
            if d < 4:
                source = src.at[:, (1, ROWS)[d]] if d < 2 else staged.at[d - 2]
                target = dst.at[d]
            else:
                source, target = corners.at[d - 4], cdst.at[d - 4]
            (edges if d < 4 else diagonals).append(
                pltpu.make_async_remote_copy(
                    src_ref=source, dst_ref=target, send_sem=send.at[d], recv_sem=recv.at[d],
                    device_id=neighbours[d], device_id_type=MESH,
                )
            )
        return diagonals, edges

    def pack(src, staged, corners, fields):
        for f in range(fields):
            corners[0, f : f + 1, :] = src[f, 1, 0:1, :]
            corners[1, f : f + 1, :] = src[f, 1, COLS - 1 : COLS, :]
            corners[2, f : f + 1, :] = src[f, ROWS, 0:1, :]
            corners[3, f : f + 1, :] = src[f, ROWS, COLS - 1 : COLS, :]
            for a in range(ROWS):
                staged[0, f, a : a + 1, :] = src[f, a + 1, 0:1, :]
                staged[1, f, a : a + 1, :] = src[f, a + 1, COLS - 1 : COLS, :]

    PLACE = (3, 2, 1, 0)

    def put(buf, rows, base):
        for q, row in enumerate(rows):
            buf[pl.ds(q * FS + base, 8), :] = row

    def cell(buf, c):
        return buf[pl.ds(c, 32, stride=FS), :]

    def turned(cells):
        return jnp.concatenate([cell(fb, c) for c in cells], axis=0).astype(bf16).T

    def centre(a, col, o):
        base = cell(ib, (a + 1) * 8 + col)
        return jnp.concatenate([base[0:16], base[16:32] * al[o] + be[o]], axis=0).astype(bf16)

    def at_block(part, block, blocks):
        pieces = []
        if block > 0:
            pieces.append(jnp.zeros((32 * block, 128), bf16))
        pieces.append(part)
        if block < blocks - 1:
            pieces.append(jnp.zeros((32 * (blocks - 1 - block), 128), bf16))
        return jnp.concatenate(pieces, axis=0) if len(pieces) > 1 else part

    def collect(sums, col, part):
        if col is not None:
            sums[col] = part if sums[col] is None else sums[col] + part

    def overlap(left, right, slot, sums, cols, mirrors=(None, None)):
        w = jnp.maximum(jnp.dot(left, right, preferred_element_type=f32), 0.0)
        w2 = w * w
        wb[slot] = w2
        w3 = w2 * w
        part = jnp.sum(w3.reshape(16, 8, 256), axis=0)
        for e in range(2):
            collect(sums, cols[e], part[:, 128 * e : 128 * e + 128])
            if mirrors[e] is not None:
                aj[mirrors[e]] += w3[:, 128 * e : 128 * e + 128]

    def own_tiles(a, ox3, lrow, slot, sums, tiles=OWN_TILES, mirror_row=None):
        for q, (ca, cb, ja, jb, group) in enumerate(tiles):
            blocks = 8 if group == 2 else 4
            halves = []
            mirrors = []
            for col, j, e in ((ca, ja, 0), (cb, jb, 1)):
                if col is None:
                    halves.append(jnp.zeros((32 * blocks, 128), bf16))
                    mirrors.append(None)
                    continue
                block = (j + 2 * e if group == 2 else j - GROUP_START[group])
                halves.append(at_block(centre(a, col, ox3 + (j - col + 1)), block, blocks))
                keep = mirror_row is not None and not (tiles is ROW_TILES and col == j)
                mirrors.append(mirror_row * COLS + j if keep else None)
            left = jnp.concatenate([lrow[0], lrow[1]], axis=1) if group == 2 else lrow[group]
            overlap(left, jnp.concatenate(halves, axis=1), slot + q, sums, (ca, cb), mirrors)

    def edge_tile(a, ox3, r, slot, sums):
        pa = centre(a, 0, ox3)
        pb = centre(a, COLS - 1, ox3 + 2)
        group, odd = divmod(r, 2) if 0 <= r < ROWS else (3, int(r >= ROWS))
        right = jnp.concatenate([at_block(pa, 2 * odd, 4), at_block(pb, 2 * odd + 1, 4)], axis=1)
        overlap(gh[group], right, slot + 8, sums, (0, COLS - 1))

    def halves_of(w2):
        hi = w2.astype(bf16)
        return hi, (w2 - hi.astype(f32)).astype(bf16)

    def pull(hi, lo, left, sums, cols):
        both = jnp.concatenate([left, left], axis=1)
        total = jnp.dot(both, jnp.concatenate([hi, lo], axis=0), preferred_element_type=f32)
        for e in range(2):
            collect(sums, cols[e], total[32 * e : 32 * e + 32, 128 * e : 128 * e + 128])

    def pair_rows(block, ca, cb):
        return jnp.concatenate([tf[block, ca], tf[block, ca if cb is None else cb]], axis=0)

    def own_pulls(r, slot, sums, a=None, mirrored=None, tiles=OWN_TILES):
        for q, (ca, cb, ja, jb, group) in enumerate(tiles):
            hi, lo = halves_of(wb[slot + q])
            pull(hi, lo, pair_rows(r, ja, jb), sums, (ca, cb))
            if mirrored is None:
                continue
            row = tiles is ROW_TILES
            cols = tuple(None if row and c == j else j for c, j in ((ca, ja), (cb, jb)))
            if cols == (None, None):
                continue
            turn = [
                jnp.concatenate([v[:, 0:128].T, v[:, 128:256].T], axis=1) for v in (hi, lo)
            ]
            pull(turn[0], turn[1], pair_rows(a, ca, cb), mirrored, cols)

    def side_cells(r):
        if r < 0:
            return (CORNERS, 0), (CORNERS, 1)
        if r >= ROWS:
            return (CORNERS, 2), (CORNERS, 3)
        return (LEFT, r), (RIGHT, r)

    def moment_rows(block, px, py):
        rows = [None] * 32
        for q in range(4):
            field = None if q == 0 else tp[q - 1, block]
            for e, p in enumerate((px, py)):
                pieces = split3(p if field is None else p * field)
                for level in range(3):
                    rows[level * 8 + 2 * q + e] = pieces[level]
            if field is None:
                rows[24], rows[28] = jnp.ones_like(px), jnp.zeros_like(px)
            else:
                rows[24 + q] = rnd(field)
                rows[28 + q] = rnd(field - rows[24 + q])
        return rows

    position_copies = halo_copies(bp, stage, cstage, rb, crb, hs, hr)
    term_copies = halo_copies(tp, tstage, ctstage, trb, ctrb, ts, tr)

    def start(pair):
        for copy in pair[0] + pair[1]:
            copy.start()

    def coefficients():
        alive = st[4] > 0.5
        for f in range(2):
            free = st[f] + TIME_STEP * (st[2 + f] + TIME_STEP * st[13 + f]) - 0.5
            step = TIME_STEP * TIME_STEP
            bp[3 * f, 1 : ROWS + 1] = jnp.where(alive, free + step * st[7 + 3 * f], FAR)
            bp[3 * f + 1, 1 : ROWS + 1] = step * st[8 + 3 * f]
            bp[3 * f + 2, 1 : ROWS + 1] = step * st[9 + 3 * f]
        pack(bp, stage, cstage, 6)

    def side_tiles(which):
        done = []
        for t in range(18):
            a, ox = t // 3, t % 3 - 1
            r = a + ox
            outside = r < 0 or r >= ROWS
            if which == "edges" and outside:
                done.append((t, a, ox, r, True))
            if outside == (which == "corners"):
                done.append((t, a, ox, r, False))
        return done

    def add_up(buf, a, sums):
        for s in range(COLS):
            if sums[s] is not None:
                buf[a, s] += sums[s]

    def densities(it):
        relax0, relax1 = rl[0], rl[1]
        for f in range(2):
            for r in range(ROWS):
                xp[f, r + 1] = bp[3 * f, r + 1] + relax0 * bp[3 * f + 1, r + 1] + relax1 * bp[3 * f + 2, r + 1]
        for r in range(ROWS):
            jrow, irow = feature_rows(xp[0, r + 1], xp[1, r + 1])
            put(fb, jrow, (r + 1) * 8)
            put(ib, irow, (r + 1) * 8)
        for r in range(ROWS):
            for g in range(2):
                lt[(r + 1) * 2 + g] = turned([(r + 1) * 8 + GROUP_START[g] + s for s in range(4)])
        def row_with_itself(a, sums):
            own_tiles(a, 3, (lt[(a + 1) * 2], lt[(a + 1) * 2 + 1]), (3 * a + 1) * 9, sums, ROW_TILES, a)
            for s in range(COLS):
                block = aj[a * COLS + s].T
                aj[a * COLS + s] = jnp.zeros((128, 128), f32)
                collect(sums, s, jnp.sum(block.reshape(16, 8, 128), axis=0))

        def keep(a, sums):
            for s in range(COLS):
                da[pl.ds(a * 64 + s * 8, 8), :] = sums[s]

        def density(a, c):
            sums = [None] * COLS
            row_with_itself(a, sums)
            own_tiles(
                a, 6, (lt[(a + 2) * 2], lt[(a + 2) * 2 + 1]), (3 * a + 2) * 9, sums, OWN_TILES, a + 1
            )
            keep(a, sums)
            return c

        lax.fori_loop(0, ROWS - 1, density, 0, unroll=UNROLL_DENSITY)
        diagonals, edges = position_copies
        for copy in edges:
            copy.wait()
        for d, block in enumerate((BOTTOM, TOP, RIGHT, LEFT)):
            for f in range(2):
                xp[f, block] = rb[d, 3 * f] + relax0 * rb[d, 3 * f + 1] + relax1 * rb[d, 3 * f + 2]
        for block in EDGES:
            jrow, _ = feature_rows(xp[0, block], xp[1, block])
            put(fb, jrow, block * 8)
        for block in (TOP, BOTTOM):
            for g in range(2):
                lt[block * 2 + g] = turned([block * 8 + GROUP_START[g] + s for s in range(4)])
        for q in range(3):
            gh[q] = turned([b * 8 + s for r in (2 * q, 2 * q + 1) for b, s in side_cells(r)])
        sums = [None] * COLS
        row_with_itself(ROWS - 1, sums)
        keep(ROWS - 1, sums)

        def side_density(tiles):
            for t, a, ox, r, row in tiles:
                sums = [None] * COLS
                if row:
                    own_tiles(a, (ox + 1) * 3, (lt[(r + 1) * 2], lt[(r + 1) * 2 + 1]), t * 9, sums)
                else:
                    edge_tile(a, (ox + 1) * 3, r, t * 9, sums)
                for s in range(COLS):
                    if sums[s] is not None:
                        da[a * 64 + s * 8 : a * 64 + s * 8 + 8, :] += sums[s]

        edge_tiles = side_tiles("edges")
        side_density(edge_tiles[:EDGE_FIRST])
        for copy in diagonals:
            copy.wait()
        for d in range(4):
            for f in range(2):
                xp[f, CORNERS, PLACE[d] : PLACE[d] + 1, :] = (
                    crb[d, 3 * f : 3 * f + 1, :] + relax0[0:1] * crb[d, 3 * f + 1 : 3 * f + 2, :]
                    + relax1[0:1] * crb[d, 3 * f + 2 : 3 * f + 3, :]
                )
        jrow, _ = feature_rows(xp[0, CORNERS], xp[1, CORNERS])
        put(fb, jrow, CORNERS * 8)
        gh[3] = turned([CORNERS * 8 + q for q in range(4)])
        side_density(edge_tiles[EDGE_FIRST:-1] + side_tiles("corners") + edge_tiles[-1:])

    def bounds_copies(now, src_slot, dst, send, recv, targets):
        return [
            pltpu.make_async_remote_copy(
                src_ref=ar0.at[now, src_slot], dst_ref=dst.at[now, d],
                send_sem=send.at[now, d], recv_sem=recv.at[now, d],
                device_id=target, device_id_type=MESH,
            )
            for d, target in enumerate(targets)
        ]

    def forces(it):
        now = lax.rem(it, 2)
        alive = st[4] > 0.5
        hot = st[5] > 0.5
        rows = []
        for a in range(ROWS):
            parts = [da[pl.ds(a * 64 + q, 8, stride=8), :] for q in range(8)]
            while len(parts) > 1:
                parts = [parts[q] + parts[q + 1] for q in range(0, len(parts), 2)]
            rows.append(parts[0])
        density_now = KERNEL_NORM * jnp.stack(rows)
        ratio = density_now / jnp.where(hot, REST_HEAVY, REST_LIGHT)
        lit = alive & jnp.logical_not(hot)
        hvy = alive & hot
        peaks = (
            jnp.where(lit, ratio, NEG), jnp.where(hvy, ratio, NEG),
            jnp.where(lit, -ratio, NEG), jnp.where(hvy, -ratio, NEG),
        )
        vec = jnp.full((1, 128), NEG, f32)
        for q in range(4):
            top = jnp.max(jnp.max(peaks[q], axis=0), axis=0, keepdims=True)
            top = jnp.max(top, axis=1, keepdims=True)
            vec = jnp.where(lane == q, top, vec)
        ar0[now, 0] = vec
        first = bounds_copies(now, 0, ar1, a1s, a1r, first_peers)
        for copy in first:
            copy.start()

        safe = jnp.where(alive, density_now, 1.0)
        inverse = 1.0 / (safe * safe)
        excess = jnp.where(hot, STIFF_HEAVY, STIFF_LIGHT) * (ratio - 1.0)
        t0 = jnp.where(alive, st[6] * inverse, 0.0)
        u = excess * inverse
        u0 = jnp.where(lit, u, 0.0)
        u1 = jnp.where(hvy, u, 0.0)
        tp[0, 1 : ROWS + 1] = t0
        tp[1, 1 : ROWS + 1] = u0
        tp[2, 1 : ROWS + 1] = u1
        pack(tp, tstage, ctstage, 3)
        start(term_copies)

        for a in range(ROWS):
            put(fb, moment_rows(a + 1, xp[0, a + 1] + (a - 2.5), xp[1, a + 1] + row_cols), (a + 1) * 8)
        for a in range(ROWS):
            for s in range(COLS):
                tf[a + 1, s] = cell(fb, (a + 1) * 8 + s).astype(bf16)

        def force(a, c):
            here = [None] * COLS
            below = [None] * COLS
            own_pulls(a + 1, (3 * a + 1) * 9, here, a + 1, here, ROW_TILES)
            own_pulls(a + 2, (3 * a + 2) * 9, here, a + 1, below, OWN_TILES)
            for s in range(COLS):
                fa[a, s] += here[s]
                fa[a + 1, s] = below[s]
            return c

        for s in range(COLS):
            fa[0, s] = jnp.zeros((32, 128), f32)
        lax.fori_loop(0, FORCE_FIRST, force, 0)
        for copy in first:
            copy.wait()
        best = vec
        for d in range(len(first_peers)):
            best = jnp.maximum(best, ar1[now, d])
        ar0[now, 1] = best
        second = bounds_copies(now, 1, ar2, a2s, a2r, second_peers)
        for copy in second:
            copy.start()

        lax.fori_loop(FORCE_FIRST, ROWS - 1, force, 0)
        here = [None] * COLS
        own_pulls(ROWS, (3 * ROWS - 2) * 9, here, ROWS, here, ROW_TILES)
        add_up(fa, ROWS - 1, here)

        diagonals, edges = term_copies
        for copy in edges:
            copy.wait()
        for d, block in enumerate((BOTTOM, TOP, RIGHT, LEFT)):
            for f in range(3):
                tp[f, block] = trb[d, f]
        edge_x = {TOP: -3.5, BOTTOM: 3.5, LEFT: sub_f - 2.5, RIGHT: sub_f - 2.5}
        edge_y = {TOP: row_cols, BOTTOM: row_cols, LEFT: -3.5, RIGHT: 3.5}
        for block in EDGES:
            put(fb, moment_rows(block, xp[0, block] + edge_x[block], xp[1, block] + edge_y[block]), block * 8)
        for block in EDGES:
            for s in range(ROWS):
                tf[block, s] = cell(fb, block * 8 + s).astype(bf16)

        def side_pull(t, r, sums):
            (lb, ls), (ub, us) = side_cells(r)
            hi, lo = halves_of(wb[t * 9 + 8])
            pull(hi, lo, jnp.concatenate([tf[lb, ls], tf[ub, us]], axis=0), sums, (0, COLS - 1))

        for t, a, ox, r, row in side_tiles("edges"):
            sums = [None] * COLS
            if row:
                own_pulls(r + 1, t * 9, sums)
            else:
                side_pull(t, r, sums)
            add_up(fa, a, sums)

        for copy in diagonals:
            copy.wait()
        for d in range(4):
            for f in range(3):
                tp[f, CORNERS, PLACE[d] : PLACE[d] + 1, :] = ctrb[d, f : f + 1, :]
        corner_x = jnp.where(sub < 2, -3.5, 3.5)
        corner_y = jnp.where(lax.rem(sub, 2) == 0, -3.5, 3.5)
        put(fb, moment_rows(CORNERS, xp[0, CORNERS] + corner_x, xp[1, CORNERS] + corner_y), CORNERS * 8)
        for s in range(4):
            tf[CORNERS, s] = cell(fb, CORNERS * 8 + s).astype(bf16)
        for t, a, ox, r, row in side_tiles("corners"):
            sums = [None] * COLS
            side_pull(t, r, sums)
            add_up(fa, a, sums)

        for a in range(ROWS):
            for s in range(COLS):
                part = fa[a, s]
                row = a * 8 + s
                mb[pl.ds(row, 8, stride=FS), :] = part[0:8] + part[8:16] + part[16:24]
                mb[pl.ds(8 * FS + row, 8, stride=FS), :] = part[24:32]

        for a in range(ROWS):
            def mom(q):
                return mb[q * FS + a * 8 : q * FS + a * 8 + 8, :]

            s1 = mom(8) + mom(12)
            factor = jnp.where(
                alive[a], 6.0 * KERNEL_NORM / jnp.where(hot[a], MASS_HEAVY, MASS_LIGHT), 0.0
            )
            for f in range(2):
                p = xp[f, a + 1] + (a - 2.5 if f == 0 else row_cols)
                arm = p * s1 - mom(f)
                for q, term in enumerate((t0[a], u0[a], u1[a])):
                    push = term * arm + p * (mom(9 + q) + mom(13 + q)) - mom(2 + 2 * q + f)
                    st[7 + 3 * f + q, a] = jnp.where(alive[a], factor * push, 0.0)

        @pl.when(it < ITERS - 1)
        def _():
            coefficients()
            start(position_copies)

        for copy in second:
            copy.wait()
        for d in range(len(second_peers)):
            best = jnp.maximum(best, ar2[now, d])
        out_ref[pl.ds(OUT_MONITOR + it, 1), :] = jnp.where(lane < 2, best, -best)
        relax0 = jnp.broadcast_to(1.0 / (1.0 + best[:, 0:1] + best[:, 2:3]), (8, 128))
        relax1 = jnp.broadcast_to(1.0 / (1.0 + best[:, 1:2] + best[:, 3:4]), (8, 128))
        rl[0] = relax0
        rl[1] = relax1
        for a in range(ROWS):
            relax = jnp.where(hot[a], relax1, relax0)
            st[6, a] = jnp.where(alive[a], st[6, a] + relax * excess[a], 0.0)

    coefficients()
    pl.semaphore_wait(barrier, len(neighbours) + len(first_peers) + len(second_peers))
    start(position_copies)

    def whole(it, carry):
        densities(it)
        forces(it)
        return carry

    lax.fori_loop(0, ITERS, whole, 0)

    for a in range(ROWS):
        live = st[4, a]
        for f in range(2):
            accel = st[7 + 3 * f, a] + rl[0] * st[8 + 3 * f, a] + rl[1] * st[9 + 3 * f, a]
            v = live * (st[2 + f, a] + TIME_STEP * (st[13 + f, a] + accel))
            p = live * (st[f, a] + TIME_STEP * v)
            out_ref[pl.ds(a * 12 + f, COLS, stride=2), :] = p[0:COLS]
            out_ref[pl.ds(OUT_VELOCITY + a * 12 + f, COLS, stride=2), :] = v[0:COLS]
        out_ref[OUT_PRESSURE + a * 8 : OUT_PRESSURE + a * 8 + 8, :] = st[6, a]


def spread(in_ref, npos_ref, nvel_ref, pres_ref, mon_ref, rest, sems):
    copies = [
        pltpu.make_async_copy(in_ref.at[pl.ds(first, out.shape[0])], out, sems.at[q])
        for q, (first, out) in enumerate(((0, npos_ref), (OUT_VELOCITY, nvel_ref), (OUT_PRESSURE, rest)))
    ]
    for copy in copies:
        copy.start()
    for copy in copies:
        copy.wait()
    for a in range(ROWS):
        pres_ref[a] = rest[a * 8 : a * 8 + COLS, :]
    mon_ref[...] = rest[ROWS * 8 : ROWS * 8 + ITERS, 0:4]


def flat(value):
    return value.transpose(1, 2, 0, 3).reshape(ROWS * COLS * 2, 128)


def unflat(value):
    return value.reshape(ROWS, COLS, 2, 128).transpose(2, 0, 1, 3)


def local(position, velocity, other_accel, phase_ids, counts):
    vmem = pl.BlockSpec(memory_space=pltpu.VMEM)
    hbm = pl.BlockSpec(memory_space=pl.ANY)
    dma = pltpu.SemaphoreType.DMA
    n1 = lax.axis_size("y") * lax.axis_size("core") - 1
    n2 = lax.axis_size("x") * lax.axis_size("zl") * lax.axis_size("zh") - 1
    packed = pl.pallas_call(
        kernel,
        out_shape=jax.ShapeDtypeStruct((OUT_ROWS, 128), f32),
        in_specs=[hbm] * 4 + [pl.BlockSpec(memory_space=pltpu.SMEM)],
        out_specs=vmem,
        scratch_shapes=[
            pltpu.VMEM((ROWS * COLS * 2, 128), f32),
            pltpu.VMEM((ROWS * COLS * 2, 128), f32),
            pltpu.VMEM((ROWS * COLS * 2, 128), f32),
            pltpu.VMEM((ROWS, COLS, 128), jnp.int32),
            pltpu.VMEM((15, ROWS, 8, 128), f32),
            pltpu.VMEM((2, BLOCKS, 8, 128), f32),
            pltpu.VMEM((6, BLOCKS, 8, 128), f32),
            pltpu.VMEM((3, BLOCKS, 8, 128), f32),
            pltpu.VMEM((2, 6, 8, 128), f32),
            pltpu.VMEM((2, 3, 8, 128), f32),
            pltpu.VMEM((4, 8, 128), f32),
            pltpu.VMEM((4, 8, 128), f32),
            pltpu.VMEM((4, 6, 8, 128), f32),
            pltpu.VMEM((4, 3, 8, 128), f32),
            pltpu.VMEM((4, 8, 128), f32),
            pltpu.VMEM((4, 8, 128), f32),
            pltpu.VMEM((32 * FS, 128), f32),
            pltpu.VMEM((32 * FS, 128), f32),
            pltpu.VMEM((16, 128, 128), bf16),
            pltpu.VMEM((4, 128, 128), bf16),
            pltpu.VMEM((162, 128, 256), f32),
            pltpu.VMEM((ROWS * COLS, 128, 128), f32),
            pltpu.VMEM((ROWS * 64, 128), f32),
            pltpu.VMEM((ROWS, COLS, 32, 128), f32),
            pltpu.VMEM((BLOCKS, 8, 32, 128), bf16),
            pltpu.VMEM((16 * FS, 128), f32),
            pltpu.VMEM((9, 16, 128), f32),
            pltpu.VMEM((9, 16, 128), f32),
            pltpu.VMEM((2, 8, 128), f32),
            pltpu.VMEM((2, 2, 1, 128), f32),
            pltpu.VMEM((2, n1, 1, 128), f32),
            pltpu.VMEM((2, n2, 1, 128), f32),
            dma((4,)), dma((8,)), dma((8,)), dma((8,)), dma((8,)),
            dma((2, n1)), dma((2, n1)), dma((2, n2)), dma((2, n2)),
        ],
        compiler_params=pltpu.CompilerParams(
            collective_id=0, has_side_effects=True, vmem_limit_bytes=60 * 1024 * 1024
        ),
    )(flat(position), flat(velocity), flat(other_accel), phase_ids, counts)
    new_pos, new_vel, pressure, monitor = pl.pallas_call(
        spread,
        out_shape=(
            jax.ShapeDtypeStruct((ROWS * COLS * 2, 128), f32),
            jax.ShapeDtypeStruct((ROWS * COLS * 2, 128), f32),
            jax.ShapeDtypeStruct((ROWS, COLS, 128), f32),
            jax.ShapeDtypeStruct((ITERS, 4), f32),
        ),
        in_specs=[hbm],
        out_specs=[vmem] * 4,
        scratch_shapes=[pltpu.VMEM((OUT_ROWS - OUT_PRESSURE, 128), f32), dma((3,))],
        compiler_params=pltpu.CompilerParams(vmem_limit_bytes=60 * 1024 * 1024),
    )(packed)
    return unflat(new_pos), unflat(new_vel), pressure, monitor


def solution(mesh):
    gx = ("x", "zl")
    gy = ("zh", "y", "core")
    torus = Mesh(mesh.devices.reshape(4, 2, 2, 4, 2), SPLIT)
    wide = P(None, gx, gy, None)
    return jax.shard_map(
        local, mesh=torus, in_specs=(wide, wide, wide, P(gx, gy, None), P(gx, gy)),
        out_specs=(wide, wide, P(gx, gy, None), P()), check_vma=False,
    )
```
